128 devices in a mesh: part: 1, loc: 2 (over core), grp: 64 (over z, y, x).
Axes of the slice: x: 4, y: 4, z: 4, core: 2. Of those that a mesh axis runs over, the one named last changes fastest.
Arguments:
- x_rows: bfloat16 [98304, 1024], P(('part', 'grp', 'loc'))
- dy_rows: bfloat16 [98304, 1024], P(('part', 'grp', 'loc'))
- expert_ids: int32 [98304, 8], P(('part', 'grp', 'loc'))
- gate_vals: float32 [98304, 8], P(('part', 'grp', 'loc'))
- w_gate: bfloat16 [128, 1024, 384], P(('part', 'grp', 'loc'))
- w_up: bfloat16 [128, 1024, 384], P(('part', 'grp', 'loc'))
- w_down: bfloat16 [128, 384, 1024], P(('part', 'grp', 'loc'))
Outputs:
- output 1: bfloat16 [98304, 1024], P(('part', 'grp', 'loc'))
- output 2: float32 [98304, 8], P(('part', 'grp', 'loc'))
- output 3: bfloat16 [128, 1024, 384], P(('part', 'grp', 'loc'))
- output 4: bfloat16 [128, 1024, 384], P(('part', 'grp', 'loc'))
- output 5: bfloat16 [128, 384, 1024], P(('part', 'grp', 'loc'))
All inputs are finite; a program needn't handle non-finite values.
Results may differ from the reference program's by a relative error of at most 0.001.
Values are sent between devices in bfloat16 or wider.
A program may use at most 1 GiB of HBM per device.

```python
import jax
import jax.numpy as jnp
from jax import lax

GROUPS = 64
LOC_DEVS = 2
TOK_DEV = 768
EXPERTS = 128
TOP_K = 8
D_MODEL = 1024
D_FF = 384

DEV_COUNT = GROUPS * LOC_DEVS
TOKENS = TOK_DEV * DEV_COUNT
NUM_ITEMS = TOKENS * TOP_K
GROUP_LIMIT = min(TOP_K // 2, GROUPS)
PER_GROUP = TOP_K // GROUP_LIMIT
GROUP_EXPERTS = EXPERTS // GROUPS
GROUP_ROWS = GROUP_LIMIT * TOK_DEV // GROUPS
MEAN_LOAD = TOK_DEV * TOP_K // EXPERTS
SPREAD_MAX = min(MEAN_LOAD, GROUP_ROWS - MEAN_LOAD)
EXPERT_CAP = DEV_COUNT * (MEAN_LOAD + SPREAD_MAX)


def block_routing(block_key):
    key_sig, key_off, key_perm, key_amp, key_slot = jax.random.split(block_key, 5)
    tok_perm = jax.random.permutation(key_sig, TOK_DEV)
    offsets = jax.random.permutation(key_off, GROUPS)[:GROUP_LIMIT]
    shifted = (tok_perm[:, None] + offsets[None, :]) % TOK_DEV
    group_of = shifted % GROUPS
    pair_pos = jnp.arange(GROUP_LIMIT)[None, :] * (TOK_DEV // GROUPS) + shifted // GROUPS
    local_perm = jax.vmap(lambda sub_key: jax.random.permutation(sub_key, GROUP_EXPERTS))(jax.random.split(key_perm, GROUPS))
    spread = jax.random.randint(key_amp, (GROUPS, GROUP_EXPERTS // 2), 0, SPREAD_MAX + 1)
    spread = spread.at[:, 0].set(SPREAD_MAX)
    counts = jnp.stack([MEAN_LOAD + spread, MEAN_LOAD - spread], axis=-1).reshape(GROUPS, GROUP_EXPERTS)
    cum_ends = jnp.cumsum(counts, axis=1)
    seq_pos = jnp.arange(PER_GROUP)[None, None, :] * GROUP_ROWS + pair_pos[:, :, None]
    rank_idx = jnp.sum(seq_pos[..., None] >= cum_ends[group_of][:, :, None, :], axis=-1)
    local_ids = local_perm[group_of[:, :, None], rank_idx]
    expert = (group_of[:, :, None] * GROUP_EXPERTS + local_ids).reshape(TOK_DEV, TOP_K)
    slot_keys = jax.random.randint(key_slot, (TOK_DEV, TOP_K), 0, 4096) * TOP_K + jnp.arange(TOP_K)[None, :]
    slot_order = jnp.argsort(slot_keys, axis=1)
    return jnp.take_along_axis(expert, slot_order, axis=1).astype(jnp.int32)


def draw_routing(route_key):
    blocks = jax.vmap(block_routing)(jax.random.split(route_key, DEV_COUNT))
    return blocks.reshape(TOKENS, TOP_K)


def setup_inputs(seed: int = 0, part: int = 0) -> dict:
    base_key = jax.random.fold_in(jax.random.key(seed), part)
    keys = jax.random.split(base_key, 7)
    x_rows = jax.random.normal(keys[0], (TOKENS, D_MODEL), jnp.float32).astype(jnp.bfloat16)
    dy_rows = jax.random.normal(keys[1], (TOKENS, D_MODEL), jnp.float32).astype(jnp.bfloat16)
    expert_ids = draw_routing(keys[2])
    gate_vals = jax.random.uniform(keys[3], (TOKENS, TOP_K), jnp.float32, 0.25, 1.0)
    w_gate = (jax.random.normal(keys[4], (EXPERTS, D_MODEL, D_FF), jnp.float32) * D_MODEL ** -0.5).astype(jnp.bfloat16)
    w_up = (jax.random.normal(keys[5], (EXPERTS, D_MODEL, D_FF), jnp.float32) * D_MODEL ** -0.5).astype(jnp.bfloat16)
    w_down = (jax.random.normal(keys[6], (EXPERTS, D_FF, D_MODEL), jnp.float32) * D_FF ** -0.5).astype(jnp.bfloat16)
    return {'x_rows': x_rows, 'dy_rows': dy_rows, 'expert_ids': expert_ids, 'gate_vals': gate_vals, 'w_gate': w_gate, 'w_up': w_up, 'w_down': w_down}


def expert_lists(expert_ids):
    flat_ids = expert_ids.reshape(-1)
    item_order = jnp.argsort(flat_ids, stable=True)
    sorted_ids = flat_ids[item_order]
    load_sizes = jnp.zeros((EXPERTS,), jnp.int32).at[flat_ids].add(1)
    starts = jnp.cumsum(load_sizes) - load_sizes
    slot_rank = jnp.arange(NUM_ITEMS) - starts[sorted_ids]
    slot_lists = jnp.full((EXPERTS * EXPERT_CAP,), NUM_ITEMS, jnp.int32)
    slot_lists = slot_lists.at[sorted_ids * EXPERT_CAP + slot_rank].set(item_order.astype(jnp.int32))
    return slot_lists.reshape(GROUPS, GROUP_EXPERTS, EXPERT_CAP)


def reference(x_rows, dy_rows, expert_ids, gate_vals, w_gate, w_up, w_down):
    slot_lists = expert_lists(expert_ids)
    gate_flat = gate_vals.reshape(-1)

    def expert_step(part_sum, inputs):
        slot_items, wg_one, wu_one, wd_one = inputs
        is_live = slot_items < NUM_ITEMS
        tok_idx = jnp.where(is_live, slot_items // TOP_K, 0)
        x_sel = jnp.where(is_live[:, None], x_rows[tok_idx], 0).astype(jnp.bfloat16)
        dy_sel = jnp.where(is_live[:, None], dy_rows[tok_idx], 0).astype(jnp.bfloat16)
        gate_sel = jnp.where(is_live, gate_flat[jnp.minimum(slot_items, NUM_ITEMS - 1)], 0.0)
        pre_gate = jnp.dot(x_sel, wg_one, preferred_element_type=jnp.float32)
        pre_up = jnp.dot(x_sel, wu_one, preferred_element_type=jnp.float32)
        sig_gate = jax.nn.sigmoid(pre_gate)
        silu_out = pre_gate * sig_gate
        hidden = (silu_out * pre_up).astype(jnp.bfloat16)
        expert_out = jnp.dot(hidden, wd_one, preferred_element_type=jnp.float32)
        dgate_sel = jnp.sum(dy_sel.astype(jnp.float32) * expert_out, axis=-1)
        d_out = (gate_sel[:, None] * dy_sel.astype(jnp.float32)).astype(jnp.bfloat16)
        d_hidden = jnp.dot(d_out, wd_one.T, preferred_element_type=jnp.float32)
        dwd_one = jnp.dot(hidden.T, d_out, preferred_element_type=jnp.float32).astype(jnp.bfloat16)
        d_pre_up = (d_hidden * silu_out).astype(jnp.bfloat16)
        d_pre_gate = (d_hidden * pre_up * sig_gate * (1.0 + pre_gate * (1.0 - sig_gate))).astype(jnp.bfloat16)
        dwg_one = jnp.dot(x_sel.T, d_pre_gate, preferred_element_type=jnp.float32).astype(jnp.bfloat16)
        dwu_one = jnp.dot(x_sel.T, d_pre_up, preferred_element_type=jnp.float32).astype(jnp.bfloat16)
        d_rows = (jnp.dot(d_pre_gate, wg_one.T, preferred_element_type=jnp.float32) + jnp.dot(d_pre_up, wu_one.T, preferred_element_type=jnp.float32)).astype(jnp.bfloat16)
        part_sum = part_sum.at[tok_idx].add(d_rows.astype(jnp.float32))
        return part_sum, (dwg_one, dwu_one, dwd_one, dgate_sel)

    def group_step(dx_acc, inputs):
        part_sum, outputs = lax.scan(expert_step, jnp.zeros((TOKENS, D_MODEL), jnp.float32), inputs)
        return dx_acc + part_sum.astype(jnp.bfloat16).astype(jnp.float32), outputs

    weights = (w_gate.reshape(GROUPS, GROUP_EXPERTS, D_MODEL, D_FF), w_up.reshape(GROUPS, GROUP_EXPERTS, D_MODEL, D_FF), w_down.reshape(GROUPS, GROUP_EXPERTS, D_FF, D_MODEL))
    dx_acc, outputs = lax.scan(group_step, jnp.zeros((TOKENS, D_MODEL), jnp.float32), (slot_lists,) + weights)
    dw_gate, dw_up, dw_down, dgate_vals = outputs
    d_gates = jnp.zeros((NUM_ITEMS + 1,), jnp.float32).at[slot_lists.reshape(-1)].set(dgate_vals.reshape(-1))
    return (dx_acc.astype(jnp.bfloat16), d_gates[:NUM_ITEMS].reshape(TOKENS, TOP_K), dw_gate.reshape(EXPERTS, D_MODEL, D_FF), dw_up.reshape(EXPERTS, D_MODEL, D_FF), dw_down.reshape(EXPERTS, D_FF, D_MODEL))
```

```python
import jax
import jax.numpy as jnp
from jax import lax
from jax.experimental import pallas as pl
from jax.experimental.pallas import tpu as pltpu
from jax.sharding import PartitionSpec as P

MESH = pl.DeviceIdType.MESH
LANES = 128
WIDE = 256
F32 = jnp.float32
BF16 = jnp.bfloat16
SIDE = 4
PLANE = SIDE * SIDE
GROUPS = SIDE ** 3
TOK = 768
TOP_K = 8
D = 1024
F = 384
SLOTS = 48
ROUNDS = 3
RS = SLOTS // ROUNDS
NBLK = TOK // LANES
FWD = ((0, 640), (640, 640), (1280, 768))
BWD = ((0, 384), (384, 384), (768, 256))
OFFS = sorted(((a, b) for a in range(SIDE) for b in range(SIDE) if (a, b) != (0, 0)),
              key=lambda o: sum(min(v, SIDE - v) for v in o))


def dot(a, b, ca=1, cb=0):
    return lax.dot_general(a, b, (((ca,), (cb,)), ((), ())), preferred_element_type=F32)


def first(n):
    return pl.ds(0, n)


def over_lanes(v):
    return jnp.sum(v, axis=1, keepdims=True)


def over_rows(v):
    return jnp.sum(v, axis=0, keepdims=True)


def iota(shape, dim):
    return lax.broadcasted_iota(jnp.int32, shape, dim)


def kernel(x_hbm, dy_hbm, idst_hbm, gatt_hbm, ids_ref, wg_hbm, wu_hbm, wd_hbm,
           dx_hbm, dgate_ref, dwg_hbm, dwu_hbm, dwd_hbm, ia, ib, ic, rb,
           gat, snd, rx, wgu, wdn, acc, hd, ubuf, abuf, pbuf, slots, gws, slotn, idst, gatt,
           mg, mr, dgb, dgr, dgi, dgh, vbuf, dgacc,
           loc_sem, meta_s, meta_r, g1_s, g1_r, g2_s, g2_r, f2_s, f2_r, mg_s, mg_r, d2_s, d2_r, dm_s, dm_r,
           c_s, c_r, dg_s, dg_r, b1_s, b1_r, b1m_s, b1m_r, bl_s, b2_s, b2_r, b2m_s, b2m_r, out_s, credit):
    g = lax.axis_index('grp')
    l = lax.axis_index('loc')
    z, y, x = g // PLANE, (g // SIDE) % SIDE, g % SIDE
    coord = (x, y, z)
    other = 1 - l

    def gid(zz, yy, xx):
        return zz * PLANE + yy * SIDE + xx

    def along(c, k):
        return gid(*(k if a == c else coord[a] for a in (2, 1, 0)))

    def in_plane(c, a, b):
        if c == 0:
            return gid(a, b, x)
        if c == 1:
            return gid(a, y, b)
        return gid(z, a, b)

    my_plane = ((z, y), (z, x), (y, x))
    my_p = tuple(a * SIDE + b for a, b in my_plane)

    def rmod(v):
        return lax.rem(v, SIDE)

    def remote(src, dst, ss, rs, grp=None, loc=None):
        return pltpu.make_async_remote_copy(src, dst, ss, rs, device_id={'grp': g if grp is None else grp, 'loc': l if loc is None else loc},
                                            device_id_type=MESH)

    def local(src, dst, sem):
        return pltpu.make_async_copy(src, dst, sem)

    barrier = pltpu.get_barrier_semaphore()
    peers = []
    for dz in range(SIDE):
        for dyy in range(SIDE):
            for dxx in range(SIDE):
                if (dz, dyy, dxx) != (0, 0, 0) and 0 in (dz, dyy, dxx):
                    peers.append(gid(rmod(z + dz), rmod(y + dyy), rmod(x + dxx)))
    for p in peers:
        pl.semaphore_signal(barrier, inc=1, device_id={'grp': p, 'loc': l}, device_id_type=MESH)
    pl.semaphore_signal(barrier, inc=1, device_id={'grp': g, 'loc': other}, device_id_type=MESH)
    pl.semaphore_wait(barrier, len(peers) + 1)

    def slab_copies(c, make):
        c0, w = FWD[c]
        out = []
        if c0 < D:
            n = min(w, D - c0)
            out.append(make(x_hbm.at[:, pl.ds(c0, n)], pl.ds(c0, n)))
        if c0 + w > D:
            s = max(c0, D)
            out.append(make(dy_hbm.at[:, pl.ds(s - D, c0 + w - s)], pl.ds(s, c0 + w - s)))
        return out

    def cols(c):
        return pl.ds(*FWD[c])

    for c in range(3):
        for k in (1, 3, 2):
            t = along(c, rmod(coord[c] + k))
            remote(idst_hbm, idst.at[c, coord[c]], meta_s.at[c, 0], meta_r.at[c, 0], t).start()
            if c == 0:
                remote(gatt_hbm, gatt.at[x], meta_s.at[c, 1], meta_r.at[c, 1], t).start()
    for d, k in enumerate((1, 3)):
        for c in range(3):
            t = along(c, rmod(coord[c] + k))
            for cp in slab_copies(c, lambda src, cs: remote(src, gat.at[coord[c], :, cs], g1_s.at[c, d], g1_r.at[c, d], t)):
                cp.start()
    for c in range(3):
        local(idst_hbm, idst.at[c, coord[c]], loc_sem.at[0, c]).start()
    local(gatt_hbm, gatt.at[x], loc_sem.at[0, 3]).start()
    for c in range(3):
        for cp in slab_copies(c, lambda src, cs: local(src, gat.at[coord[c], :, cs], loc_sem.at[1, c])):
            cp.start()
    weights = [local(wg_hbm, wgu.at[:, first(F)], loc_sem.at[2, 0]), local(wu_hbm, wgu.at[:, pl.ds(F, F)], loc_sem.at[2, 1]),
               local(wd_hbm, wdn, loc_sem.at[2, 2])]
    for cp in weights:
        cp.start()
    for c in range(3):
        local(idst_hbm, idst.at[c, coord[c]], loc_sem.at[0, c]).wait()
    local(gatt_hbm, gatt.at[x], loc_sem.at[0, 3]).wait()

    tri = (iota((LANES, LANES), 0) < iota((LANES, LANES), 1)).astype(BF16)

    def plane_gid(c):
        p = iota((PLANE, 1), 0)
        a, b = p // SIDE, lax.rem(p, SIDE)
        return in_plane(c, a, b)

    def make_table(c, k):
        gids = plane_gid(c)
        carry = jnp.zeros((PLANE, 1), F32)
        for blk in range(NBLK):
            ls = pl.ds(blk * LANES, LANES)
            ids = idst[c, k, :, ls]
            member = jnp.zeros((PLANE, LANES), F32)
            w0 = jnp.zeros((PLANE, LANES), F32)
            w1 = jnp.zeros((PLANE, LANES), F32)
            for j in range(TOP_K):
                idj = ids[j:j + 1, :]
                e0 = idj == 2 * gids
                e1 = idj == 2 * gids + 1
                member = jnp.where(e0 | e1, 1.0, member)
                if c == 0:
                    gj = gatt[k, pl.ds(j, 1), ls]
                    w0 = jnp.where(e0, gj, w0)
                    w1 = jnp.where(e1, gj, w1)
            rank = dot(member.astype(BF16), tri) + carry
            carry = carry + over_lanes(member)
            slots[c, k, :, ls] = jnp.where(member > 0, rank, -1.0)
            if c == 0:
                gws[k, 0, :, ls] = w0
                gws[k, 1, :, ls] = w1

    for c in range(3):
        make_table(c, coord[c])

    rowtri = (iota((LANES, LANES), 1) < iota((LANES, LANES), 0)).astype(BF16)
    carry = jnp.zeros((1, GROUPS), F32)
    for blk in range(NBLK):
        ts = pl.ds(blk * LANES, LANES)
        ids = ids_ref[ts, :]
        member = jnp.zeros((LANES, GROUPS), F32)
        for j in range(TOP_K):
            member = jnp.where((ids[:, j:j + 1] // 2) == iota((1, GROUPS), 1), 1.0, member)
        rank = dot(rowtri, member.astype(BF16)) + carry
        carry = carry + over_rows(member)
        slotn[ts, :] = jnp.where(member > 0, rank, -1.0).astype(BF16)

    for r in range(ROUNDS):
        mg[r] = jnp.zeros((PLANE, 1, LANES), F32)

    def gather(c, k, r, s):
        base = (iota((RS, 1), 0) + r * RS).astype(F32)
        lane = iota((RS, LANES), 1)
        row = iota((RS, 1), 0)

        def one(p, carry_):
            mask = slots[c, k, pl.ds(p, 1), :] == base
            pbuf[pl.ds(p * RS, RS), :] = mask.astype(F32).astype(BF16)
            if c == 0:
                line = jnp.zeros((1, LANES), F32)
                for e in range(2):
                    col = over_lanes(jnp.where(mask, gws[k, e, pl.ds(p, 1), :], 0.0))
                    line = line + over_rows(jnp.where(lane == e * 64 + k * RS + row, col, 0.0))
                mg[r, p] = mg[r, p] + line
            return carry_

        lax.fori_loop(0, PLANE, one, 0)
        c0, w = FWD[c]
        rows = dot(pbuf[...], gat[k, :, pl.ds(c0, w)]).astype(BF16)
        snd[s, :, k, :, pl.ds(c0, w)] = rows.reshape(PLANE, RS, w)

    def slot_of(r):
        return lax.rem(r, 2)

    def gather_all(c, k, rounds):
        def one(r, carry_):
            gather(c, k, r, slot_of(r))
            return carry_
        lax.fori_loop(rounds[0], rounds[1], one, 0)

    for c in range(3):
        for cp in slab_copies(c, lambda src, cs: local(src, gat.at[coord[c], :, cs], loc_sem.at[1, c])):
            cp.wait()
        gather_all(c, coord[c], (0, 2))
    acc[...] = jnp.zeros_like(acc)

    for c in range(3):
        proxy = idst.at[c, first(3)]
        local(proxy, proxy, meta_r.at[c, 0]).wait()
        local(proxy, proxy, meta_s.at[c, 0]).wait()
        if c == 0:
            proxy = gatt.at[first(3)]
            local(proxy, proxy, meta_r.at[c, 1]).wait()
            local(proxy, proxy, meta_s.at[c, 1]).wait()
    for c in range(3):
        for k in (1, 3, 2):
            make_table(c, rmod(coord[c] + k))

    half = TOK // 2
    for d, k in enumerate((1, 3)):
        for c in range(3):
            src = rmod(coord[c] + SIDE - k)
            block = gat.at[src, :, cols(c)]
            local(block, block, g1_r.at[c, d]).wait()
            t = along(c, rmod(coord[c] + k))
            part = gat.at[src, pl.ds(d * half, half), cols(c)]
            remote(part, part, g2_s.at[c, d], g2_r.at[c, d], t).start()
    for d, k in enumerate((1, 3)):
        for c in range(3):
            gather_all(c, rmod(coord[c] + SIDE - k), (0, 2))

    def send_round(r):
        s = slot_of(r)
        for a, b in OFFS:
            for c in range(3):
                pa, pb = rmod(my_plane[c][0] + a), rmod(my_plane[c][1] + b)
                src = snd.at[s, pa * SIDE + pb, :, :, cols(c)]
                dst = (rx.at[l, r, z, y, :, :, cols(c)], rx.at[l, r, z, :, x, :, cols(c)], rx.at[l, r, :, y, x, :, cols(c)])[c]
                t = in_plane(c, pa, pb)
                remote(src, dst, f2_s.at[r, c], f2_r.at[r, c], t).start()
                if c == 0:
                    remote(mg.at[r, pa * SIDE + pb], mr.at[l, r, z * SIDE + y], mg_s.at[r], mg_r.at[r], t).start()
        for c in range(3):
            own = snd[s, my_p[c], :, :, cols(c)]
            if c == 0:
                rx[l, r, z, y, :, :, cols(c)] = own
            elif c == 1:
                rx[l, r, z, :, x, :, cols(c)] = own
            else:
                rx[l, r, :, y, x, :, cols(c)] = own
        mr[l, r, z * SIDE + y] = mg[r, my_p[0]]

    def proxy15(c, table):
        c0, w = table[c]
        return snd.at[0, first(PLANE - 1), :, :, first(w)]

    def wait_send(r):
        for c in range(3):
            local(proxy15(c, FWD), proxy15(c, FWD), f2_s.at[r, c]).wait()
        m = mg.at[r, first(PLANE - 1)]
        local(m, m, mg_s.at[r]).wait()

    for c in range(3):
        for d in range(2):
            src = rmod(coord[c] + 2)
            part = gat.at[src, pl.ds(d * half, half), cols(c)]
            local(part, part, g2_r.at[c, d]).wait()
    for r in range(2):
        for c in range(3):
            gather_all(c, rmod(coord[c] + 2), (r, r + 1))
        send_round(r)
    wait_send(0)
    for c in range(3):
        def one(k, carry_):
            gather(c, k, 2, 0)
            return carry_
        lax.fori_loop(0, SIDE, one, 0)
    send_round(2)
    for cp in weights:
        cp.wait()

    mine = (iota((64, LANES), 1) == l * 64 + iota((64, LANES), 0))

    def chunk(r, kk):
        lp = jnp.where(kk < 2, l, other)
        z0 = lax.rem(kk, 2) * 2
        zs = pl.ds(z0, 2)

        def col(c0, w):
            return rx[lp, r, zs, :, :, :, pl.ds(c0, w)].reshape(512, w)

        abuf[...] = dot(col(0, D), wgu[...])
        for m in range(8):
            line = mr[lp, r, z0 * SIDE + m]
            gcol = over_lanes(jnp.where(mine, line, 0.0))
            part = rx[lp, r, z0 + m // SIDE, m % SIDE, :, :, pl.ds(D, D)].reshape(64, D)
            ubuf[pl.ds(m * 64, 64), :] = (gcol * part.astype(F32)).astype(BF16)
        dh = dot(ubuf[...], wdn[...], 1, 1)
        a = abuf[:, :F]
        b = abuf[:, F:]
        sig = jax.nn.sigmoid(a)
        silu = a * sig
        hd[:, first(F)] = (silu * b).astype(BF16)
        hd[:, pl.ds(F, F)] = (dh * b * sig * (1.0 + a * (1.0 - sig))).astype(BF16)
        hd[:, pl.ds(2 * F, F)] = (dh * silu).astype(BF16)
        dg = jnp.zeros((512, 1), F32)
        for n in range(4):
            o = dot(hd[:, first(F)], wdn[:, pl.ds(n * WIDE, WIDE)])
            dg = dg + over_lanes(col(D + n * WIDE, WIDE).astype(F32) * o)
        for m in range(8):
            line = over_rows(jnp.where(mine, dg[m * 64:(m + 1) * 64, :], 0.0))
            dgb[kk // 2, r, z0 * SIDE + m] = line
        acc[first(F), :] += dot(hd[:, first(F)], ubuf[...], 0, 0)
        acc[pl.ds(F, 2 * F), :] += dot(hd[:, pl.ds(F, 2 * F)], col(0, D), 0, 0)
        for n in range(4):
            cval = dot(hd[:, pl.ds(F, 2 * F)], wgu[pl.ds(n * WIDE, WIDE), :], 1, 1)
            rx[lp, r, zs, :, :, :, pl.ds(n * WIDE, WIDE)] = cval.astype(BF16).reshape(2, SIDE, SIDE, RS, WIDE)

    def relay(r):
        for c, buf in enumerate((ia, ib, ic)):
            local(proxy15(c, BWD), proxy15(c, BWD), b1_r.at[r, c]).wait()
            own = buf.at[r, 0, 0]
            local(own, own, bl_s.at[r, c]).wait()
        m = dgi.at[r, first(PLANE - 1)]
        local(m, m, b1m_r.at[r]).wait()
        for k in (1, 3, 2):
            for c, buf in enumerate((ia, ib, ic)):
                to = rmod(coord[c] + k)
                cs = pl.ds(*BWD[c])
                dst = (rb.at[r, :, :, x, :, cs], rb.at[r, :, y, :, :, cs], rb.at[r, z, :, :, :, cs])[c]
                remote(buf.at[r, :, :, to], dst, b2_s.at[r, c], b2_r.at[r, c], along(c, to)).start()
                if c == 0:
                    remote(dgi.at[r], dgh.at[r, x], b2m_s.at[r], b2m_r.at[r], along(0, to)).start()
        dgh[r, x] = dgi[r]

    def round_body(r, carry_):
        for c in range(3):
            local(proxy15(c, FWD), proxy15(c, FWD), f2_r.at[r, c]).wait()
        m = mg.at[0, first(PLANE - 1)]
        local(m, m, mg_r.at[r]).wait()
        for h in range(2):
            blk = rx.at[l, r, pl.ds(2 * h, 2)]
            remote(blk, blk, d2_s.at[r, h], d2_r.at[r, h], loc=other).start()
        remote(mr.at[l, r], mr.at[l, r], dm_s.at[r], dm_r.at[r], loc=other).start()

        def step(kk, carry2):
            @pl.when(kk >= 2)
            def _():
                blk = rx.at[other, r, pl.ds((kk - 2) * 2, 2)]
                local(blk, blk, d2_r.at[r, kk - 2]).wait()

            @pl.when(kk == 2)
            def _():
                local(mr.at[other, r], mr.at[other, r], dm_r.at[r]).wait()

            @pl.when(kk < 2)
            def _():
                blk = rx.at[l, r, pl.ds(kk * 2, 2)]
                local(blk, blk, d2_s.at[r, kk]).wait()

            chunk(r, kk)

            @pl.when(kk == 1)
            def _():
                pl.semaphore_signal(credit.at[r], inc=1, device_id={'grp': g, 'loc': other}, device_id_type=MESH)

                @pl.when(r > 0)
                def _():
                    relay(r - 1)

            @pl.when(kk == 2)
            def _():
                pl.semaphore_wait(credit.at[r], 1)

            @pl.when(kk >= 2)
            def _():
                zs = pl.ds((kk - 2) * 2, 2)
                remote(rx.at[other, r, zs, :, :, :, first(D)], rx.at[other, r, zs, :, :, :, pl.ds(D, D)],
                       c_s.at[r, kk - 2], c_r.at[r, kk - 2], loc=other).start()
            return carry2

        lax.fori_loop(0, 4, step, 0)
        remote(dgb.at[1, r], dgr.at[r], dg_s.at[r], dg_r.at[r], loc=other).start()
        for h in range(2):
            blk = rx.at[l, r, pl.ds(2 * h, 2), :, :, :, pl.ds(D, D)]
            local(blk, blk, c_r.at[r, h]).wait()

            def add(zy, carry2):
                zz, yy = 2 * h + zy // SIDE, lax.rem(zy, SIDE)
                p0 = rx[l, r, zz, yy, :, :, first(D)].astype(F32)
                p1 = rx[l, r, zz, yy, :, :, pl.ds(D, D)].astype(F32)
                rx[l, r, zz, yy, :, :, first(D)] = (p0 + p1).astype(BF16)
                return carry2

            lax.fori_loop(0, 8, add, 0)
        local(dgr.at[r], dgr.at[r], dg_r.at[r]).wait()
        dgb[0, r] = dgb[0, r] + dgr[r]
        for c, buf in enumerate((ia, ib, ic)):
            cs = pl.ds(*BWD[c])
            src = (rx.at[l, r, z, y, :, :, cs], rx.at[l, r, z, :, x, :, cs], rx.at[l, r, :, y, x, :, cs])[c]
            local(src, buf.at[r, my_plane[c][0], my_plane[c][1]], bl_s.at[r, c]).start()
        for a, b in OFFS:
            for c, buf in enumerate((ia, ib, ic)):
                pa, pb = rmod(my_plane[c][0] + a), rmod(my_plane[c][1] + b)
                cs = pl.ds(*BWD[c])
                src = (rx.at[l, r, pa, pb, :, :, cs], rx.at[l, r, pa, :, pb, :, cs], rx.at[l, r, :, pa, pb, :, cs])[c]
                t = in_plane(c, pa, pb)
                remote(src, buf.at[r, my_plane[c][0], my_plane[c][1]], b1_s.at[r, c], b1_r.at[r, c], t).start()
                if c == 0:
                    remote(dgb.at[0, r, pa * SIDE + pb], dgi.at[r, my_p[0]], b1m_s.at[r], b1m_r.at[r], t).start()
        dgi[r, my_p[0]] = dgb[0, r, my_p[0]]
        return carry_

    lax.fori_loop(0, ROUNDS, round_body, 0)

    for c in range(3):
        for d in range(2):
            part = gat.at[0, first(half), cols(c)]
            local(part, part, g2_s.at[c, d]).wait()
    gat[1, first(F), first(D)] = acc[first(F), :].astype(BF16)
    gat[2, first(2 * F), first(D)] = acc[pl.ds(F, 2 * F), :].astype(BF16)
    outs = [local(gat.at[1, first(F), first(D)], dwd_hbm, out_s.at[0]),
            local(gat.at[2, first(F), first(D)], dwg_hbm, out_s.at[1]),
            local(gat.at[2, pl.ds(F, F), first(D)], dwu_hbm, out_s.at[2])]

    relay(ROUNDS - 1)
    for cp in outs:
        cp.start()
    wait_send(1)
    wait_send(2)

    dgacc[...] = jnp.zeros_like(dgacc)
    acc[first(TOK), :] = jnp.zeros((TOK, D), F32)
    for r in range(ROUNDS):
        half_cols = (r % 2) * D
        stage = snd.at[r // 2, :, :, :, pl.ds(half_cols, D)]
        for c, buf in enumerate((ia, ib, ic)):
            own = snd.at[0, first(12), :, :, first(BWD[c][1])]
            local(own, own, b2_r.at[r, c]).wait()
        m = dgh.at[r, first(3)]
        local(m, m, b2m_r.at[r]).wait()
        pieces = []
        for zy in range(PLANE):
            pieces.append(local(rb.at[r, zy // SIDE, zy % SIDE], snd.at[r // 2, zy, :, :, pl.ds(half_cols, D)], loc_sem.at[3, 0]))
        for cp in pieces:
            cp.start()
        spread = (iota((GROUPS, GROUPS * RS), 0) == iota((GROUPS, GROUPS * RS), 1) // RS).astype(F32).astype(BF16)
        want = (lax.rem(iota((1, GROUPS * RS), 1), RS) + r * RS).astype(F32)
        for n in range(4):
            ns = pl.ds(n * WIDE, WIDE)
            got = dot(slotn[...], spread[:, n * WIDE:(n + 1) * WIDE])
            gat[0, :, ns] = (got == want[:, n * WIDE:(n + 1) * WIDE]).astype(F32).astype(BF16)
        lane = iota((RS, LANES), 1)
        row = iota((RS, LANES), 0)

        def one(gg, carry_):
            line = dgh[r, lax.rem(gg, SIDE), gg // SIDE]
            out = jnp.zeros((RS, LANES), F32)
            for e in range(2):
                colv = over_lanes(jnp.where(lane == e * 64 + x * RS + row, line, 0.0))
                out = jnp.where(lane == 2 * gg + e, colv, out)
            vbuf[pl.ds(gg * RS, RS), :] = out
            return carry_

        lax.fori_loop(0, GROUPS, one, 0)
        rest = vbuf[...]
        for _ in range(3):
            part = rest.astype(BF16)
            dgacc[...] += dot(gat[0, :, first(D)], part)
            rest = rest - part.astype(F32)
        for cp in pieces:
            cp.wait()
        own_pieces = []
        for q in range(PLANE):
            a, b = q // SIDE, q % SIDE
            own_pieces.append(local(ia.at[r, a, b, x], snd.at[r // 2, q, x, :, pl.ds(half_cols + BWD[0][0], BWD[0][1])], loc_sem.at[3, 1]))
            own_pieces.append(local(ib.at[r, a, b, y], snd.at[r // 2, a * SIDE + y, b, :, pl.ds(half_cols + BWD[1][0], BWD[1][1])], loc_sem.at[3, 1]))
            own_pieces.append(local(ic.at[r, a, b, z], snd.at[r // 2, z * SIDE + a, b, :, pl.ds(half_cols + BWD[2][0], BWD[2][1])], loc_sem.at[3, 1]))
        for cp in own_pieces:
            cp.start()
        for cp in own_pieces:
            cp.wait()
        for n in range(4):
            got = snd[r // 2, :, :, :, pl.ds(half_cols + n * WIDE, WIDE)].reshape(GROUPS * RS, WIDE)
            acc[first(TOK), pl.ds(n * WIDE, WIDE)] += dot(gat[0, :, first(D)], got)
    gat[3, :, first(D)] = acc[first(TOK), :].astype(BF16)
    dx_out = local(gat.at[3, :, first(D)], dx_hbm, out_s.at[3])
    dx_out.start()
    lane = iota((TOK, LANES), 1)
    for j in range(TOP_K):
        hit = lane == ids_ref[:, j:j + 1]
        dgate_ref[:, j:j + 1] = over_lanes(jnp.where(hit, dgacc[...], 0.0))

    for c in range(3):
        for d in range(2):
            block = gat.at[0, :, cols(c)]
            local(block, block, g1_s.at[c, d]).wait()
    for r in range(ROUNDS):
        local(mr.at[0, r], mr.at[0, r], dm_s.at[r]).wait()
        local(dgr.at[r], dgr.at[r], dg_s.at[r]).wait()
        for h in range(2):
            blk = rx.at[0, r, pl.ds(2 * h, 2), :, :, :, first(D)]
            local(blk, blk, c_s.at[r, h]).wait()
        for c in range(3):
            local(proxy15(c, BWD), proxy15(c, BWD), b1_s.at[r, c]).wait()
            own = snd.at[0, first(12), :, :, first(BWD[c][1])]
            local(own, own, b2_s.at[r, c]).wait()
        m = dgi.at[r, first(PLANE - 1)]
        local(m, m, b1m_s.at[r]).wait()
        m = dgh.at[r, first(3)]
        local(m, m, b2m_s.at[r]).wait()
    for cp in outs:
        cp.wait()
    dx_out.wait()


def solution(mesh):
    spec = P(('part', 'grp', 'loc'))

    def device_step(x_rows, dy_rows, expert_ids, gate_vals, w_gate, w_up, w_down):
        any_ = pl.BlockSpec(memory_space=pl.ANY)
        vmem = pl.BlockSpec(memory_space=pltpu.VMEM)
        dma = pltpu.SemaphoreType.DMA
        sd = jax.ShapeDtypeStruct
        out = pl.pallas_call(
            kernel,
            name='moe_backward',
            in_specs=[any_] * 4 + [vmem] + [any_] * 3,
            out_specs=[any_, vmem] + [any_] * 7,
            out_shape=[sd((TOK, D), BF16), sd((TOK, TOP_K), F32), sd((F, D), BF16), sd((F, D), BF16), sd((F, D), BF16),
                       sd((ROUNDS, SIDE, SIDE, SIDE, RS, BWD[0][1]), BF16), sd((ROUNDS, SIDE, SIDE, SIDE, RS, BWD[1][1]), BF16),
                       sd((ROUNDS, SIDE, SIDE, SIDE, RS, BWD[2][1]), BF16), sd((ROUNDS, SIDE, SIDE, SIDE, RS, D), BF16)],
            scratch_shapes=[
                pltpu.VMEM((SIDE, TOK, 2 * D), BF16),
                pltpu.VMEM((2, PLANE, SIDE, RS, 2 * D), BF16),
                pltpu.VMEM((2, ROUNDS, SIDE, SIDE, SIDE, RS, 2 * D), BF16),
                pltpu.VMEM((D, 2 * F), BF16),
                pltpu.VMEM((F, D), BF16),
                pltpu.VMEM((3 * F, D), F32),
                pltpu.VMEM((512, 3 * F), BF16),
                pltpu.VMEM((512, D), BF16),
                pltpu.VMEM((512, 2 * F), F32),
                pltpu.VMEM((PLANE * RS, TOK), BF16),
                pltpu.VMEM((3, SIDE, PLANE, TOK), F32),
                pltpu.VMEM((SIDE, 2, PLANE, TOK), F32),
                pltpu.VMEM((TOK, GROUPS), BF16),
                pltpu.VMEM((3, SIDE, TOP_K, TOK), jnp.int32),
                pltpu.VMEM((SIDE, TOP_K, TOK), F32),
                pltpu.VMEM((ROUNDS, PLANE, 1, LANES), F32),
                pltpu.VMEM((2, ROUNDS, PLANE, 1, LANES), F32),
                pltpu.VMEM((2, ROUNDS, PLANE, 1, LANES), F32),
                pltpu.VMEM((ROUNDS, PLANE, 1, LANES), F32),
                pltpu.VMEM((ROUNDS, PLANE, 1, LANES), F32),
                pltpu.VMEM((ROUNDS, SIDE, PLANE, 1, LANES), F32),
                pltpu.VMEM((GROUPS * RS, LANES), F32),
                pltpu.VMEM((TOK, LANES), F32),
                dma((4, 4)), *[dma((3, 2))] * 6, *[dma((ROUNDS, 3))] * 2, *[dma((ROUNDS,))] * 2, *[dma((ROUNDS, 2))] * 2,
                *[dma((ROUNDS,))] * 2, *[dma((ROUNDS, 2))] * 2, *[dma((ROUNDS,))] * 2, *[dma((ROUNDS, 3))] * 2,
                *[dma((ROUNDS,))] * 2, *[dma((ROUNDS, 3))] * 3, *[dma((ROUNDS,))] * 2, dma((4,)),
                pltpu.SemaphoreType.REGULAR((ROUNDS,)),
            ],
            compiler_params=pltpu.CompilerParams(collective_id=0, has_side_effects=True, vmem_limit_bytes=67043328),
        )(x_rows, dy_rows, expert_ids.T, gate_vals.T, expert_ids, w_gate[0], w_up[0], w_down[0])
        dx, d_gates, dwg_t, dwu_t, dwd = out[:5]
        return dx, d_gates, dwg_t.T[None], dwu_t.T[None], dwd[None]

    return jax.shard_map(device_step, mesh=mesh, in_specs=(spec,) * 7, out_specs=(spec,) * 5, check_vma=False)
```

```python
import jax
import jax.numpy as jnp
from jax import lax
from jax.experimental import pallas as pl
from jax.experimental.pallas import tpu as pltpu
from jax.sharding import PartitionSpec as P

MESH = pl.DeviceIdType.MESH
LANES = 128
WIDE = 256
F32 = jnp.float32
BF16 = jnp.bfloat16
SIDE = 4
PLANE = SIDE * SIDE
GROUPS = SIDE ** 3
TOK = 768
TOP_K = 8
D = 1024
F = 384
SLOTS = 48
ROUNDS = 3
RS = SLOTS // ROUNDS
NBLK = TOK // LANES
FWD = ((0, 640), (640, 640), (1280, 768))
BWD = ((0, 384), (384, 384), (768, 256))
OFFS = sorted(((a, b) for a in range(SIDE) for b in range(SIDE) if (a, b) != (0, 0)),
              key=lambda o: sum(min(v, SIDE - v) for v in o))


def dot(a, b, ca=1, cb=0):
    return lax.dot_general(a, b, (((ca,), (cb,)), ((), ())), preferred_element_type=F32)


def first(n):
    return pl.ds(0, n)


def over_lanes(v):
    return jnp.sum(v, axis=1, keepdims=True)


def over_rows(v):
    return jnp.sum(v, axis=0, keepdims=True)


scope = jax.named_scope


def iota(shape, dim):
    return lax.broadcasted_iota(jnp.int32, shape, dim)


def kernel(x_hbm, dy_hbm, idst_hbm, gatt_hbm, wg_hbm, wu_hbm, wd_hbm,
           dx_hbm, dgate_ref, dwg_hbm, dwu_hbm, dwd_hbm, ia, ib, ic, rb,
           gat, snd, rx, wgu, wdn, acc, pbuf, slots, gws, slott, idst, gatt,
           mg, mr, dgb, dgr, dgi, dgj, dgh, dgacc,
           loc_sem, meta_s, meta_r, g1_s, g1_r, g2_s, g2_r, f2_s, f2_r, mg_s, mg_r, d2_s, d2_r, dm_s, dm_r,
           c_s, c_r, dg_s, dg_r, b1_s, b1_r, b1m_s, b1m_r, bl_s, b2_s, b2_r, b2m_s, b2m_r, out_s, credit):
    g = lax.axis_index('grp')
    l = lax.axis_index('loc')
    z, y, x = g // PLANE, (g // SIDE) % SIDE, g % SIDE
    coord = (x, y, z)
    other = 1 - l

    def gid(zz, yy, xx):
        return zz * PLANE + yy * SIDE + xx

    def along(c, k):
        return gid(*(k if a == c else coord[a] for a in (2, 1, 0)))

    def in_plane(c, a, b):
        if c == 0:
            return gid(a, b, x)
        if c == 1:
            return gid(a, y, b)
        return gid(z, a, b)

    my_plane = ((z, y), (z, x), (y, x))
    my_p = tuple(a * SIDE + b for a, b in my_plane)

    def rmod(v):
        return lax.rem(v, SIDE)

    def remote(src, dst, ss, rs, grp=None, loc=None):
        return pltpu.make_async_remote_copy(src, dst, ss, rs, device_id={'grp': g if grp is None else grp, 'loc': l if loc is None else loc},
                                            device_id_type=MESH)

    def local(src, dst, sem):
        return pltpu.make_async_copy(src, dst, sem)

    barrier = pltpu.get_barrier_semaphore()
    peers = []
    for dz in range(SIDE):
        for dyy in range(SIDE):
            for dxx in range(SIDE):
                if (dz, dyy, dxx) != (0, 0, 0) and 0 in (dz, dyy, dxx):
                    peers.append(gid(rmod(z + dz), rmod(y + dyy), rmod(x + dxx)))
    for p in peers:
        pl.semaphore_signal(barrier, inc=1, device_id={'grp': p, 'loc': l}, device_id_type=MESH)
    pl.semaphore_signal(barrier, inc=1, device_id={'grp': g, 'loc': other}, device_id_type=MESH)

    def slab_copies(c, make):
        c0, w = FWD[c]
        out = []
        if c0 < D:
            n = min(w, D - c0)
            out.append(make(x_hbm.at[:, pl.ds(c0, n)], pl.ds(c0, n)))
        if c0 + w > D:
            s = max(c0, D)
            out.append(make(dy_hbm.at[:, pl.ds(s - D, c0 + w - s)], pl.ds(s, c0 + w - s)))
        return out

    def cols(c):
        return pl.ds(*FWD[c])

    for c in range(3):
        local(idst_hbm, idst.at[c, coord[c]], loc_sem.at[0, c]).start()
    local(gatt_hbm, gatt.at[x], loc_sem.at[0, 3]).start()
    for c in range(3):
        for cp in slab_copies(c, lambda src, cs: local(src, gat.at[coord[c], :, cs], loc_sem.at[1, c])):
            cp.start()
    weights = [local(wg_hbm, wgu.at[:, first(F)], loc_sem.at[2, 0]), local(wu_hbm, wgu.at[:, pl.ds(F, F)], loc_sem.at[2, 1]),
               local(wd_hbm, wdn, loc_sem.at[2, 2])]
    for cp in weights:
        cp.start()
    with scope('entry'):
        pl.semaphore_wait(barrier, len(peers) + 1)
    for c in range(3):
        for k in (1, 3, 2):
            t = along(c, rmod(coord[c] + k))
            remote(idst_hbm, idst.at[c, coord[c]], meta_s.at[c, 0], meta_r.at[c, 0], t).start()
            if c == 0:
                remote(gatt_hbm, gatt.at[x], meta_s.at[c, 1], meta_r.at[c, 1], t).start()
    for d, k in enumerate((1, 3)):
        for c in range(3):
            t = along(c, rmod(coord[c] + k))
            for cp in slab_copies(c, lambda src, cs: remote(src, gat.at[coord[c], :, cs], g1_s.at[c, d], g1_r.at[c, d], t)):
                cp.start()
    for c in range(3):
        local(idst_hbm, idst.at[c, coord[c]], loc_sem.at[0, c]).wait()
    local(gatt_hbm, gatt.at[x], loc_sem.at[0, 3]).wait()

    tri = (iota((LANES, LANES), 0) < iota((LANES, LANES), 1)).astype(BF16)

    def plane_gid(c):
        p = iota((PLANE, 1), 0)
        a, b = p // SIDE, lax.rem(p, SIDE)
        return in_plane(c, a, b)

    def make_table(c, k):
        gids = plane_gid(c)
        carry = jnp.zeros((PLANE, 1), F32)
        for blk in range(NBLK):
            ls = pl.ds(blk * LANES, LANES)
            ids = idst[c, k, :, ls]
            member = jnp.zeros((PLANE, LANES), F32)
            w0 = jnp.zeros((PLANE, LANES), F32)
            w1 = jnp.zeros((PLANE, LANES), F32)
            for j in range(TOP_K):
                idj = ids[j:j + 1, :]
                e0 = idj == 2 * gids
                e1 = idj == 2 * gids + 1
                member = jnp.where(e0 | e1, 1.0, member)
                if c == 0:
                    gj = gatt[k, pl.ds(j, 1), ls]
                    w0 = jnp.where(e0, gj, w0)
                    w1 = jnp.where(e1, gj, w1)
            rank = dot(member.astype(BF16), tri) + carry
            carry = carry + over_lanes(member)
            slots[c, k, :, ls] = jnp.where(member > 0, rank, -1.0)
            if c == 0:
                gws[k, 0, :, ls] = w0
                gws[k, 1, :, ls] = w1

    with scope('own_tables'):
        for c in range(3):
            make_table(c, coord[c])

    def home_gid():
        v = iota((GROUPS, 1), 0)
        return lax.rem(v, PLANE) * SIDE + v // PLANE

    with scope('home_table'):
        carry = jnp.zeros((GROUPS, 1), F32)
        for blk in range(NBLK):
            ls = pl.ds(blk * LANES, LANES)
            member = jnp.zeros((GROUPS, LANES), F32)
            for j in range(TOP_K):
                member = jnp.where(idst[0, x, pl.ds(j, 1), ls] // 2 == home_gid(), 1.0, member)
            rank = dot(member.astype(BF16), tri) + carry
            carry = carry + over_lanes(member)
            slott[:, ls] = jnp.where(member > 0, rank, -1.0)

    for r in range(ROUNDS):
        mg[r] = jnp.zeros((PLANE, 1, LANES), F32)

    def gather(c, k, r):
        base = (iota((RS, 1), 0) + r * RS).astype(F32)
        lane = iota((RS, LANES), 1)
        row = iota((RS, 1), 0)

        for p in range(PLANE):
            mask = slots[c, k, pl.ds(p, 1), :] == base
            pbuf[pl.ds(p * RS, RS), :] = mask.astype(F32).astype(BF16)
            if c == 0:
                line = jnp.zeros((1, LANES), F32)
                for e in range(2):
                    col = over_lanes(jnp.where(mask, gws[k, e, pl.ds(p, 1), :], 0.0))
                    line = line + over_rows(jnp.where(lane == e * 64 + k * RS + row, col, 0.0))
                mg[r, p] = mg[r, p] + line
        c0, w = FWD[c]
        rows = dot(pbuf[...], gat[k, :, pl.ds(c0, w)]).astype(BF16)
        snd[r, :, k, :, pl.ds(c0, w)] = rows.reshape(PLANE, RS, w)

    for c in range(3):
        for cp in slab_copies(c, lambda src, cs: local(src, gat.at[coord[c], :, cs], loc_sem.at[1, c])):
            cp.wait()

    def own_gather(r, carry_):
        for c in range(3):
            gather(c, coord[c], r)
        return carry_

    with scope('own_gather'):
        lax.fori_loop(0, ROUNDS, own_gather, 0)
    acc[...] = jnp.zeros_like(acc)

    for c in range(3):
        proxy = idst.at[c, first(3)]
        local(proxy, proxy, meta_r.at[c, 0]).wait()
        local(proxy, proxy, meta_s.at[c, 0]).wait()
        if c == 0:
            proxy = gatt.at[first(3)]
            local(proxy, proxy, meta_r.at[c, 1]).wait()
            local(proxy, proxy, meta_s.at[c, 1]).wait()
    for c in range(3):
        for k in (1, 3, 2):
            with scope('far_table'):
                make_table(c, rmod(coord[c] + k))

    half = TOK // 2
    for d, k in enumerate((1, 3)):
        for c in range(3):
            src = rmod(coord[c] + SIDE - k)
            block = gat.at[src, :, cols(c)]
            with scope('wait_g1'):
                local(block, block, g1_r.at[c, d]).wait()
            t = along(c, rmod(coord[c] + k))
            part = gat.at[src, pl.ds(d * half, half), cols(c)]
            remote(part, part, g2_s.at[c, d], g2_r.at[c, d], t).start()
    def next_gather(r, i):
        off = jnp.where(i == 2, 2, SIDE - 1 - 2 * i)
        for c in range(3):
            gather(c, rmod(coord[c] + off), r)

    def send_round(r):
        for a, b in OFFS:
            for c in range(3):
                pa, pb = rmod(my_plane[c][0] + a), rmod(my_plane[c][1] + b)
                src = snd.at[r, pa * SIDE + pb, :, :, cols(c)]
                dst = (rx.at[l, r, z, y, :, :, cols(c)], rx.at[l, r, z, :, x, :, cols(c)], rx.at[l, r, :, y, x, :, cols(c)])[c]
                t = in_plane(c, pa, pb)
                remote(src, dst, f2_s.at[r, c], f2_r.at[r, c], t).start()
                if c == 0:
                    remote(mg.at[r, pa * SIDE + pb], mr.at[l, r, z * SIDE + y], mg_s.at[r], mg_r.at[r], t).start()
        for c in range(3):
            own = snd[r, my_p[c], :, :, cols(c)]
            if c == 0:
                rx[l, r, z, y, :, :, cols(c)] = own
            elif c == 1:
                rx[l, r, z, :, x, :, cols(c)] = own
            else:
                rx[l, r, :, y, x, :, cols(c)] = own
        mr[l, r, z * SIDE + y] = mg[r, my_p[0]]

    def proxy15(c, table):
        c0, w = table[c]
        return snd.at[0, first(PLANE - 1), :, :, first(w)]

    def wait_send(r):
        for c in range(3):
            local(proxy15(c, FWD), proxy15(c, FWD), f2_s.at[r, c]).wait()
        m = mg.at[r, first(PLANE - 1)]
        local(m, m, mg_s.at[r]).wait()

    def early(i, carry_):
        next_gather(i // 2, lax.rem(i, 2))
        return carry_

    with scope('near_gather'):
        lax.fori_loop(0, SIDE, early, 0)
    for c in range(3):
        for d in range(2):
            src = rmod(coord[c] + 2)
            part = gat.at[src, pl.ds(d * half, half), cols(c)]
            with scope('wait_g2'):
                local(part, part, g2_r.at[c, d]).wait()

    def late(r, carry_):
        def one(i, carry2):
            next_gather(r, i)
            return carry2

        with scope('late_gather'):
            lax.fori_loop(jnp.where(r < 2, 2, 0), 3, one, 0)
        with scope('send_round'):
            send_round(r)
        return carry_

    lax.fori_loop(0, ROUNDS, late, 0)
    for c in range(3):
        for d in range(2):
            part = gat.at[0, pl.ds(d * half, half), cols(c)]
            local(part, part, g2_s.at[c, d]).wait()
    for cp in weights:
        cp.wait()

    mine = (iota((64, LANES), 1) == l * 64 + iota((64, LANES), 0))

    ubuf = gat.at[0, first(512), first(D)]
    hd = gat.at[1, first(512), first(3 * F)]

    def chunk(r, kk):
        lp = jnp.where(kk < 2, l, other)
        z0 = lax.rem(kk, 2) * 2
        zs = pl.ds(z0, 2)

        def col(c0, w):
            return rx[lp, r, zs, :, :, :, pl.ds(c0, w)].reshape(512, w)

        for h in range(2):
            hs = pl.ds(h * WIDE, WIDE)
            for m in range(4):
                line = mr[lp, r, z0 * SIDE + 4 * h + m]
                gcol = over_lanes(jnp.where(mine, line, 0.0))
                part = rx[lp, r, z0 + h, m, :, :, pl.ds(D, D)].reshape(64, D)
                gat[0, pl.ds(h * WIDE + m * 64, 64), first(D)] = (gcol * part.astype(F32)).astype(BF16)
            ab = dot(rx[lp, r, z0 + h, :, :, :, first(D)].reshape(WIDE, D), wgu[...])
            dh = dot(ubuf[hs, :], wdn[...], 1, 1)
            a = ab[:, :F]
            b = ab[:, F:]
            sig = jax.nn.sigmoid(a)
            silu = a * sig
            hd[hs, first(F)] = (silu * b).astype(BF16)
            hd[hs, pl.ds(F, F)] = (dh * b * sig * (1.0 + a * (1.0 - sig))).astype(BF16)
            hd[hs, pl.ds(2 * F, F)] = (dh * silu).astype(BF16)
        dg = jnp.zeros((512, 1), F32)
        for n in range(4):
            o = dot(hd[:, first(F)], wdn[:, pl.ds(n * WIDE, WIDE)])
            dg = dg + over_lanes(col(D + n * WIDE, WIDE).astype(F32) * o)
        for m in range(8):
            line = over_rows(jnp.where(mine, dg[m * 64:(m + 1) * 64, :], 0.0))
            dgb[kk // 2, r, z0 * SIDE + m] = line
        acc[first(F), :] += dot(hd[:, first(F)], ubuf[...], 0, 0)
        for i in (1, 2):
            acc[pl.ds(i * F, F), :] += dot(hd[:, pl.ds(i * F, F)], col(0, D), 0, 0)
        for n in range(4):
            ns = pl.ds(n * WIDE, WIDE)
            cval = dot(hd[:, pl.ds(F, 2 * F)], wgu[ns, :], 1, 1).astype(BF16)

            @pl.when(kk < 2)
            def _():
                gat[2 + kk, first(512), ns] = cval

            @pl.when(kk >= 2)
            def _():
                rx[lp, r, zs, :, :, :, ns] = cval.reshape(2, SIDE, SIDE, RS, WIDE)

    def relay(r):
        for c, buf in enumerate((ia, ib, ic)):
            local(proxy15(c, BWD), proxy15(c, BWD), b1_r.at[r, c]).wait()
            own = buf.at[r, 0, 0]
            local(own, own, bl_s.at[r, c]).wait()
        m = dgi.at[r, first(PLANE - 1)]
        local(m, m, b1m_r.at[r]).wait()
        for p in range(PLANE):
            dgj[r, pl.ds(p, 1), :] = dgi[r, p]
        for k in (1, 3, 2):
            for c, buf in enumerate((ia, ib, ic)):
                to = rmod(coord[c] + k)
                cs = pl.ds(*BWD[c])
                dst = (rb.at[r, :, :, x, :, cs], rb.at[r, :, y, :, :, cs], rb.at[r, z, :, :, :, cs])[c]
                remote(buf.at[r, :, :, to], dst, b2_s.at[r, c], b2_r.at[r, c], along(c, to)).start()
                if c == 0:
                    remote(dgj.at[r], dgh.at[r, x], b2m_s.at[r], b2m_r.at[r], along(0, to)).start()
        dgh[r, x] = dgj[r]

    def round_body(r, carry_):
        for c in range(3):
            with scope('wait_f2'):
                local(proxy15(c, FWD), proxy15(c, FWD), f2_r.at[r, c]).wait()
        m = mg.at[0, first(PLANE - 1)]
        local(m, m, mg_r.at[r]).wait()
        for h in range(2):
            blk = rx.at[l, r, pl.ds(2 * h, 2)]
            remote(blk, blk, d2_s.at[r, h], d2_r.at[r, h], loc=other).start()
        remote(mr.at[l, r], mr.at[l, r], dm_s.at[r], dm_r.at[r], loc=other).start()

        def step(kk, carry2):
            @pl.when(kk >= 2)
            def _():
                blk = rx.at[other, r, pl.ds((kk - 2) * 2, 2)]
                with scope('wait_d2'):
                    local(blk, blk, d2_r.at[r, kk - 2]).wait()

            @pl.when(kk == 2)
            def _():
                local(mr.at[other, r], mr.at[other, r], dm_r.at[r]).wait()

            with scope('chunk'):
                chunk(r, kk)

            @pl.when(kk == 1)
            def _():
                for h in range(2):
                    sent = rx.at[l, r, pl.ds(2 * h, 2)]
                    local(sent, sent, d2_s.at[r, h]).wait()
                pl.semaphore_signal(credit.at[r], inc=1, device_id={'grp': g, 'loc': other}, device_id_type=MESH)

            @pl.when(kk == 2)
            def _():
                with scope('credit'):
                    pl.semaphore_wait(credit.at[r], 1)

            @pl.when(kk >= 2)
            def _():
                zs = pl.ds((kk - 2) * 2, 2)
                remote(rx.at[other, r, zs, :, :, :, first(D)], rx.at[other, r, zs, :, :, :, pl.ds(D, D)],
                       c_s.at[r, kk - 2], c_r.at[r, kk - 2], loc=other).start()
            return carry2

        lax.fori_loop(0, 4, step, 0)
        remote(dgb.at[1, r], dgr.at[r], dg_s.at[r], dg_r.at[r], loc=other).start()
        for h in range(2):
            blk = rx.at[l, r, pl.ds(2 * h, 2), :, :, :, pl.ds(D, D)]
            with scope('wait_c'):
                local(blk, blk, c_r.at[r, h]).wait()

            def add(zy, carry2):
                zz, yy = 2 * h + zy // SIDE, lax.rem(zy, SIDE)
                p0 = gat[2 + h, pl.ds(zy * 64, 64), first(D)].astype(F32).reshape(SIDE, RS, D)
                p1 = rx[l, r, zz, yy, :, :, pl.ds(D, D)].astype(F32)
                rx[l, r, zz, yy, :, :, first(D)] = (p0 + p1).astype(BF16)
                return carry2

            with scope('add'):
                lax.fori_loop(0, 8, add, 0)
        local(dgr.at[r], dgr.at[r], dg_r.at[r]).wait()
        dgb[0, r] = dgb[0, r] + dgr[r]
        for c, buf in enumerate((ia, ib, ic)):
            cs = pl.ds(*BWD[c])
            src = (rx.at[l, r, z, y, :, :, cs], rx.at[l, r, z, :, x, :, cs], rx.at[l, r, :, y, x, :, cs])[c]
            local(src, buf.at[r, my_plane[c][0], my_plane[c][1]], bl_s.at[r, c]).start()
        for a, b in OFFS:
            for c, buf in enumerate((ia, ib, ic)):
                pa, pb = rmod(my_plane[c][0] + a), rmod(my_plane[c][1] + b)
                cs = pl.ds(*BWD[c])
                src = (rx.at[l, r, pa, pb, :, :, cs], rx.at[l, r, pa, :, pb, :, cs], rx.at[l, r, :, pa, pb, :, cs])[c]
                t = in_plane(c, pa, pb)
                remote(src, buf.at[r, my_plane[c][0], my_plane[c][1]], b1_s.at[r, c], b1_r.at[r, c], t).start()
                if c == 0:
                    remote(dgb.at[0, r, pa * SIDE + pb], dgi.at[r, my_p[0]], b1m_s.at[r], b1m_r.at[r], t).start()
        dgi[r, my_p[0]] = dgb[0, r, my_p[0]]
        return carry_

    lax.fori_loop(0, ROUNDS, round_body, 0)

    for r in range(2):
        with scope('relay'):
            relay(r)

    with scope('flush'):
        gat[1, first(F), first(D)] = acc[first(F), :].astype(BF16)
        gat[2, first(2 * F), first(D)] = acc[pl.ds(F, 2 * F), :].astype(BF16)
        outs = [local(gat.at[1, first(F), first(D)], dwd_hbm, out_s.at[0]),
                local(gat.at[2, first(F), first(D)], dwg_hbm, out_s.at[1]),
                local(gat.at[2, pl.ds(F, F), first(D)], dwu_hbm, out_s.at[2])]
        for cp in outs:
            cp.start()
        dgacc[...] = jnp.zeros_like(dgacc)
        acc[first(TOK), :] = jnp.zeros((TOK, D), F32)
        for r in range(ROUNDS):
            wait_send(r)
        slotn = slott[...].astype(BF16)
        glane = iota((GROUPS, GROUPS * RS), 1) // RS
        spread = (home_gid() == glane).astype(F32).astype(BF16)

    with scope('last_relay'):
        relay(ROUNDS - 1)

    for r in range(ROUNDS):
        with scope('pick'):
            want = (lax.rem(iota((1, GROUPS * RS), 1), RS) + r * RS).astype(F32)
            for n in range(4):
                ns = pl.ds(n * WIDE, WIDE)
                got = dot(slotn, spread[:, n * WIDE:(n + 1) * WIDE], 0, 0)
                gat[0, :, ns] = (got == want[:, n * WIDE:(n + 1) * WIDE]).astype(F32).astype(BF16)
        for c in range(3):
            own = snd.at[0, first(12), :, :, first(BWD[c][1])]
            with scope('wait_b2'):
                local(own, own, b2_r.at[r, c]).wait()
        m = dgh.at[r, first(3)]
        local(m, m, b2m_r.at[r]).wait()
        with scope('stage'):
            pieces = []
            for zy in range(PLANE):
                pieces.append(local(rb.at[r, zy // SIDE, zy % SIDE], snd.at[r, zy, :, :, first(D)], loc_sem.at[3, 0]))
            for cp in pieces:
                cp.start()
        with scope('dg'):
            for e in range(2):
                cur = dgacc[e]
                lines = jnp.zeros((GROUPS, RS), F32)
                for k in range(SIDE):
                    mine_k = dgh[r, :, :, pl.ds(e * 64 + k * RS, RS)].reshape(GROUPS, RS)
                    lines = jnp.where(x == k, mine_k, lines)
                for i in range(RS):
                    cur = jnp.where(slott[...] == float(r * RS + i), lines[:, i:i + 1], cur)
                dgacc[e] = cur
        with scope('own_pieces'):
            for cp in pieces:
                cp.wait()
            own_pieces = []
            for q in range(PLANE):
                a, b = q // SIDE, q % SIDE
                own_pieces.append(local(ia.at[r, a, b, x], snd.at[r, q, x, :, pl.ds(*BWD[0])], loc_sem.at[3, 1]))
                own_pieces.append(local(ib.at[r, a, b, y], snd.at[r, a * SIDE + y, b, :, pl.ds(*BWD[1])], loc_sem.at[3, 1]))
                own_pieces.append(local(ic.at[r, a, b, z], snd.at[r, z * SIDE + a, b, :, pl.ds(*BWD[2])], loc_sem.at[3, 1]))
            for cp in own_pieces:
                cp.start()
            for cp in own_pieces:
                cp.wait()
        with scope('combine'):
            for n in range(4):
                got = snd[r, :, :, :, pl.ds(n * WIDE, WIDE)].reshape(GROUPS * RS, WIDE)
                acc[first(TOK), pl.ds(n * WIDE, WIDE)] += dot(gat[0, :, first(D)], got)
    with scope('finish'):
        gat[3, :, first(D)] = acc[first(TOK), :].astype(BF16)
        dx_out = local(gat.at[3, :, first(D)], dx_hbm, out_s.at[3])
        dx_out.start()
        for j in range(TOP_K):
            idj = idst[0, x, pl.ds(j, 1), :]
            val = jnp.where(lax.rem(idj, 2) == 0, dgacc[0], dgacc[1])
            dgate_ref[pl.ds(j, 1), :] = over_rows(jnp.where(idj // 2 == home_gid(), val, 0.0))

    with scope('drain'):
        for c in range(3):
            for d in range(2):
                block = gat.at[0, :, cols(c)]
                local(block, block, g1_s.at[c, d]).wait()
        for r in range(ROUNDS):
            local(mr.at[0, r], mr.at[0, r], dm_s.at[r]).wait()
            local(dgr.at[r], dgr.at[r], dg_s.at[r]).wait()
            for h in range(2):
                blk = rx.at[0, r, pl.ds(2 * h, 2), :, :, :, first(D)]
                local(blk, blk, c_s.at[r, h]).wait()
            for c in range(3):
                local(proxy15(c, BWD), proxy15(c, BWD), b1_s.at[r, c]).wait()
                own = snd.at[0, first(12), :, :, first(BWD[c][1])]
                local(own, own, b2_s.at[r, c]).wait()
            m = dgi.at[r, first(PLANE - 1)]
            local(m, m, b1m_s.at[r]).wait()
            m = dgh.at[r, first(3)]
            local(m, m, b2m_s.at[r]).wait()
        for cp in outs:
            cp.wait()
        dx_out.wait()


def solution(mesh):
    spec = P(('part', 'grp', 'loc'))

    def device_step(x_rows, dy_rows, expert_ids, gate_vals, w_gate, w_up, w_down):
        any_ = pl.BlockSpec(memory_space=pl.ANY)
        vmem = pl.BlockSpec(memory_space=pltpu.VMEM)
        dma = pltpu.SemaphoreType.DMA
        sd = jax.ShapeDtypeStruct
        out = pl.pallas_call(
            kernel,
            name='moe_backward',
            in_specs=[any_] * 7,
            out_specs=[any_, vmem] + [any_] * 7,
            out_shape=[sd((TOK, D), BF16), sd((TOP_K, TOK), F32), sd((F, D), BF16), sd((F, D), BF16), sd((F, D), BF16),
                       sd((ROUNDS, SIDE, SIDE, SIDE, RS, BWD[0][1]), BF16), sd((ROUNDS, SIDE, SIDE, SIDE, RS, BWD[1][1]), BF16),
                       sd((ROUNDS, SIDE, SIDE, SIDE, RS, BWD[2][1]), BF16), sd((ROUNDS, SIDE, SIDE, SIDE, RS, D), BF16)],
            scratch_shapes=[
                pltpu.VMEM((SIDE, TOK, 2 * D), BF16),
                pltpu.VMEM((ROUNDS, PLANE, SIDE, RS, 2 * D), BF16),
                pltpu.VMEM((2, ROUNDS, SIDE, SIDE, SIDE, RS, 2 * D), BF16),
                pltpu.VMEM((D, 2 * F), BF16),
                pltpu.VMEM((F, D), BF16),
                pltpu.VMEM((3 * F, D), F32),
                pltpu.VMEM((PLANE * RS, TOK), BF16),
                pltpu.VMEM((3, SIDE, PLANE, TOK), F32),
                pltpu.VMEM((SIDE, 2, PLANE, TOK), F32),
                pltpu.VMEM((GROUPS, TOK), F32),
                pltpu.VMEM((3, SIDE, TOP_K, TOK), jnp.int32),
                pltpu.VMEM((SIDE, TOP_K, TOK), F32),
                pltpu.VMEM((ROUNDS, PLANE, 1, LANES), F32),
                pltpu.VMEM((2, ROUNDS, PLANE, 1, LANES), F32),
                pltpu.VMEM((2, ROUNDS, PLANE, 1, LANES), F32),
                pltpu.VMEM((ROUNDS, PLANE, 1, LANES), F32),
                pltpu.VMEM((ROUNDS, PLANE, 1, LANES), F32),
                pltpu.VMEM((ROUNDS, PLANE, LANES), F32),
                pltpu.VMEM((ROUNDS, SIDE, PLANE, LANES), F32),
                pltpu.VMEM((2, GROUPS, TOK), F32),
                dma((4, 4)), *[dma((3, 2))] * 6, *[dma((ROUNDS, 3))] * 2, *[dma((ROUNDS,))] * 2, *[dma((ROUNDS, 2))] * 2,
                *[dma((ROUNDS,))] * 2, *[dma((ROUNDS, 2))] * 2, *[dma((ROUNDS,))] * 2, *[dma((ROUNDS, 3))] * 2,
                *[dma((ROUNDS,))] * 2, *[dma((ROUNDS, 3))] * 3, *[dma((ROUNDS,))] * 2, dma((4,)),
                pltpu.SemaphoreType.REGULAR((ROUNDS,)),
            ],
            compiler_params=pltpu.CompilerParams(collective_id=0, has_side_effects=True, vmem_limit_bytes=67043328),
        )(x_rows, dy_rows, expert_ids.T, gate_vals.T, w_gate[0], w_up[0], w_down[0])
        dx, d_gates, dwg_t, dwu_t, dwd = out[:5]
        return dx, d_gates.T, dwg_t.T[None], dwu_t.T[None], dwd[None]

    return jax.shard_map(device_step, mesh=mesh, in_specs=(spec,) * 7, out_specs=(spec,) * 5, check_vma=False)
```

```python
import jax
import jax.numpy as jnp
from jax import lax
from jax.experimental import pallas as pl
from jax.experimental.pallas import tpu as pltpu
from jax.sharding import PartitionSpec as P

MESH = pl.DeviceIdType.MESH
F32 = jnp.float32
BF16 = jnp.bfloat16
LANES = 128
WIDE = 256
SIDE = 4
PLANE = SIDE * SIDE
GROUPS = SIDE ** 3
TOK = 768
HALF = TOK // 2
TOP_K = 8
D = 1024
F = 384
SLOTS = 48
ROUNDS = 3
RS = SLOTS // ROUNDS
LINE = SIDE * RS
CH = 2 * PLANE * RS
NBLK = TOK // LANES
FWD = ((0, 640), (640, 640), (1280, 768))
BWD = ((0, 384), (384, 384), (768, 256))
AXES = ((1, 2), (2, 0), (0, 1))
NEAR = (1, 3, 2)
scope = jax.named_scope


def dot(a, b, ca=1, cb=0):
    return lax.dot_general(a, b, (((ca,), (cb,)), ((), ())), preferred_element_type=F32)


def first(n):
    return pl.ds(0, n)


def over_lanes(v):
    return jnp.sum(v, axis=1, keepdims=True)


def over_rows(v):
    return jnp.sum(v, axis=0, keepdims=True)


def iota(shape, dim):
    return lax.broadcasted_iota(jnp.int32, shape, dim)


def onehot(mask):
    return mask.astype(F32).astype(BF16)


def kernel(x_hbm, dy_hbm, idst_hbm, gatt_hbm, wg_hbm, wu_hbm, wd_hbm,
           dx_hbm, dgate_ref, dwg_hbm, dwu_hbm, dwd_hbm, ja, jb, jc, ia, ib, ic,
           gat, snd, rx, wgu, wdn, acc, hd, pbuf, slott, idst, gatt, mg, jm, mr, dgb, dgr, km, dgi, dgj, dgh, dgacc,
           loc_sem, out_sem, meta_s, meta_r, g1_s, g1_r, g2_s, g2_r, fa_s, fa_r, fb_s, fb_r, fl, fm_s, fm_r,
           d2_s, d2_r, c_s, c_r, dm_s, dm_r, ba_s, ba_r, bb_s, bb_r, bc_s, bc_r, bl, bm_s, bm_r, credit, free):
    g = lax.axis_index('grp')
    l = lax.axis_index('loc')
    z, y, x = g // PLANE, (g // SIDE) % SIDE, g % SIDE
    coord = (x, y, z)
    other = 1 - l

    def rmod(v):
        return lax.rem(v, SIDE)

    def gid(zz, yy, xx):
        return zz * PLANE + yy * SIDE + xx

    def along(axis, k):
        return gid(*(k if a == axis else coord[a] for a in (2, 1, 0)))

    def in_plane(c, a, b):
        at = {c: coord[c], AXES[c][0]: a, AXES[c][1]: b}
        return gid(at[2], at[1], at[0])

    def remote(src, dst, ss, rs, grp=g, loc=l):
        return pltpu.make_async_remote_copy(src, dst, ss, rs, device_id={'grp': grp, 'loc': loc}, device_id_type=MESH)

    def local(src, dst, sem):
        return pltpu.make_async_copy(src, dst, sem)

    def wait(ref, sem):
        local(ref, ref, sem).wait()

    neighbours = [along(axis, rmod(coord[axis] + k)) for axis in range(3) for k in NEAR]

    barrier = pltpu.get_barrier_semaphore()
    for p in neighbours:
        pl.semaphore_signal(barrier, inc=1, device_id={'grp': p, 'loc': l}, device_id_type=MESH)
    pl.semaphore_signal(barrier, inc=1, device_id={'grp': g, 'loc': other}, device_id_type=MESH)

    def slab_copies(c, rows, make):
        c0, w = FWD[c]
        out = []
        if c0 < D:
            n = min(w, D - c0)
            out.append(make(x_hbm.at[rows, pl.ds(c0, n)], pl.ds(c0, n)))
        if c0 + w > D:
            s = max(c0, D)
            out.append(make(dy_hbm.at[rows, pl.ds(s - D, c0 + w - s)], pl.ds(s, c0 + w - s)))
        return out

    def cols(c):
        return pl.ds(*FWD[c])

    def own_slab(c):
        return slab_copies(c, first(TOK), lambda src, cs: local(src, gat.at[coord[c], :, cs], loc_sem.at[1, c]))

    routing = [local(idst_hbm, idst.at[c, coord[c]], loc_sem.at[0, c]) for c in range(3)]
    routing.append(local(gatt_hbm, gatt.at[x], loc_sem.at[0, 3]))
    weights = [local(wg_hbm, wgu.at[:, first(F)], loc_sem.at[2, 0]), local(wu_hbm, wgu.at[:, pl.ds(F, F)], loc_sem.at[2, 1]),
               local(wd_hbm, wdn, loc_sem.at[2, 2])]
    for cp in routing + own_slab(0) + own_slab(1) + own_slab(2) + weights:
        cp.start()
    with scope('entry'):
        pl.semaphore_wait(barrier, len(neighbours) + 1)

    for c in range(3):
        for k in NEAR:
            t = along(c, rmod(coord[c] + k))
            remote(idst_hbm, idst.at[c, coord[c]], meta_s.at[c, 0], meta_r.at[c, 0], t).start()
            if c == 0:
                remote(gatt_hbm, gatt.at[x], meta_s.at[c, 1], meta_r.at[c, 1], t).start()
    for i in range(2):
        for d, k in enumerate((1, 3)):
            h = (d + i) % 2
            rows = pl.ds(h * HALF, HALF)
            for c in range(3):
                t = along(c, rmod(coord[c] + k))
                for cp in slab_copies(c, rows, lambda src, cs: remote(src, gat.at[coord[c], rows, cs], g1_s.at[c, d, h],
                                                                      g1_r.at[c, d, h], t)):
                    cp.start()
    for cp in routing:
        cp.wait()

    tri = onehot(iota((LANES, LANES), 0) < iota((LANES, LANES), 1))
    tables = 3 * SIDE * PLANE

    def table(c, k, p):
        return acc.at[pl.ds((c * SIDE + k) * PLANE + p, 1), first(TOK)]

    def gates(k, e, p):
        return acc.at[pl.ds(tables + (k * 2 + e) * PLANE + p, 1), first(TOK)]

    def make_table(c, k):
        p = iota((PLANE, 1), 0)
        gids = in_plane(c, p // SIDE, rmod(p))
        carry = jnp.zeros((PLANE, 1), F32)
        for blk in range(NBLK):
            ls = pl.ds(blk * LANES, LANES)
            ids = idst[c, k, :, ls]
            member = jnp.zeros((PLANE, LANES), F32)
            w0 = jnp.zeros((PLANE, LANES), F32)
            w1 = jnp.zeros((PLANE, LANES), F32)
            for j in range(TOP_K):
                idj = ids[j:j + 1, :]
                e0 = idj == 2 * gids
                e1 = idj == 2 * gids + 1
                member = jnp.where(e0 | e1, 1.0, member)
                if c == 0:
                    gj = gatt[k, pl.ds(j, 1), ls]
                    w0 = jnp.where(e0, gj, w0)
                    w1 = jnp.where(e1, gj, w1)
            rank = dot(member.astype(BF16), tri) + carry
            carry = carry + over_lanes(member)
            acc[pl.ds((c * SIDE + k) * PLANE, PLANE), ls] = jnp.where(member > 0, rank, -1.0)
            if c == 0:
                acc[pl.ds(tables + k * 2 * PLANE, PLANE), ls] = w0
                acc[pl.ds(tables + (k * 2 + 1) * PLANE, PLANE), ls] = w1

    with scope('own_tables'):
        for c in range(3):
            make_table(c, coord[c])

    def home_gid():
        v = iota((GROUPS, 1), 0)
        return lax.rem(v, PLANE) * SIDE + v // PLANE

    with scope('home_table'):
        carry = jnp.zeros((GROUPS, 1), F32)
        for blk in range(NBLK):
            ls = pl.ds(blk * LANES, LANES)
            member = jnp.zeros((GROUPS, LANES), F32)
            for j in range(TOP_K):
                member = jnp.where(idst[0, x, pl.ds(j, 1), ls] // 2 == home_gid(), 1.0, member)
            rank = dot(member.astype(BF16), tri) + carry
            carry = carry + over_lanes(member)
            slott[:, ls] = jnp.where(member > 0, rank, -1.0)

    for r in range(ROUNDS):
        mg[r] = jnp.zeros((SIDE, SIDE, 1, LANES), F32)

    def gather(c, k, r):
        base = (iota((RS, 1), 0) + r * RS).astype(F32)
        lane = iota((RS, LANES), 1)
        row = iota((RS, 1), 0)
        for p in range(PLANE):
            mask = table(c, k, p)[...] == base
            pbuf[pl.ds(p * RS, RS), :] = onehot(mask)
            if c == 0:
                line = jnp.zeros((1, LANES), F32)
                for e in range(2):
                    col = over_lanes(jnp.where(mask, gates(k, e, p)[...], 0.0))
                    line = line + over_rows(jnp.where(lane == e * LINE + k * RS + row, col, 0.0))
                mg[r, p // SIDE, p % SIDE] = mg[r, p // SIDE, p % SIDE] + line
        rows = dot(pbuf[...], gat[k, :, cols(c)]).astype(BF16).reshape(SIDE, SIDE, RS, FWD[c][1])
        if c == 2:
            snd[r, :, k, :, :, cols(c)] = rows
        else:
            snd[r, :, :, k, :, cols(c)] = rows

    for c in range(3):
        for cp in own_slab(c):
            cp.wait()

    def own_gather(r, carry_):
        for c in range(3):
            gather(c, coord[c], r)
        return carry_

    with scope('own_gather'):
        lax.fori_loop(0, ROUNDS, own_gather, 0)

    for c in range(3):
        wait(idst.at[c, first(3)], meta_r.at[c, 0])
        wait(idst.at[c, first(3)], meta_s.at[c, 0])
    wait(gatt.at[first(3)], meta_r.at[0, 1])
    wait(gatt.at[first(3)], meta_s.at[0, 1])
    with scope('far_table'):
        for c in range(3):
            for k in NEAR:
                make_table(c, rmod(coord[c] + k))

    def part(c, k, h):
        return gat.at[k, pl.ds(h * HALF, HALF), cols(c)]

    for d, k in enumerate((1, 3)):
        for c in range(3):
            src = rmod(coord[c] + SIDE - k)
            with scope('wait_g1'):
                wait(part(c, src, d), g1_r.at[c, d, d])
            remote(part(c, src, d), part(c, src, d), g2_s.at[c, d], g2_r.at[c, d], along(c, rmod(coord[c] + k))).start()
    for d, k in enumerate((1, 3)):
        for c in range(3):
            with scope('wait_g1b'):
                wait(part(c, rmod(coord[c] + SIDE - k), 1 - d), g1_r.at[c, d, 1 - d])

    def next_gather(r, i):
        off = jnp.where(i == 2, 2, SIDE - 1 - 2 * i)
        for c in range(3):
            gather(c, rmod(coord[c] + off), r)

    def early(i, carry_):
        next_gather(i // 2, lax.rem(i, 2))
        return carry_

    with scope('near_gather'):
        lax.fori_loop(0, SIDE, early, 0)
    for c in range(3):
        for d in range(2):
            with scope('wait_g2'):
                wait(part(c, rmod(coord[c] + 2), d), g2_r.at[c, d])

    def plane_hop(r):
        for c, buf in enumerate((ja, jb, jc)):
            axis = AXES[c][0]
            dst = buf.at[r, :, coord[axis], :, :, :] if c == 2 else buf.at[r, coord[axis]]
            for k in NEAR:
                to = rmod(coord[axis] + k)
                remote(snd.at[r, to, :, :, :, cols(c)], dst, fa_s.at[r, c], fa_r.at[r, c], along(axis, to)).start()
                if c == 0:
                    remote(mg.at[r, to], jm.at[r, y], fm_s.at[0, r], fm_r.at[0, r], along(axis, to)).start()
            local(snd.at[r, coord[axis], :, :, :, cols(c)], dst, fl.at[0, r, c]).start()
        jm[r, y] = mg[r, y]

    def blocks(n, w):
        return snd.at[0, first(n), :, :, :, first(w)]

    def pass_on(r):
        for c, buf in enumerate((ja, jb, jc)):
            axis = AXES[c][1]
            w = FWD[c][1]
            with scope('wait_fa'):
                wait(blocks(3, w), fa_r.at[r, c])
            wait(blocks(1, w), fl.at[0, r, c])
            dst = (rx.at[l, r, z, :, :, :, cols(c)], rx.at[l, r, :, :, x, :, cols(c)], rx.at[l, r, :, y, :, :, cols(c)])[c]
            if c == 0:
                wait(mg.at[0, first(3)], fm_r.at[0, r])
            for k in (*NEAR, 0):
                to = rmod(coord[axis] + k)
                src = buf.at[r, :, :, to] if c == 2 else buf.at[r, :, to]
                if k:
                    remote(src, dst, fb_s.at[r, c], fb_r.at[r, c], along(axis, to)).start()
                    if c == 0:
                        remote(jm.at[r, :, to], mr.at[l, r, z], fm_s.at[1, r], fm_r.at[1, r], along(axis, to)).start()
                else:
                    local(src, dst, fl.at[1, r, c]).start()
        mr[l, r, z] = jm[r, :, z]
        for c in range(3):
            wait(blocks(3, FWD[c][1]), fa_s.at[r, c])
        wait(mg.at[0, first(3)], fm_s.at[0, r])
        for p in neighbours:
            pl.semaphore_signal(free.at[r], inc=1, device_id={'grp': p, 'loc': l}, device_id_type=MESH)

    def late(r, carry_):
        def one(i, carry2):
            next_gather(r, i)
            return carry2

        with scope('late_gather'):
            lax.fori_loop(jnp.where(r < 2, 2, 0), 3, one, 0)

        @pl.when(r < 2)
        def _():
            plane_hop(r)
        return carry_

    lax.fori_loop(0, ROUNDS, late, 0)
    with scope('pass_on'):
        pass_on(0)
    plane_hop(2)
    with scope('pass_on'):
        pass_on(1)
    for c in range(3):
        for d in range(2):
            wait(part(c, 0, d), g2_s.at[c, d])
            for h in range(2):
                wait(part(c, 0, d), g1_s.at[c, d, h])
    acc[...] = jnp.zeros_like(acc)
    for cp in weights:
        cp.wait()

    mine = (iota((LINE, LANES), 1) == l * LINE + iota((LINE, LANES), 0))
    ubuf = gat.at[0, first(CH), pl.ds(D, D)]

    def result(kk, n=first(D)):
        return gat.at[kk, first(CH), n]

    def chunk(r, kk):
        who, half = kk // 2, lax.rem(kk, 2)
        lp = jnp.where(who == 0, l, other)
        z0 = half * 2
        zs = pl.ds(z0, 2)

        def col(c0, w):
            return rx[lp, r, zs, :, :, :, pl.ds(c0, w)].reshape(CH, w)

        for m in range(2 * SIDE):
            zz, yy = z0 + m // SIDE, m % SIDE
            gcol = over_lanes(jnp.where(mine, mr[lp, r, zz, yy], 0.0))
            rows = rx[lp, r, zz, yy, :, :, pl.ds(D, D)].reshape(LINE, D)
            ubuf[pl.ds(m * LINE, LINE), :] = (gcol * rows.astype(F32)).astype(BF16)
        for h in range(2):
            hs = pl.ds(h * WIDE, WIDE)
            ab = dot(rx[lp, r, z0 + h, :, :, :, first(D)].reshape(WIDE, D), wgu[...])
            dh = dot(ubuf[hs, :], wdn[...], 1, 1)
            a = ab[:, :F]
            b = ab[:, F:]
            sig = jax.nn.sigmoid(a)
            silu = a * sig
            hd[hs, first(F)] = (silu * b).astype(BF16)
            hd[hs, pl.ds(F, F)] = (dh * b * sig * (1.0 + a * (1.0 - sig))).astype(BF16)
            hd[hs, pl.ds(2 * F, F)] = (dh * silu).astype(BF16)
        dg = jnp.zeros((CH, 1), F32)
        for n in range(4):
            o = dot(hd[:, first(F)], wdn[:, pl.ds(n * WIDE, WIDE)])
            dg = dg + over_lanes(col(D + n * WIDE, WIDE).astype(F32) * o)
        for m in range(2 * SIDE):
            line = over_rows(jnp.where(mine, dg[m * LINE:(m + 1) * LINE, :], 0.0))
            dgb[who, r, z0 + m // SIDE, m % SIDE] = line
        acc[first(F), :] += dot(hd[:, first(F)], ubuf[...], 0, 0)
        for i in (1, 2):
            acc[pl.ds(i * F, F), :] += dot(hd[:, pl.ds(i * F, F)], col(0, D), 0, 0)
        for n in range(4):
            cval = dot(hd[:, pl.ds(F, 2 * F)], wgu[pl.ds(n * WIDE, WIDE), :], 1, 1)
            result(kk, pl.ds(n * WIDE, WIDE))[...] = cval.astype(BF16)

    def home_first(r):
        pl.semaphore_wait(free.at[r], len(neighbours))
        for c in range(3):
            axis = AXES[c][1]
            cs = pl.ds(*BWD[c])
            dst = snd.at[r, coord[axis], :, :, :, pl.ds(D + BWD[c][0], BWD[c][1])]
            for k in (*NEAR, 0):
                to = rmod(coord[axis] + k)
                src = (rx.at[l, r, to, :, :, :, cs], rx.at[l, r, :, :, to, :, cs], rx.at[l, r, :, to, :, :, cs])[c]
                if k:
                    remote(src, dst, ba_s.at[r, c], ba_r.at[r, c], along(axis, to)).start()
                    if c == 0:
                        remote(dgb.at[0, r, to], km.at[r, z], bm_s.at[0, r], bm_r.at[0, r], along(axis, to)).start()
                else:
                    dst[...] = src[...]
        km[r, z] = dgb[0, r, z]

    def home_second(r):
        for c, buf in enumerate((ia, ib, ic)):
            axis = AXES[c][0]
            with scope('wait_ba'):
                wait(blocks(3, BWD[c][1]), ba_r.at[r, c])
            if c == 0:
                wait(mg.at[0, first(3)], bm_r.at[0, r])
            dst = buf.at[r, coord[axis]] if c == 1 else buf.at[r, :, coord[axis]]
            cs = pl.ds(D + BWD[c][0], BWD[c][1])
            for k in (*NEAR, 0):
                to = rmod(coord[axis] + k)
                src = snd.at[r, :, :, to, :, cs] if c == 2 else snd.at[r, :, to, :, :, cs]
                if k:
                    remote(src, dst, bb_s.at[r, c], bb_r.at[r, c], along(axis, to)).start()
                    if c == 0:
                        remote(km.at[r, :, to], dgi.at[r, :, y], bm_s.at[1, r], bm_r.at[1, r], along(axis, to)).start()
                else:
                    local(src, dst, bl.at[0, r, c]).start()
        dgi[r, :, y] = km[r, :, y]

    def home_third(r):
        for c, buf in enumerate((ia, ib, ic)):
            with scope('wait_bb'):
                wait(blocks(3, BWD[c][1]), bb_r.at[r, c])
            wait(blocks(1, BWD[c][1]), bl.at[0, r, c])
            if c == 0:
                wait(mg.at[0, first(3)], bm_r.at[1, r])
                for p in range(PLANE):
                    dgj[r, pl.ds(p, 1), :] = dgi[r, p // SIDE, p % SIDE]
            cs = pl.ds(*BWD[c])
            dst = (snd.at[r, :, :, x, :, cs], snd.at[r, :, y, :, :, cs], snd.at[r, z, :, :, :, cs])[c]
            for k in (*NEAR, 0):
                to = rmod(coord[c] + k)
                src = buf.at[r, :, :, to]
                if k:
                    remote(src, dst, bc_s.at[r, c], bc_r.at[r, c], along(c, to)).start()
                    if c == 0:
                        remote(dgj.at[r], dgh.at[r, x], bm_s.at[2, r], bm_r.at[2, r], along(c, to)).start()
                else:
                    local(src, dst, bl.at[1, r, c]).start()
        dgh[r, x] = dgj[r]

    hooks = (((0, 3), 'pass_on2', lambda: pass_on(2)), ((2, 0), 'home_second0', lambda: home_second(0)),
             ((2, 2), 'home_second1', lambda: home_second(1)), ((2, 3), 'home_third0', lambda: home_third(0)))

    def round_body(r, carry_):
        for c in range(3):
            with scope('wait_fb'):
                wait(blocks(3, FWD[c][1]), fb_r.at[r, c])
            wait(blocks(1, FWD[c][1]), fl.at[1, r, c])
        wait(mg.at[0, first(3)], fm_r.at[1, r])
        for h in range(2):
            blk = rx.at[l, r, pl.ds(2 * h, 2)]
            remote(blk, blk, d2_s.at[r, h], d2_r.at[r, h], loc=other).start()
        remote(mr.at[l, r], mr.at[l, r], dm_s.at[0, r], dm_r.at[0, r], loc=other).start()

        def step(kk, carry2):
            half = lax.rem(kk, 2)
            zs = pl.ds(half * 2, 2)

            @pl.when(kk >= 2)
            def _():
                with scope('wait_d2'):
                    wait(rx.at[other, r, zs], d2_r.at[r, half])

            @pl.when(kk == 2)
            def _():
                wait(mr.at[other, r], dm_r.at[0, r])

            with scope('chunk'):
                chunk(r, kk)

            @pl.when(kk == 1)
            def _():
                for h in range(2):
                    wait(rx.at[l, r, pl.ds(2 * h, 2)], d2_s.at[r, h])
                pl.semaphore_signal(credit.at[r], inc=1, device_id={'grp': g, 'loc': other}, device_id_type=MESH)

            for (rr, at), name, hook in hooks:
                @pl.when((r == rr) & (kk == at))
                def _():
                    with scope(name):
                        hook()

            @pl.when(kk == 2)
            def _():
                with scope('credit'):
                    pl.semaphore_wait(credit.at[r], 1)

            @pl.when(kk >= 2)
            def _():
                rx[other, r, zs, :, :, :, first(D)] = result(kk)[...].reshape(2, SIDE, SIDE, RS, D)
                remote(rx.at[other, r, zs, :, :, :, first(D)], rx.at[other, r, zs, :, :, :, pl.ds(D, D)],
                       c_s.at[r, half], c_r.at[r, half], loc=other).start()
            return carry2

        lax.fori_loop(0, 4, step, 0)
        remote(dgb.at[1, r], dgr.at[r], dm_s.at[1, r], dm_r.at[1, r], loc=other).start()
        for h in range(2):
            with scope('wait_c'):
                wait(rx.at[l, r, pl.ds(2 * h, 2), :, :, :, pl.ds(D, D)], c_r.at[r, h])

            def add(zy, carry2):
                zz, yy = 2 * h + zy // SIDE, lax.rem(zy, SIDE)
                p0 = gat[h, pl.ds(zy * LINE, LINE), first(D)].astype(F32).reshape(SIDE, RS, D)
                p1 = rx[l, r, zz, yy, :, :, pl.ds(D, D)].astype(F32)
                rx[l, r, zz, yy, :, :, first(D)] = (p0 + p1).astype(BF16)
                return carry2

            with scope('add'):
                lax.fori_loop(0, 2 * SIDE, add, 0)
        wait(dgr.at[r], dm_r.at[1, r])
        dgb[0, r] = dgb[0, r] + dgr[r]
        with scope('home_first'):
            home_first(r)
        return carry_

    lax.fori_loop(0, ROUNDS, round_body, 0)

    with scope('flush'):
        gat[1, first(F), first(D)] = acc[first(F), :].astype(BF16)
        gat[2, first(2 * F), first(D)] = acc[pl.ds(F, 2 * F), :].astype(BF16)
        outs = [local(gat.at[1, first(F), first(D)], dwd_hbm, out_sem.at[0]),
                local(gat.at[2, first(F), first(D)], dwg_hbm, out_sem.at[1]),
                local(gat.at[2, pl.ds(F, F), first(D)], dwu_hbm, out_sem.at[2])]
        for cp in outs:
            cp.start()
        dgacc[...] = jnp.zeros_like(dgacc)
        acc[first(TOK), :] = jnp.zeros((TOK, D), F32)
        slotn = slott[...].astype(BF16)
        glane = iota((GROUPS, GROUPS * RS), 1) // RS
        spread = onehot(home_gid() == glane)
    with scope('home_third1'):
        home_third(1)
    with scope('home_second'):
        home_second(2)

    def combine(r):
        with scope('pick'):
            want = (lax.rem(iota((1, GROUPS * RS), 1), RS) + r * RS).astype(F32)
            for n in range(4):
                ns = pl.ds(n * WIDE, WIDE)
                got = dot(slotn, spread[:, n * WIDE:(n + 1) * WIDE], 0, 0)
                gat[0, :, ns] = onehot(got == want[:, n * WIDE:(n + 1) * WIDE])
        wait(dgh.at[r, first(3)], bm_r.at[2, r])
        with scope('dg'):
            for e in range(2):
                cur = dgacc[e]
                lines = jnp.zeros((GROUPS, RS), F32)
                for k in range(SIDE):
                    mine_k = dgh[r, :, :, pl.ds(e * LINE + k * RS, RS)].reshape(GROUPS, RS)
                    lines = jnp.where(x == k, mine_k, lines)
                for i in range(RS):
                    cur = jnp.where(slott[...] == float(r * RS + i), lines[:, i:i + 1], cur)
                dgacc[e] = cur
        for c in range(3):
            with scope('wait_bc'):
                wait(blocks(3, BWD[c][1]), bc_r.at[r, c])
            wait(blocks(1, BWD[c][1]), bl.at[1, r, c])
        with scope('combine'):
            for n in range(4):
                ns = pl.ds(n * WIDE, WIDE)
                acc[first(TOK), ns] += dot(gat[0, :, first(D)], snd[r, :, :, :, :, ns].reshape(GROUPS * RS, WIDE))

    combine(0)
    with scope('home_third2'):
        home_third(2)
    combine(1)
    combine(2)
    with scope('finish'):
        gat[3, :, first(D)] = acc[first(TOK), :].astype(BF16)
        dx_out = local(gat.at[3, :, first(D)], dx_hbm, out_sem.at[3])
        dx_out.start()
        for j in range(TOP_K):
            idj = idst[0, x, pl.ds(j, 1), :]
            val = jnp.where(lax.rem(idj, 2) == 0, dgacc[0], dgacc[1])
            dgate_ref[pl.ds(j, 1), :] = over_rows(jnp.where(idj // 2 == home_gid(), val, 0.0))

    with scope('drain'):
        for r in range(ROUNDS):
            for i in range(3):
                wait(dgh.at[0, first(3)] if i == 2 else mg.at[0, first(3)], bm_s.at[i, r])
            wait(mg.at[0, first(3)], fm_s.at[1, r])
            for i in range(2):
                wait(dgr.at[r], dm_s.at[i, r])
                wait(rx.at[0, r, first(2), :, :, :, first(D)], c_s.at[r, i])
            for c in range(3):
                wait(blocks(3, FWD[c][1]), fb_s.at[r, c])
                for sem in (ba_s, bb_s, bc_s):
                    wait(blocks(3, BWD[c][1]), sem.at[r, c])
        for cp in outs:
            cp.wait()
        dx_out.wait()


def solution(mesh):
    spec = P(('part', 'grp', 'loc'))

    def device_step(x_rows, dy_rows, expert_ids, gate_vals, w_gate, w_up, w_down):
        any_ = pl.BlockSpec(memory_space=pl.ANY)
        vmem = pl.BlockSpec(memory_space=pltpu.VMEM)
        dma = pltpu.SemaphoreType.DMA
        sd = jax.ShapeDtypeStruct
        cube = (ROUNDS, SIDE, SIDE, SIDE, RS)
        lines = (ROUNDS, SIDE, SIDE, 1, LANES)
        weight = sd((F, D), BF16)
        out = pl.pallas_call(
            kernel,
            name='moe_backward',
            in_specs=[any_] * 7,
            out_specs=[any_, vmem] + [any_] * 9,
            out_shape=[sd((TOK, D), BF16), sd((TOP_K, TOK), F32), weight, weight, weight,
                       *[sd((*cube, w), BF16) for _, w in FWD + BWD]],
            scratch_shapes=[
                pltpu.VMEM((SIDE, TOK, 2 * D), BF16),
                pltpu.VMEM((*cube, 2 * D), BF16),
                pltpu.VMEM((2, *cube, 2 * D), BF16),
                pltpu.VMEM((D, 2 * F), BF16),
                pltpu.VMEM((F, D), BF16),
                pltpu.VMEM((3 * F, D), F32),
                pltpu.VMEM((CH, 3 * F), BF16),
                pltpu.VMEM((PLANE * RS, TOK), BF16),
                pltpu.VMEM((GROUPS, TOK), F32),
                pltpu.VMEM((3, SIDE, TOP_K, TOK), jnp.int32),
                pltpu.VMEM((SIDE, TOP_K, TOK), F32),
                pltpu.VMEM(lines, F32),
                pltpu.VMEM(lines, F32),
                pltpu.VMEM((2, *lines), F32),
                pltpu.VMEM((2, *lines), F32),
                pltpu.VMEM(lines, F32),
                pltpu.VMEM(lines, F32),
                pltpu.VMEM(lines, F32),
                pltpu.VMEM((ROUNDS, PLANE, LANES), F32),
                pltpu.VMEM((ROUNDS, SIDE, PLANE, LANES), F32),
                pltpu.VMEM((2, GROUPS, TOK), F32),
                dma((3, 4)), dma((4,)), *[dma((3, 2))] * 2, *[dma((3, 2, 2))] * 2, *[dma((3, 2))] * 2,
                *[dma((ROUNDS, 3))] * 4, dma((2, ROUNDS, 3)), *[dma((2, ROUNDS))] * 2,
                *[dma((ROUNDS, 2))] * 4, *[dma((2, ROUNDS))] * 2, *[dma((ROUNDS, 3))] * 6, dma((2, ROUNDS, 3)),
                *[dma((3, ROUNDS))] * 2, *[pltpu.SemaphoreType.REGULAR((ROUNDS,))] * 2,
            ],
            compiler_params=pltpu.CompilerParams(collective_id=0, has_side_effects=True, vmem_limit_bytes=67043328),
        )(x_rows, dy_rows, expert_ids.T, gate_vals.T, w_gate[0], w_up[0], w_down[0])
        dx, d_gates, dwg_t, dwu_t, dwd = out[:5]
        return dx, d_gates.T, dwg_t.T[None], dwu_t.T[None], dwd[None]

    return jax.shard_map(device_step, mesh=mesh, in_specs=(spec,) * 7, out_specs=(spec,) * 5, check_vma=False)
```

```python
import jax
import jax.numpy as jnp
from jax import lax
from jax.experimental import pallas as pl
from jax.experimental.pallas import tpu as pltpu
from jax.sharding import PartitionSpec as P

MESH = pl.DeviceIdType.MESH
F32 = jnp.float32
BF16 = jnp.bfloat16
LANES = 128
WIDE = 256
SIDE = 4
PLANE = SIDE * SIDE
GROUPS = SIDE ** 3
TOK = 768
HALF = TOK // 2
TOP_K = 8
D = 1024
F = 384
SLOTS = 48
ROUNDS = 6
PAIRS = ROUNDS // 2
RS = SLOTS // ROUNDS
GS = 2 * RS
LINE = SIDE * RS
CH = GROUPS * RS
NBLK = TOK // LANES
FWD = ((0, 640), (640, 640), (1280, 768))
BWD = ((0, 384), (384, 384), (768, 256))
AXES = ((1, 2), (2, 0), (0, 1))
NEAR = (1, 3, 2)
scope = jax.named_scope


def dot(a, b, ca=1, cb=0):
    return lax.dot_general(a, b, (((ca,), (cb,)), ((), ())), preferred_element_type=F32)


def first(n):
    return pl.ds(0, n)


def over_lanes(v):
    return jnp.sum(v, axis=1, keepdims=True)


def over_rows(v):
    return jnp.sum(v, axis=0, keepdims=True)


def iota(shape, dim):
    return lax.broadcasted_iota(jnp.int32, shape, dim)


def onehot(mask):
    return mask.astype(F32).astype(BF16)


def kernel(x_hbm, dy_hbm, idst_hbm, gatt_hbm, wg_hbm, wu_hbm, wd_hbm,
           dx_hbm, dgate_ref, dwg_hbm, dwu_hbm, dwd_hbm, ja, jb, jc, ia, ib, ic,
           gat, snd, rx, wgu, wdn, acc, hd, pbuf, slott, idst, gatt, mg, jm, mr, dgb, dgr, km, dgi, dgj, dgh, dgacc,
           loc_sem, out_sem, meta_s, meta_r, g1_s, g1_r, g2_s, g2_r, fa_s, fa_r, fb_s, fb_r, fl, fm_s, fm_r,
           d2_s, d2_r, c_s, c_r, dm_s, dm_r, ba_s, ba_r, bb_s, bb_r, bc_s, bc_r, bl, bm_s, bm_r, credit, free):
    g = lax.axis_index('grp')
    l = lax.axis_index('loc')
    z, y, x = g // PLANE, (g // SIDE) % SIDE, g % SIDE
    coord = (x, y, z)
    other = 1 - l

    def rmod(v):
        return lax.rem(v, SIDE)

    def gid(zz, yy, xx):
        return zz * PLANE + yy * SIDE + xx

    def along(axis, k):
        return gid(*(k if a == axis else coord[a] for a in (2, 1, 0)))

    def in_plane(c, a, b):
        at = {c: coord[c], AXES[c][0]: a, AXES[c][1]: b}
        return gid(at[2], at[1], at[0])

    def remote(src, dst, ss, rs, grp=g, loc=l):
        return pltpu.make_async_remote_copy(src, dst, ss, rs, device_id={'grp': grp, 'loc': loc}, device_id_type=MESH)

    def local(src, dst, sem):
        return pltpu.make_async_copy(src, dst, sem)

    def wait(ref, sem):
        local(ref, ref, sem).wait()

    neighbours = [along(axis, rmod(coord[axis] + k)) for axis in range(3) for k in NEAR]

    barrier = pltpu.get_barrier_semaphore()
    for p in neighbours:
        pl.semaphore_signal(barrier, inc=1, device_id={'grp': p, 'loc': l}, device_id_type=MESH)
    pl.semaphore_signal(barrier, inc=1, device_id={'grp': g, 'loc': other}, device_id_type=MESH)

    def slab_copies(c, rows, make):
        c0, w = FWD[c]
        out = []
        if c0 < D:
            n = min(w, D - c0)
            out.append(make(x_hbm.at[rows, pl.ds(c0, n)], pl.ds(c0, n)))
        if c0 + w > D:
            s = max(c0, D)
            out.append(make(dy_hbm.at[rows, pl.ds(s - D, c0 + w - s)], pl.ds(s, c0 + w - s)))
        return out

    def cols(c):
        return pl.ds(*FWD[c])

    def own_slab(c):
        return slab_copies(c, first(TOK), lambda src, cs: local(src, gat.at[coord[c], :, cs], loc_sem.at[1, c]))

    routing = [local(idst_hbm, idst.at[c, coord[c]], loc_sem.at[0, c]) for c in range(3)]
    routing.append(local(gatt_hbm, gatt.at[x], loc_sem.at[0, 3]))
    weights = [local(wg_hbm, wgu.at[:, first(F)], loc_sem.at[2, 0]), local(wu_hbm, wgu.at[:, pl.ds(F, F)], loc_sem.at[2, 1]),
               local(wd_hbm, wdn, loc_sem.at[2, 2])]
    for cp in routing + own_slab(0) + own_slab(1) + own_slab(2) + weights:
        cp.start()
    with scope('entry'):
        pl.semaphore_wait(barrier, len(neighbours) + 1)

    def slab_send(i):
        for d, k in enumerate((1, 3)):
            h = (d + i) % 2
            rows = pl.ds(h * HALF, HALF)
            for c in range(3):
                t = along(c, rmod(coord[c] + k))
                for cp in slab_copies(c, rows, lambda src, cs: remote(src, gat.at[coord[c], rows, cs], g1_s.at[c, d, h],
                                                                      g1_r.at[c, d, h], t)):
                    cp.start()

    slab_send(0)
    for c in range(3):
        for k in NEAR:
            t = along(c, rmod(coord[c] + k))
            remote(idst_hbm, idst.at[c, coord[c]], meta_s.at[c, 0], meta_r.at[c, 0], t).start()
            if c == 0:
                remote(gatt_hbm, gatt.at[x], meta_s.at[c, 1], meta_r.at[c, 1], t).start()
    slab_send(1)
    for cp in routing:
        cp.wait()

    tri = onehot(iota((LANES, LANES), 0) < iota((LANES, LANES), 1))
    tables = 3 * SIDE * PLANE

    def table(c, k, p):
        return acc.at[pl.ds((c * SIDE + k) * PLANE + p, 1), first(TOK)]

    def gates(k, e, p):
        return acc.at[pl.ds(tables + (k * 2 + e) * PLANE + p, 1), first(TOK)]

    def make_table(c, k):
        p = iota((PLANE, 1), 0)
        gids = in_plane(c, p // SIDE, rmod(p))
        carry = jnp.zeros((PLANE, 1), F32)
        for blk in range(NBLK):
            ls = pl.ds(blk * LANES, LANES)
            ids = idst[c, k, :, ls]
            member = jnp.zeros((PLANE, LANES), F32)
            w0 = jnp.zeros((PLANE, LANES), F32)
            w1 = jnp.zeros((PLANE, LANES), F32)
            for j in range(TOP_K):
                idj = ids[j:j + 1, :]
                e0 = idj == 2 * gids
                e1 = idj == 2 * gids + 1
                member = jnp.where(e0 | e1, 1.0, member)
                if c == 0:
                    gj = gatt[k, pl.ds(j, 1), ls]
                    w0 = jnp.where(e0, gj, w0)
                    w1 = jnp.where(e1, gj, w1)
            rank = dot(member.astype(BF16), tri) + carry
            carry = carry + over_lanes(member)
            acc[pl.ds((c * SIDE + k) * PLANE, PLANE), ls] = jnp.where(member > 0, rank, -1.0)
            if c == 0:
                acc[pl.ds(tables + k * 2 * PLANE, PLANE), ls] = w0
                acc[pl.ds(tables + (k * 2 + 1) * PLANE, PLANE), ls] = w1

    with scope('own_tables'):
        for c in range(3):
            make_table(c, coord[c])

    def home_gid():
        v = iota((GROUPS, 1), 0)
        return lax.rem(v, PLANE) * SIDE + v // PLANE

    with scope('home_table'):
        carry = jnp.zeros((GROUPS, 1), F32)
        for blk in range(NBLK):
            ls = pl.ds(blk * LANES, LANES)
            member = jnp.zeros((GROUPS, LANES), F32)
            for j in range(TOP_K):
                member = jnp.where(idst[0, x, pl.ds(j, 1), ls] // 2 == home_gid(), 1.0, member)
            rank = dot(member.astype(BF16), tri) + carry
            carry = carry + over_lanes(member)
            slott[:, ls] = jnp.where(member > 0, rank, -1.0)

    for r in range(ROUNDS):
        mg[r] = jnp.zeros((SIDE, SIDE, 1, LANES), F32)

    def gather(c, k, pair):
        base = (iota((GS, 1), 0) + pair * GS).astype(F32)
        row = iota((GS, LANES), 0)
        at = iota((GS, LANES), 1) - k * RS - lax.rem(row, RS)
        for p in range(PLANE):
            mask = table(c, k, p)[...] == base
            pbuf[pl.ds(p * GS, GS), :] = onehot(mask)
            if c == 0:
                both = jnp.zeros((GS, LANES), F32)
                for e in range(2):
                    col = over_lanes(jnp.where(mask, gates(k, e, p)[...], 0.0))
                    both = jnp.where(at == e * LINE, col, both)
                for i in range(2):
                    line = over_rows(jnp.where(row // RS == i, both, 0.0))
                    mg[2 * pair + i, p // SIDE, p % SIDE] = mg[2 * pair + i, p // SIDE, p % SIDE] + line
        w = FWD[c][1]
        rows = dot(pbuf[...], gat[k, :, cols(c)]).astype(BF16).reshape(SIDE, SIDE, 2, RS, w)
        for i in range(2):
            if c == 2:
                snd[2 * pair + i, :, k, :, :, cols(c)] = rows[:, :, i]
            else:
                snd[2 * pair + i, :, :, k, :, cols(c)] = rows[:, :, i]

    for c in range(3):
        for cp in own_slab(c):
            cp.wait()

    hop_bufs = (ja, jb, jc)

    def hop_part(r, c, k):
        axis = AXES[c][0]
        for off in NEAR:
            to = rmod(coord[axis] + off)
            if c == 2:
                src, dst = snd.at[r, to, k, :, :, cols(c)], jc.at[r, k, coord[axis]]
            else:
                src, dst = snd.at[r, to, :, k, :, cols(c)], hop_bufs[c].at[r, coord[axis], :, k]
            remote(src, dst, fa_s.at[r, c], fa_r.at[r, c], along(axis, to)).start()

    def hop_dst(r, c):
        axis = AXES[c][0]
        return jc.at[r, :, coord[axis], :, :, :] if c == 2 else hop_bufs[c].at[r, coord[axis]]

    def hop_rest(r):
        for c in range(3):
            local(snd.at[r, coord[AXES[c][0]], :, :, :, cols(c)], hop_dst(r, c), fl.at[0, r, c]).start()
        for off in NEAR:
            to = rmod(y + off)
            remote(mg.at[r, to], jm.at[r, y], fm_s.at[0, r], fm_r.at[0, r], along(AXES[0][0], to)).start()
        jm[r, y] = mg[r, y]

    def plane_hop(r):
        for c in range(3):
            axis = AXES[c][0]
            for off in NEAR:
                to = rmod(coord[axis] + off)
                remote(snd.at[r, to, :, :, :, cols(c)], hop_dst(r, c), fa_s.at[r, c], fa_r.at[r, c], along(axis, to)).start()
        hop_rest(r)

    def part(c, k, h):
        return gat.at[k, pl.ds(h * HALF, HALF), cols(c)]

    def blocks(n, w):
        return snd.at[0, first(n), :, :, :, first(w)]

    def pass_on(r):
        for c, buf in enumerate(hop_bufs):
            axis = AXES[c][1]
            w = FWD[c][1]
            with scope('wait_fa'):
                wait(blocks(3, w), fa_r.at[r, c])
            wait(blocks(1, w), fl.at[0, r, c])
            dst = (rx.at[l, r, z, :, :, :, cols(c)], rx.at[l, r, :, :, x, :, cols(c)], rx.at[l, r, :, y, :, :, cols(c)])[c]
            if c == 0:
                wait(mg.at[0, first(3)], fm_r.at[0, r])
            for k in (*NEAR, 0):
                to = rmod(coord[axis] + k)
                src = buf.at[r, :, :, to] if c == 2 else buf.at[r, :, to]
                if k:
                    remote(src, dst, fb_s.at[r, c], fb_r.at[r, c], along(axis, to)).start()
                    if c == 0:
                        remote(jm.at[r, :, to], mr.at[l, r, z], fm_s.at[1, r], fm_r.at[1, r], along(axis, to)).start()
                else:
                    local(src, dst, fl.at[1, r, c]).start()
        mr[l, r, z] = jm[r, :, z]
        for c in range(3):
            wait(blocks(3, FWD[c][1]), fa_s.at[r, c])
        wait(mg.at[0, first(3)], fm_s.at[0, r])
        for p in neighbours:
            pl.semaphore_signal(free.at[r], inc=1, device_id={'grp': p, 'loc': l}, device_id_type=MESH)

    def before_near():
        for r in range(2):
            for c in (0, 2):
                hop_part(r, c, coord[c])

        for c in range(3):
            wait(idst.at[c, first(3)], meta_r.at[c, 0])
            wait(idst.at[c, first(3)], meta_s.at[c, 0])
        wait(gatt.at[first(3)], meta_r.at[0, 1])
        wait(gatt.at[first(3)], meta_s.at[0, 1])
        with scope('far_table'):
            def far_table(k, carry_):
                for c in range(3):
                    make_table(c, rmod(coord[c] + k))
                return carry_

            lax.fori_loop(1, SIDE, far_table, 0)

        for d, k in enumerate((1, 3)):
            for c in range(3):
                src = rmod(coord[c] + SIDE - k)
                with scope('wait_g1'):
                    wait(part(c, src, d), g1_r.at[c, d, d])
                remote(part(c, src, d), part(c, src, d), g2_s.at[c, d], g2_r.at[c, d], along(c, rmod(coord[c] + k))).start()
        for d, k in enumerate((1, 3)):
            for c in range(3):
                with scope('wait_g1b'):
                    wait(part(c, rmod(coord[c] + SIDE - k), 1 - d), g1_r.at[c, d, 1 - d])


    def before_second_near():
        hop_part(0, 1, y)
        for c in range(3):
            for k in (1, 3):
                hop_part(0, c, rmod(coord[c] + k))

    def before_far():
        for c in range(3):
            for d in range(2):
                with scope('wait_g2'):
                    wait(part(c, rmod(coord[c] + 2), d), g2_r.at[c, d])

    def after_far():
        for c in range(3):
            hop_part(0, c, rmod(coord[c] + 2))
        hop_rest(0)
        hop_part(1, 1, y)
        for k in NEAR:
            for c in range(3):
                hop_part(1, c, rmod(coord[c] + k))
        hop_rest(1)

    events = ((3, before_near), (5, before_second_near), (7, before_far), (8, after_far))

    def gather_step(i, carry_):
        for at, event in events:
            @pl.when(i == at)
            def _():
                event()
        far = (i == 7) | (i == 8) | (i == 11)
        off = jnp.where(i < 3, 0, jnp.where(far, 2, jnp.where(lax.rem(i, 2) == 1, 3, 1)))
        pair = jnp.where(i < 3, i, jnp.where(i > 8, 2, jnp.where((i == 5) | (i == 6) | (i == 8), 1, 0)))
        with scope('gather'):
            for c in range(3):
                gather(c, rmod(coord[c] + off), pair)
        return carry_

    lax.fori_loop(0, SIDE * PAIRS, gather_step, 0)
    for r in range(2):
        with scope('pass_on'):
            pass_on(r)
        plane_hop(r + 2)
    for c in range(3):
        for d in range(2):
            wait(part(c, 0, d), g2_s.at[c, d])
            for h in range(2):
                wait(part(c, 0, d), g1_s.at[c, d, h])
    acc[...] = jnp.zeros_like(acc)
    for cp in weights:
        cp.wait()

    mine = (iota((LINE, LANES), 1) == l * LINE + iota((LINE, LANES), 0))
    ubuf = gat.at[0, first(CH), pl.ds(D, D)]

    def result(kk, n=first(D)):
        return gat.at[kk, first(CH), n]

    def chunk(r, kk):
        lp = jnp.where(kk == 0, l, other)

        def col(c0, w):
            return rx[lp, r, :, :, :, :, pl.ds(c0, w)].reshape(CH, w)

        for m in range(PLANE):
            zz, yy = m // SIDE, m % SIDE
            gcol = over_lanes(jnp.where(mine, mr[lp, r, zz, yy], 0.0))
            rows = rx[lp, r, zz, yy, :, :, pl.ds(D, D)].reshape(LINE, D)
            ubuf[pl.ds(m * LINE, LINE), :] = (gcol * rows.astype(F32)).astype(BF16)
        for h in range(2):
            hs = pl.ds(h * WIDE, WIDE)
            ab = dot(rx[lp, r, pl.ds(2 * h, 2), :, :, :, first(D)].reshape(WIDE, D), wgu[...])
            dh = dot(ubuf[hs, :], wdn[...], 1, 1)
            a = ab[:, :F]
            b = ab[:, F:]
            sig = jax.nn.sigmoid(a)
            silu = a * sig
            hd[hs, first(F)] = (silu * b).astype(BF16)
            hd[hs, pl.ds(F, F)] = (dh * b * sig * (1.0 + a * (1.0 - sig))).astype(BF16)
            hd[hs, pl.ds(2 * F, F)] = (dh * silu).astype(BF16)
        dg = jnp.zeros((CH, 1), F32)
        for n in range(4):
            o = dot(hd[:, first(F)], wdn[:, pl.ds(n * WIDE, WIDE)])
            dg = dg + over_lanes(col(D + n * WIDE, WIDE).astype(F32) * o)
        for m in range(PLANE):
            line = over_rows(jnp.where(mine, dg[m * LINE:(m + 1) * LINE, :], 0.0))
            dgb[kk, r, m // SIDE, m % SIDE] = line
        acc[first(F), :] += dot(hd[:, first(F)], ubuf[...], 0, 0)
        for i in (1, 2):
            acc[pl.ds(i * F, F), :] += dot(hd[:, pl.ds(i * F, F)], col(0, D), 0, 0)
        for n in range(4):
            cval = dot(hd[:, pl.ds(F, 2 * F)], wgu[pl.ds(n * WIDE, WIDE), :], 1, 1)
            result(kk, pl.ds(n * WIDE, WIDE))[...] = cval.astype(BF16)

    def home_first(r):
        pl.semaphore_wait(free.at[r], len(neighbours))
        for c in range(3):
            axis = AXES[c][1]
            cs = pl.ds(*BWD[c])
            dst = snd.at[r, coord[axis], :, :, :, pl.ds(D + BWD[c][0], BWD[c][1])]
            for k in (*NEAR, 0):
                to = rmod(coord[axis] + k)
                src = (rx.at[l, r, to, :, :, :, cs], rx.at[l, r, :, :, to, :, cs], rx.at[l, r, :, to, :, :, cs])[c]
                if k:
                    remote(src, dst, ba_s.at[r, c], ba_r.at[r, c], along(axis, to)).start()
                    if c == 0:
                        remote(dgb.at[0, r, to], km.at[r, z], bm_s.at[0, r], bm_r.at[0, r], along(axis, to)).start()
                else:
                    dst[...] = src[...]
        km[r, z] = dgb[0, r, z]

    def home_second(r):
        for c, buf in enumerate((ia, ib, ic)):
            axis = AXES[c][0]
            with scope('wait_ba'):
                wait(blocks(3, BWD[c][1]), ba_r.at[r, c])
            if c == 0:
                wait(mg.at[0, first(3)], bm_r.at[0, r])
            dst = buf.at[r, coord[axis]] if c == 1 else buf.at[r, :, coord[axis]]
            cs = pl.ds(D + BWD[c][0], BWD[c][1])
            for k in (*NEAR, 0):
                to = rmod(coord[axis] + k)
                src = snd.at[r, :, :, to, :, cs] if c == 2 else snd.at[r, :, to, :, :, cs]
                if k:
                    remote(src, dst, bb_s.at[r, c], bb_r.at[r, c], along(axis, to)).start()
                    if c == 0:
                        remote(km.at[r, :, to], dgi.at[r, :, y], bm_s.at[1, r], bm_r.at[1, r], along(axis, to)).start()
                else:
                    local(src, dst, bl.at[0, r, c]).start()
        dgi[r, :, y] = km[r, :, y]

    def home_third(r):
        for c, buf in enumerate((ia, ib, ic)):
            with scope('wait_bb'):
                wait(blocks(3, BWD[c][1]), bb_r.at[r, c])
            wait(blocks(1, BWD[c][1]), bl.at[0, r, c])
            if c == 0:
                wait(mg.at[0, first(3)], bm_r.at[1, r])
                for p in range(PLANE):
                    dgj[r, pl.ds(p, 1), :] = dgi[r, p // SIDE, p % SIDE]
            cs = pl.ds(*BWD[c])
            dst = (snd.at[r, :, :, x, :, cs], snd.at[r, :, y, :, :, cs], snd.at[r, z, :, :, :, cs])[c]
            for k in (*NEAR, 0):
                to = rmod(coord[c] + k)
                src = buf.at[r, :, :, to]
                if k:
                    remote(src, dst, bc_s.at[r, c], bc_r.at[r, c], along(c, to)).start()
                    if c == 0:
                        remote(dgj.at[r], dgh.at[r, x], bm_s.at[2, r], bm_r.at[2, r], along(c, to)).start()
                else:
                    local(src, dst, bl.at[1, r, c]).start()
        dgh[r, x] = dgj[r]

    def round_body(r, carry_):
        for c in range(3):
            with scope('wait_fb'):
                wait(blocks(3, FWD[c][1]), fb_r.at[r, c])
            wait(blocks(1, FWD[c][1]), fl.at[1, r, c])
        wait(mg.at[0, first(3)], fm_r.at[1, r])
        remote(rx.at[l, r], rx.at[l, r], d2_s.at[r], d2_r.at[r], loc=other).start()
        remote(mr.at[l, r], mr.at[l, r], dm_s.at[0, r], dm_r.at[0, r], loc=other).start()

        def step(kk, carry2):
            @pl.when(kk == 1)
            def _():
                wait(rx.at[l, r], d2_s.at[r])
                pl.semaphore_signal(credit.at[r], inc=1, device_id={'grp': g, 'loc': other}, device_id_type=MESH)
                with scope('wait_d2'):
                    wait(rx.at[other, r], d2_r.at[r])
                wait(mr.at[other, r], dm_r.at[0, r])

            with scope('chunk'):
                chunk(r, kk)
            return carry2

        lax.fori_loop(0, 2, step, 0)
        with scope('credit'):
            pl.semaphore_wait(credit.at[r], 1)
        rx[other, r, :, :, :, :, first(D)] = result(1)[...].reshape(SIDE, SIDE, SIDE, RS, D)
        remote(rx.at[other, r, :, :, :, :, first(D)], rx.at[other, r, :, :, :, :, pl.ds(D, D)], c_s.at[r], c_r.at[r], loc=other).start()
        remote(dgb.at[1, r], dgr.at[r], dm_s.at[1, r], dm_r.at[1, r], loc=other).start()

        @pl.when(r < ROUNDS - 2)
        def _():
            with scope('pass_on'):
                pass_on(r + 2)

        @pl.when(r < ROUNDS - 4)
        def _():
            plane_hop(r + 4)

        with scope('wait_c'):
            wait(rx.at[l, r, :, :, :, :, pl.ds(D, D)], c_r.at[r])

        def add(zy, carry2):
            zz, yy = zy // SIDE, rmod(zy)
            p0 = gat[0, pl.ds(zy * LINE, LINE), first(D)].astype(F32).reshape(SIDE, RS, D)
            p1 = rx[l, r, zz, yy, :, :, pl.ds(D, D)].astype(F32)
            rx[l, r, zz, yy, :, :, first(D)] = (p0 + p1).astype(BF16)
            return carry2

        with scope('add'):
            lax.fori_loop(0, PLANE, add, 0)
        wait(dgr.at[r], dm_r.at[1, r])
        dgb[0, r] = dgb[0, r] + dgr[r]
        with scope('home_first'):
            home_first(r)

        @pl.when(r >= 2)
        def _():
            with scope('home_second'):
                home_second(r - 2)

        @pl.when(r >= 4)
        def _():
            with scope('home_third'):
                home_third(r - 4)
        return carry_

    lax.fori_loop(0, ROUNDS, round_body, 0)

    with scope('home_third'):
        home_third(2)
    with scope('flush'):
        outs = [local(gat.at[3, first(F), pl.ds(D, D)], dwd_hbm, out_sem.at[0])]
        gat[3, first(F), pl.ds(D, D)] = acc[first(F), :].astype(BF16)
        eye = onehot(iota((F, F), 0) == iota((F, F), 1))
        for i, out in enumerate((dwg_hbm, dwu_hbm)):
            for n in range(4):
                block = acc[pl.ds((i + 1) * F, F), pl.ds(n * WIDE, WIDE)].astype(BF16)
                stage = gat.at[1 + n // 3, pl.ds(n % 3 * WIDE, WIDE), pl.ds(i * F, F)]
                stage[...] = dot(block, eye, 0, 0).astype(BF16)
                outs.append(local(stage, out.at[pl.ds(n * WIDE, WIDE), :], out_sem.at[1 + 4 * i + n]))
        for cp in outs:
            cp.start()
        dgacc[...] = jnp.zeros_like(dgacc)
        acc[first(TOK), :] = jnp.zeros((TOK, D), F32)
        slotn = slott[...].astype(BF16)
        glane = iota((GROUPS, GROUPS * RS), 1) // RS
        spread = onehot(home_gid() == glane)
    with scope('home_second'):
        home_second(4)

    def combine(r):
        with scope('pick'):
            want = (lax.rem(iota((1, GROUPS * RS), 1), RS) + r * RS).astype(F32)
            for n in range(2):
                ns = pl.ds(n * WIDE, WIDE)
                got = dot(slotn, spread[:, n * WIDE:(n + 1) * WIDE], 0, 0)
                gat[0, :, ns] = onehot(got == want[:, n * WIDE:(n + 1) * WIDE])
        wait(dgh.at[r, first(3)], bm_r.at[2, r])
        with scope('dg'):
            for e in range(2):
                cur = dgacc[e]
                lines = jnp.zeros((GROUPS, RS), F32)
                for k in range(SIDE):
                    mine_k = dgh[r, :, :, pl.ds(e * LINE + k * RS, RS)].reshape(GROUPS, RS)
                    lines = jnp.where(x == k, mine_k, lines)
                for i in range(RS):
                    cur = jnp.where(slott[...] == (r * RS + i).astype(F32), lines[:, i:i + 1], cur)
                dgacc[e] = cur
        for c in range(3):
            with scope('wait_bc'):
                wait(blocks(3, BWD[c][1]), bc_r.at[r, c])
            wait(blocks(1, BWD[c][1]), bl.at[1, r, c])
        with scope('combine'):
            for n in range(4):
                ns = pl.ds(n * WIDE, WIDE)
                acc[first(TOK), ns] += dot(gat[0, :, first(GROUPS * RS)], snd[r, :, :, :, :, ns].reshape(GROUPS * RS, WIDE))

    tail = ((0, lambda: home_third(3)), (1, lambda: home_second(5)), (2, lambda: home_third(4)), (3, lambda: home_third(5)))

    def last(r, carry_):
        for at, hook in tail:
            @pl.when(r == at)
            def _():
                with scope('tail_hook'):
                    hook()
        combine(r)
        return carry_

    lax.fori_loop(0, ROUNDS, last, 0)
    with scope('finish'):
        gat[3, :, first(D)] = acc[first(TOK), :].astype(BF16)
        dx_out = local(gat.at[3, :, first(D)], dx_hbm, out_sem.at[9])
        dx_out.start()
        for j in range(TOP_K):
            idj = idst[0, x, pl.ds(j, 1), :]
            val = jnp.where(lax.rem(idj, 2) == 0, dgacc[0], dgacc[1])
            dgate_ref[pl.ds(j, 1), :] = over_rows(jnp.where(idj // 2 == home_gid(), val, 0.0))

    with scope('drain'):
        for r in range(ROUNDS):
            for i in range(3):
                wait(dgh.at[0, first(3)] if i == 2 else mg.at[0, first(3)], bm_s.at[i, r])
            wait(mg.at[0, first(3)], fm_s.at[1, r])
            for i in range(2):
                wait(dgr.at[r], dm_s.at[i, r])
            wait(rx.at[0, r, :, :, :, :, first(D)], c_s.at[r])
            for c in range(3):
                wait(blocks(3, FWD[c][1]), fb_s.at[r, c])
                for sem in (ba_s, bb_s, bc_s):
                    wait(blocks(3, BWD[c][1]), sem.at[r, c])
        for cp in outs:
            cp.wait()
        dx_out.wait()


def solution(mesh):
    spec = P(('part', 'grp', 'loc'))

    def device_step(x_rows, dy_rows, expert_ids, gate_vals, w_gate, w_up, w_down):
        any_ = pl.BlockSpec(memory_space=pl.ANY)
        vmem = pl.BlockSpec(memory_space=pltpu.VMEM)
        dma = pltpu.SemaphoreType.DMA
        sd = jax.ShapeDtypeStruct
        cube = (ROUNDS, SIDE, SIDE, SIDE, RS)
        lines = (ROUNDS, SIDE, SIDE, 1, LANES)
        out = pl.pallas_call(
            kernel,
            name='moe_backward',
            in_specs=[any_] * 7,
            out_specs=[any_, vmem] + [any_] * 9,
            out_shape=[sd((TOK, D), BF16), sd((TOP_K, TOK), F32), *[sd((D, F), BF16)] * 2, sd((F, D), BF16),
                       *[sd((*cube, w), BF16) for _, w in FWD + BWD]],
            scratch_shapes=[
                pltpu.VMEM((SIDE, TOK, 2 * D), BF16),
                pltpu.VMEM((*cube, 2 * D), BF16),
                pltpu.VMEM((2, *cube, 2 * D), BF16),
                pltpu.VMEM((D, 2 * F), BF16),
                pltpu.VMEM((F, D), BF16),
                pltpu.VMEM((3 * F, D), F32),
                pltpu.VMEM((CH, 3 * F), BF16),
                pltpu.VMEM((PLANE * GS, TOK), BF16),
                pltpu.VMEM((GROUPS, TOK), F32),
                pltpu.VMEM((3, SIDE, TOP_K, TOK), jnp.int32),
                pltpu.VMEM((SIDE, TOP_K, TOK), F32),
                pltpu.VMEM(lines, F32),
                pltpu.VMEM(lines, F32),
                pltpu.VMEM((2, *lines), F32),
                pltpu.VMEM((2, *lines), F32),
                pltpu.VMEM(lines, F32),
                pltpu.VMEM(lines, F32),
                pltpu.VMEM(lines, F32),
                pltpu.VMEM((ROUNDS, PLANE, LANES), F32),
                pltpu.VMEM((ROUNDS, SIDE, PLANE, LANES), F32),
                pltpu.VMEM((2, GROUPS, TOK), F32),
                dma((3, 4)), dma((10,)), *[dma((3, 2))] * 2, *[dma((3, 2, 2))] * 2, *[dma((3, 2))] * 2,
                *[dma((ROUNDS, 3))] * 4, dma((2, ROUNDS, 3)), *[dma((2, ROUNDS))] * 2,
                *[dma((ROUNDS,))] * 4, *[dma((2, ROUNDS))] * 2, *[dma((ROUNDS, 3))] * 6, dma((2, ROUNDS, 3)),
                *[dma((3, ROUNDS))] * 2, *[pltpu.SemaphoreType.REGULAR((ROUNDS,))] * 2,
            ],
            compiler_params=pltpu.CompilerParams(collective_id=0, has_side_effects=True, vmem_limit_bytes=67043328),
        )(x_rows, dy_rows, expert_ids.T, gate_vals.T, w_gate[0], w_up[0], w_down[0])
        dx, d_gates, dwg, dwu, dwd = out[:5]
        return dx, d_gates.T, dwg[None], dwu[None], dwd[None]

    return jax.shard_map(device_step, mesh=mesh, in_specs=(spec,) * 7, out_specs=(spec,) * 5, check_vma=False)
```

```python
import jax
import jax.numpy as jnp
from jax import lax
from jax.experimental import pallas as pl
from jax.experimental.pallas import tpu as pltpu
from jax.sharding import PartitionSpec as P

MESH = pl.DeviceIdType.MESH
F32 = jnp.float32
BF16 = jnp.bfloat16
LANES = 128
WIDE = 256
SIDE = 4
PLANE = SIDE * SIDE
GROUPS = SIDE ** 3
TOK = 768
HALF = TOK // 2
TOP_K = 8
D = 1024
F = 384
SLOTS = 48
ROUNDS = 6
PAIRS = ROUNDS // 2
RS = SLOTS // ROUNDS
GS = 2 * RS
LINE = SIDE * RS
CH = GROUPS * RS
NBLK = TOK // LANES
FWD = ((0, 640), (640, 640), (1280, 768))
BWD = ((0, 384), (384, 384), (768, 256))
AXES = ((1, 2), (2, 0), (0, 1))
NEAR = (1, 3, 2)
BOTH = (1, 3)
scope = jax.named_scope


def dot(a, b, ca=1, cb=0):
    return lax.dot_general(a, b, (((ca,), (cb,)), ((), ())), preferred_element_type=F32)


def first(n):
    return pl.ds(0, n)


def over_lanes(v):
    return jnp.sum(v, axis=1, keepdims=True)


def over_rows(v):
    return jnp.sum(v, axis=0, keepdims=True)


def iota(shape, dim):
    return lax.broadcasted_iota(jnp.int32, shape, dim)


def onehot(mask):
    return mask.astype(F32).astype(BF16)


def kernel(x_hbm, dy_hbm, idst_hbm, gatt_hbm, wg_hbm, wu_hbm, wd_hbm,
           dx_hbm, dgate_ref, dwg_hbm, dwu_hbm, dwd_hbm, ja, jb, jc, ia, ib, ic,
           gat, snd, rx, wgu, wdn, acc, hd, pbuf, slott, idst, gatt, mg, jm, mr, dgb, dgr, km, dgi, dgj, dgh, dgacc,
           loc_sem, out_sem, meta_s, meta_r, g1_s, g1_r, g2_s, g2_r, fa_s, fa_r, fb_s, fb_r, fl, fm_s, fm_r,
           d2_s, d2_r, c_s, c_r, dm_s, dm_r, ba_s, ba_r, bb_s, bb_r, bc_s, bc_r, bl, bm_s, bm_r, credit, free):
    g = lax.axis_index('grp')
    l = lax.axis_index('loc')
    z, y, x = g // PLANE, (g // SIDE) % SIDE, g % SIDE
    coord = (x, y, z)
    other = 1 - l

    def rmod(v):
        return lax.rem(v, SIDE)

    def gid(zz, yy, xx):
        return zz * PLANE + yy * SIDE + xx

    def along(axis, k):
        return gid(*(k if a == axis else coord[a] for a in (2, 1, 0)))

    def in_plane(c, a, b):
        at = {c: coord[c], AXES[c][0]: a, AXES[c][1]: b}
        return gid(at[2], at[1], at[0])

    def remote(src, dst, ss, rs, grp=g, loc=l):
        return pltpu.make_async_remote_copy(src, dst, ss, rs, device_id={'grp': grp, 'loc': loc}, device_id_type=MESH)

    def local(src, dst, sem):
        return pltpu.make_async_copy(src, dst, sem)

    def wait(ref, sem):
        local(ref, ref, sem).wait()

    three_lines, three_planes, three_gates = mg.at[0, first(3)], dgh.at[0, first(3)], gatt.at[first(3)]
    neighbours = [along(axis, rmod(coord[axis] + k)) for axis in range(3) for k in NEAR]

    barrier = pltpu.get_barrier_semaphore()
    for p in neighbours:
        pl.semaphore_signal(barrier, inc=1, device_id={'grp': p, 'loc': l}, device_id_type=MESH)
    pl.semaphore_signal(barrier, inc=1, device_id={'grp': g, 'loc': other}, device_id_type=MESH)

    def slab_copies(c, rows, make):
        c0, w = FWD[c]
        out = []
        if c0 < D:
            n = min(w, D - c0)
            out.append(make(x_hbm.at[rows, pl.ds(c0, n)], pl.ds(c0, n)))
        if c0 + w > D:
            s = max(c0, D)
            out.append(make(dy_hbm.at[rows, pl.ds(s - D, c0 + w - s)], pl.ds(s, c0 + w - s)))
        return out

    def cols(c):
        return pl.ds(*FWD[c])

    def own_slab(c):
        return slab_copies(c, first(TOK), lambda src, cs: local(src, gat.at[coord[c], :, cs], loc_sem.at[1, c]))

    routing = [local(idst_hbm, idst.at[c, coord[c]], loc_sem.at[0, c]) for c in range(3)]
    routing.append(local(gatt_hbm, gatt.at[x], loc_sem.at[0, 3]))
    weights = [local(wg_hbm, wgu.at[:, first(F)], loc_sem.at[2, 0]), local(wu_hbm, wgu.at[:, pl.ds(F, F)], loc_sem.at[2, 1]),
               local(wd_hbm, wdn, loc_sem.at[2, 2])]
    for cp in routing + own_slab(0) + own_slab(1) + own_slab(2) + weights:
        cp.start()
    with scope('entry'):
        pl.semaphore_wait(barrier, len(neighbours) + 1)

    def slab_send(i):
        for d, k in enumerate(BOTH):
            h = (d + i) % 2
            rows = pl.ds(h * HALF, HALF)
            for c in range(3):
                t = along(c, rmod(coord[c] + k))
                for cp in slab_copies(c, rows, lambda src, cs: remote(src, gat.at[coord[c], rows, cs], g1_s.at[c, d, h],
                                                                      g1_r.at[c, d, h], t)):
                    cp.start()

    slab_send(0)
    for c in range(3):
        for k in NEAR:
            t = along(c, rmod(coord[c] + k))
            remote(idst_hbm, idst.at[c, coord[c]], meta_s.at[c, 0], meta_r.at[c, 0], t).start()
            if c == 0:
                remote(gatt_hbm, gatt.at[x], meta_s.at[c, 1], meta_r.at[c, 1], t).start()
    slab_send(1)
    for cp in routing:
        cp.wait()

    tri = onehot(iota((LANES, LANES), 0) < iota((LANES, LANES), 1))
    tables = 3 * SIDE * PLANE

    def table(c, k, p):
        return acc.at[pl.ds((c * SIDE + k) * PLANE + p, 1), first(TOK)]

    def gates(k, e, p):
        return acc.at[pl.ds(tables + (k * 2 + e) * PLANE + p, 1), first(TOK)]

    def make_table(c, k):
        p = iota((PLANE, 1), 0)
        gids = in_plane(c, p // SIDE, rmod(p))
        carry = jnp.zeros((PLANE, 1), F32)
        for blk in range(NBLK):
            ls = pl.ds(blk * LANES, LANES)
            ids = idst[c, k, :, ls]
            member = jnp.zeros((PLANE, LANES), F32)
            w0 = jnp.zeros((PLANE, LANES), F32)
            w1 = jnp.zeros((PLANE, LANES), F32)
            for j in range(TOP_K):
                idj = ids[j:j + 1, :]
                e0 = idj == 2 * gids
                e1 = idj == 2 * gids + 1
                member = jnp.where(e0 | e1, 1.0, member)
                if c == 0:
                    gj = gatt[k, pl.ds(j, 1), ls]
                    w0 = jnp.where(e0, gj, w0)
                    w1 = jnp.where(e1, gj, w1)
            rank = dot(member.astype(BF16), tri) + carry
            carry = carry + over_lanes(member)
            acc[pl.ds((c * SIDE + k) * PLANE, PLANE), ls] = jnp.where(member > 0, rank, -1.0)
            if c == 0:
                acc[pl.ds(tables + k * 2 * PLANE, PLANE), ls] = w0
                acc[pl.ds(tables + (k * 2 + 1) * PLANE, PLANE), ls] = w1

    with scope('own_tables'):
        for c in range(3):
            make_table(c, coord[c])

    def home_gid():
        v = iota((GROUPS, 1), 0)
        return lax.rem(v, PLANE) * SIDE + v // PLANE

    with scope('home_table'):
        carry = jnp.zeros((GROUPS, 1), F32)
        for blk in range(NBLK):
            ls = pl.ds(blk * LANES, LANES)
            member = jnp.zeros((GROUPS, LANES), F32)
            for j in range(TOP_K):
                member = jnp.where(idst[0, x, pl.ds(j, 1), ls] // 2 == home_gid(), 1.0, member)
            rank = dot(member.astype(BF16), tri) + carry
            carry = carry + over_lanes(member)
            slott[:, ls] = jnp.where(member > 0, rank, -1.0)

    for r in range(ROUNDS):
        mg[r] = jnp.zeros((SIDE, SIDE, 1, LANES), F32)

    def gather(c, k, pair):
        base = (iota((GS, 1), 0) + pair * GS).astype(F32)
        row = iota((GS, LANES), 0)
        at = iota((GS, LANES), 1) - k * RS - lax.rem(row, RS)
        for p in range(PLANE):
            mask = table(c, k, p)[...] == base
            pbuf[pl.ds(p * GS, GS), :] = onehot(mask)
            if c == 0:
                both = jnp.zeros((GS, LANES), F32)
                for e in range(2):
                    col = over_lanes(jnp.where(mask, gates(k, e, p)[...], 0.0))
                    both = jnp.where(at == e * LINE, col, both)
                for i in range(2):
                    line = over_rows(jnp.where(row // RS == i, both, 0.0))
                    mg[2 * pair + i, p // SIDE, p % SIDE] = mg[2 * pair + i, p // SIDE, p % SIDE] + line
        w = FWD[c][1]
        rows = dot(pbuf[...], gat[k, :, cols(c)]).astype(BF16).reshape(SIDE, SIDE, 2, RS, w)
        for i in range(2):
            if c == 2:
                snd[2 * pair + i, :, k, :, :, cols(c)] = rows[:, :, i]
            else:
                snd[2 * pair + i, :, :, k, :, cols(c)] = rows[:, :, i]

    for c in range(3):
        for cp in own_slab(c):
            cp.wait()

    hop_bufs = (ja, jb, jc)

    def hop_part(r, c, k):
        axis = AXES[c][0]
        for off in NEAR:
            to = rmod(coord[axis] + off)
            if c == 2:
                src, dst = snd.at[r, to, k, :, :, cols(c)], jc.at[r, k, coord[axis]]
            else:
                src, dst = snd.at[r, to, :, k, :, cols(c)], hop_bufs[c].at[r, coord[axis], :, k]
            remote(src, dst, fa_s.at[r, c], fa_r.at[r, c], along(axis, to)).start()

    def hop_dst(r, c):
        axis = AXES[c][0]
        return jc.at[r, :, coord[axis], :, :, :] if c == 2 else hop_bufs[c].at[r, coord[axis]]

    def hop_rest(r):
        for c in range(3):
            local(snd.at[r, coord[AXES[c][0]], :, :, :, cols(c)], hop_dst(r, c), fl.at[0, r, c]).start()
        for off in NEAR:
            to = rmod(y + off)
            remote(mg.at[r, to], jm.at[r, y], fm_s.at[0, r], fm_r.at[0, r], along(AXES[0][0], to)).start()
        jm[r, y] = mg[r, y]

    def plane_hop(r):
        for c in range(3):
            axis = AXES[c][0]
            for off in NEAR:
                to = rmod(coord[axis] + off)
                remote(snd.at[r, to, :, :, :, cols(c)], hop_dst(r, c), fa_s.at[r, c], fa_r.at[r, c], along(axis, to)).start()
        hop_rest(r)

    def part(c, k, h):
        return gat.at[k, pl.ds(h * HALF, HALF), cols(c)]

    def blocks(n, w):
        return snd.at[0, first(n), :, :, :, first(w)]

    def pass_on(r):
        for c, buf in enumerate(hop_bufs):
            axis = AXES[c][1]
            w = FWD[c][1]
            with scope('wait_fa'):
                wait(blocks(3, w), fa_r.at[r, c])
            wait(blocks(1, w), fl.at[0, r, c])
            dst = (rx.at[l, r, z, :, :, :, cols(c)], rx.at[l, r, :, :, x, :, cols(c)], rx.at[l, r, :, y, :, :, cols(c)])[c]
            if c == 0:
                wait(three_lines, fm_r.at[0, r])
            for k in (*NEAR, 0):
                to = rmod(coord[axis] + k)
                src = buf.at[r, :, :, to] if c == 2 else buf.at[r, :, to]
                if k:
                    remote(src, dst, fb_s.at[r, c], fb_r.at[r, c], along(axis, to)).start()
                    if c == 0:
                        remote(jm.at[r, :, to], mr.at[l, r, z], fm_s.at[1, r], fm_r.at[1, r], along(axis, to)).start()
                else:
                    local(src, dst, fl.at[1, r, c]).start()
        mr[l, r, z] = jm[r, :, z]
        for c in range(3):
            wait(blocks(3, FWD[c][1]), fa_s.at[r, c])
        wait(three_lines, fm_s.at[0, r])
        for p in neighbours:
            pl.semaphore_signal(free.at[r], inc=1, device_id={'grp': p, 'loc': l}, device_id_type=MESH)

    def before_near():
        for r in range(2):
            for c in (0, 2):
                hop_part(r, c, coord[c])

        for c in range(3):
            wait(idst.at[c, first(3)], meta_r.at[c, 0])
            wait(idst.at[c, first(3)], meta_s.at[c, 0])
        wait(three_gates, meta_r.at[0, 1])
        wait(three_gates, meta_s.at[0, 1])
        with scope('far_table'):
            def far_table(k, carry_):
                for c in range(3):
                    make_table(c, rmod(coord[c] + k))
                return carry_

            lax.fori_loop(1, SIDE, far_table, 0)

        for d, k in enumerate(BOTH):
            for c in range(3):
                src = rmod(coord[c] + SIDE - k)
                with scope('wait_g1'):
                    wait(part(c, src, d), g1_r.at[c, d, d])
                remote(part(c, src, d), part(c, src, d), g2_s.at[c, d], g2_r.at[c, d], along(c, rmod(coord[c] + k))).start()
        for d, k in enumerate(BOTH):
            for c in range(3):
                with scope('wait_g1b'):
                    wait(part(c, rmod(coord[c] + SIDE - k), 1 - d), g1_r.at[c, d, 1 - d])


    def before_second_near():
        hop_part(0, 1, y)
        for c in range(3):
            for k in BOTH:
                hop_part(0, c, rmod(coord[c] + k))

    def before_far():
        for c in range(3):
            for d in range(2):
                with scope('wait_g2'):
                    wait(part(c, rmod(coord[c] + 2), d), g2_r.at[c, d])

    def after_far():
        for c in range(3):
            hop_part(0, c, rmod(coord[c] + 2))
        hop_rest(0)
        hop_part(1, 1, y)
        for k in NEAR:
            for c in range(3):
                hop_part(1, c, rmod(coord[c] + k))
        hop_rest(1)

    events = ((3, before_near), (5, before_second_near), (7, before_far), (8, after_far))

    def gather_step(i, carry_):
        for at, event in events:
            @pl.when(i == at)
            def _():
                event()
        far = (i == 7) | (i == 8) | (i == 11)
        off = jnp.where(i < 3, 0, jnp.where(far, 2, jnp.where(lax.rem(i, 2) == 1, 3, 1)))
        pair = jnp.where(i < 3, i, jnp.where(i > 8, 2, jnp.where((i == 5) | (i == 6) | (i == 8), 1, 0)))
        with scope('gather'):
            for c in range(3):
                gather(c, rmod(coord[c] + off), pair)
        return carry_

    lax.fori_loop(0, SIDE * PAIRS, gather_step, 0)
    for r in range(2):
        with scope('pass_on'):
            pass_on(r)
        plane_hop(r + 2)
    for c in range(3):
        for d in range(2):
            wait(part(c, 0, d), g2_s.at[c, d])
            for h in range(2):
                wait(part(c, 0, d), g1_s.at[c, d, h])
    acc[...] = jnp.zeros_like(acc)
    for cp in weights:
        cp.wait()

    mine = (iota((LINE, LANES), 1) == l * LINE + iota((LINE, LANES), 0))
    ubuf = gat.at[0, first(CH), pl.ds(D, D)]

    def result(kk, n=first(D)):
        return gat.at[kk, first(CH), n]

    def chunk(r, kk):
        lp = jnp.where(kk == 0, l, other)

        def col(c0, w):
            return rx[lp, r, :, :, :, :, pl.ds(c0, w)].reshape(CH, w)

        for m in range(PLANE):
            zz, yy = m // SIDE, m % SIDE
            gcol = over_lanes(jnp.where(mine, mr[lp, r, zz, yy], 0.0))
            rows = rx[lp, r, zz, yy, :, :, pl.ds(D, D)].reshape(LINE, D)
            ubuf[pl.ds(m * LINE, LINE), :] = (gcol * rows.astype(F32)).astype(BF16)
        for h in range(2):
            hs = pl.ds(h * WIDE, WIDE)
            ab = dot(rx[lp, r, pl.ds(2 * h, 2), :, :, :, first(D)].reshape(WIDE, D), wgu[...])
            dh = dot(ubuf[hs, :], wdn[...], 1, 1)
            a = ab[:, :F]
            b = ab[:, F:]
            sig = jax.nn.sigmoid(a)
            silu = a * sig
            hd[hs, first(F)] = (silu * b).astype(BF16)
            hd[hs, pl.ds(F, F)] = (dh * b * sig * (1.0 + a * (1.0 - sig))).astype(BF16)
            hd[hs, pl.ds(2 * F, F)] = (dh * silu).astype(BF16)
        dg = jnp.zeros((CH, 1), F32)
        for n in range(4):
            o = dot(hd[:, first(F)], wdn[:, pl.ds(n * WIDE, WIDE)])
            dg = dg + over_lanes(col(D + n * WIDE, WIDE).astype(F32) * o)
        for m in range(PLANE):
            line = over_rows(jnp.where(mine, dg[m * LINE:(m + 1) * LINE, :], 0.0))
            dgb[kk, r, m // SIDE, m % SIDE] = line
        acc[first(F), :] += dot(hd[:, first(F)], ubuf[...], 0, 0)
        for i in (1, 2):
            acc[pl.ds(i * F, F), :] += dot(hd[:, pl.ds(i * F, F)], col(0, D), 0, 0)
        for n in range(4):
            cval = dot(hd[:, pl.ds(F, 2 * F)], wgu[pl.ds(n * WIDE, WIDE), :], 1, 1)
            result(kk, pl.ds(n * WIDE, WIDE))[...] = cval.astype(BF16)

    def home_first(r):
        pl.semaphore_wait(free.at[r], len(neighbours))
        for c in range(3):
            axis = AXES[c][1]
            cs = pl.ds(*BWD[c])
            dst = snd.at[r, coord[axis], :, :, :, pl.ds(D + BWD[c][0], BWD[c][1])]
            for k in (*NEAR, 0):
                to = rmod(coord[axis] + k)
                src = (rx.at[l, r, to, :, :, :, cs], rx.at[l, r, :, :, to, :, cs], rx.at[l, r, :, to, :, :, cs])[c]
                if k:
                    remote(src, dst, ba_s.at[r, c], ba_r.at[r, c], along(axis, to)).start()
                    if c == 0:
                        remote(dgb.at[0, r, to], km.at[r, z], bm_s.at[0, r], bm_r.at[0, r], along(axis, to)).start()
                else:
                    dst[...] = src[...]
        km[r, z] = dgb[0, r, z]

    def home_second(r):
        for c, buf in enumerate((ia, ib, ic)):
            axis = AXES[c][0]
            with scope('wait_ba'):
                wait(blocks(3, BWD[c][1]), ba_r.at[r, c])
            if c == 0:
                wait(three_lines, bm_r.at[0, r])
            dst = buf.at[r, coord[axis]] if c == 1 else buf.at[r, :, coord[axis]]
            cs = pl.ds(D + BWD[c][0], BWD[c][1])
            for k in (*NEAR, 0):
                to = rmod(coord[axis] + k)
                src = snd.at[r, :, :, to, :, cs] if c == 2 else snd.at[r, :, to, :, :, cs]
                if k:
                    remote(src, dst, bb_s.at[r, c], bb_r.at[r, c], along(axis, to)).start()
                    if c == 0:
                        remote(km.at[r, :, to], dgi.at[r, :, y], bm_s.at[1, r], bm_r.at[1, r], along(axis, to)).start()
                else:
                    local(src, dst, bl.at[0, r, c]).start()
        dgi[r, :, y] = km[r, :, y]

    def home_third(r):
        for c, buf in enumerate((ia, ib, ic)):
            with scope('wait_bb'):
                wait(blocks(3, BWD[c][1]), bb_r.at[r, c])
            wait(blocks(1, BWD[c][1]), bl.at[0, r, c])
            if c == 0:
                wait(three_lines, bm_r.at[1, r])
                for p in range(PLANE):
                    dgj[r, pl.ds(p, 1), :] = dgi[r, p // SIDE, p % SIDE]
            cs = pl.ds(*BWD[c])
            dst = (snd.at[r, :, :, x, :, cs], snd.at[r, :, y, :, :, cs], snd.at[r, z, :, :, :, cs])[c]
            for k in (*NEAR, 0):
                to = rmod(coord[c] + k)
                src = buf.at[r, :, :, to]
                if k:
                    if c == 0:
                        remote(dgj.at[r], dgh.at[r, x], bm_s.at[2, r], bm_r.at[2, r], along(c, to)).start()
                    remote(src, dst, bc_s.at[r, c], bc_r.at[r, c], along(c, to)).start()
                else:
                    local(src, dst, bl.at[1, r, c]).start()
        dgh[r, x] = dgj[r]

    start, mid, end = range(3)
    moves = ((2, end, home_second, 0), (3, end, home_second, 1), (4, mid, home_second, 2), (4, end, home_third, 0),
             (5, start, home_second, 3), (5, mid, home_third, 1), (5, end, home_second, 4), (5, end, home_third, 2))

    def move(r, place):
        for rr, at, hop, which in moves:
            if at == place:
                @pl.when(r == rr)
                def _():
                    with scope(f'{hop.__name__}{which}'):
                        hop(which)

    def round_body(r, carry_):
        for c in range(3):
            with scope('wait_fb'):
                wait(blocks(3, FWD[c][1]), fb_r.at[r, c])
            wait(blocks(1, FWD[c][1]), fl.at[1, r, c])
        wait(three_lines, fm_r.at[1, r])
        remote(rx.at[l, r], rx.at[l, r], d2_s.at[r], d2_r.at[r], loc=other).start()
        remote(mr.at[l, r], mr.at[l, r], dm_s.at[0, r], dm_r.at[0, r], loc=other).start()
        move(r, start)

        def step(kk, carry2):
            @pl.when(kk == 1)
            def _():
                wait(rx.at[l, r], d2_s.at[r])
                pl.semaphore_signal(credit.at[r], inc=1, device_id={'grp': g, 'loc': other}, device_id_type=MESH)
                with scope('wait_d2'):
                    wait(rx.at[other, r], d2_r.at[r])
                wait(mr.at[other, r], dm_r.at[0, r])
                move(r, mid)

            with scope('chunk'):
                chunk(r, kk)
            return carry2

        lax.fori_loop(0, 2, step, 0)
        with scope('credit'):
            pl.semaphore_wait(credit.at[r], 1)
        rx[other, r, :, :, :, :, first(D)] = result(1)[...].reshape(SIDE, SIDE, SIDE, RS, D)
        remote(rx.at[other, r, :, :, :, :, first(D)], rx.at[other, r, :, :, :, :, pl.ds(D, D)], c_s.at[r], c_r.at[r], loc=other).start()
        remote(dgb.at[1, r], dgr.at[r], dm_s.at[1, r], dm_r.at[1, r], loc=other).start()

        @pl.when(r < ROUNDS - 2)
        def _():
            with scope('pass_on'):
                pass_on(r + 2)

        @pl.when(r < ROUNDS - 4)
        def _():
            plane_hop(r + 4)

        with scope('wait_c'):
            wait(rx.at[l, r, :, :, :, :, pl.ds(D, D)], c_r.at[r])

        def add(zy, carry2):
            zz, yy = zy // SIDE, rmod(zy)
            p0 = gat[0, pl.ds(zy * LINE, LINE), first(D)].astype(F32).reshape(SIDE, RS, D)
            p1 = rx[l, r, zz, yy, :, :, pl.ds(D, D)].astype(F32)
            rx[l, r, zz, yy, :, :, first(D)] = (p0 + p1).astype(BF16)
            return carry2

        with scope('add'):
            lax.fori_loop(0, PLANE, add, 0)
        wait(dgr.at[r], dm_r.at[1, r])
        dgb[0, r] = dgb[0, r] + dgr[r]
        with scope('home_first'):
            home_first(r)
        move(r, end)
        return carry_

    lax.fori_loop(0, ROUNDS, round_body, 0)

    with scope('flush'):
        outs = [local(gat.at[3, first(F), pl.ds(D, D)], dwd_hbm, out_sem.at[0])]
        gat[3, first(F), pl.ds(D, D)] = acc[first(F), :].astype(BF16)
        eye = onehot(iota((F, F), 0) == iota((F, F), 1))
        for i, out in enumerate((dwg_hbm, dwu_hbm)):
            for n in range(4):
                block = acc[pl.ds((i + 1) * F, F), pl.ds(n * WIDE, WIDE)].astype(BF16)
                stage = gat.at[1 + n // 3, pl.ds(n % 3 * WIDE, WIDE), pl.ds(i * F, F)]
                stage[...] = dot(block, eye, 0, 0).astype(BF16)
                outs.append(local(stage, out.at[pl.ds(n * WIDE, WIDE), :], out_sem.at[1 + 4 * i + n]))
        for cp in outs:
            cp.start()
        dgacc[...] = jnp.zeros_like(dgacc)
        acc[first(TOK), :] = jnp.zeros((TOK, D), F32)
        slotn = slott[...].astype(BF16)
        glane = iota((GROUPS, GROUPS * RS), 1) // RS
        spread = onehot(home_gid() == glane)
    def pick(r):
        want = (lax.rem(iota((1, GROUPS * RS), 1), RS) + r * RS).astype(F32)
        for n in range(2):
            ns = pl.ds(n * WIDE, WIDE)
            got = dot(slotn, spread[:, n * WIDE:(n + 1) * WIDE], 0, 0)
            gat[0, :, ns] = onehot(got == want[:, n * WIDE:(n + 1) * WIDE])

    def gate_gradients(r):
        wait(three_planes, bm_r.at[2, r])
        for e in range(2):
            cur = dgacc[e]
            lines = jnp.zeros((GROUPS, RS), F32)
            for k in range(SIDE):
                mine_k = dgh[r, :, :, pl.ds(e * LINE + k * RS, RS)].reshape(GROUPS, RS)
                lines = jnp.where(x == k, mine_k, lines)
            for i in range(RS):
                cur = jnp.where(slott[...] == jnp.float32(r * RS + i), lines[:, i:i + 1], cur)
            dgacc[e] = cur

    def arrived(r):
        for c in range(3):
            with scope('wait_bc'):
                wait(blocks(3, BWD[c][1]), bc_r.at[r, c])
            wait(blocks(1, BWD[c][1]), bl.at[1, r, c])

    def summed(r, ns):
        return acc[first(TOK), ns] + dot(gat[0, :, first(GROUPS * RS)], snd[r, :, :, :, :, ns].reshape(GROUPS * RS, WIDE))

    tail = ((1, home_second, 5), (1, home_third, 3), (2, home_third, 4), (3, home_third, 5))

    def last(r, carry_):
        for at, hop, which in tail:
            @pl.when(r == at)
            def _():
                with scope(f'{hop.__name__}{which}'):
                    hop(which)
        with scope('pick'):
            pick(r)
        with scope('dg'):
            gate_gradients(r)
        arrived(r)
        with scope('combine'):
            for n in range(4):
                ns = pl.ds(n * WIDE, WIDE)
                acc[first(TOK), ns] = summed(r, ns)
        return carry_

    lax.fori_loop(0, ROUNDS - 1, last, 0)
    with scope('pick'):
        pick(ROUNDS - 1)
    with scope('drain'):
        for r in range(ROUNDS):
            for i in range(2):
                wait(three_lines, bm_s.at[i, r])
                wait(dgr.at[r], dm_s.at[i, r])
            wait(three_lines, fm_s.at[1, r])
            wait(rx.at[0, r, :, :, :, :, first(D)], c_s.at[r])
            for c in range(3):
                wait(blocks(3, FWD[c][1]), fb_s.at[r, c])
                for sem in (ba_s, bb_s):
                    wait(blocks(3, BWD[c][1]), sem.at[r, c])
        for cp in outs:
            cp.wait()
    with scope('dg'):
        gate_gradients(ROUNDS - 1)
        for j in range(TOP_K):
            idj = idst[0, x, pl.ds(j, 1), :]
            val = jnp.where(lax.rem(idj, 2) == 0, dgacc[0], dgacc[1])
            dgate_ref[pl.ds(j, 1), :] = over_rows(jnp.where(idj // 2 == home_gid(), val, 0.0))
    arrived(ROUNDS - 1)
    with scope('finish'):
        outs = []
        for n in range(4):
            ns = pl.ds(n * WIDE, WIDE)
            gat[3, :, ns] = summed(ROUNDS - 1, ns).astype(BF16)
            outs.append(local(gat.at[3, :, ns], dx_hbm.at[:, ns], out_sem.at[9 + n]))
            outs[-1].start()
        for r in range(ROUNDS):
            wait(three_planes, bm_s.at[2, r])
            for c in range(3):
                wait(blocks(3, BWD[c][1]), bc_s.at[r, c])
        for cp in outs:
            cp.wait()


def hand_over(*refs):
    n = len(refs) // 4
    ins, outs, bufs, sems = refs[:n], refs[n:2 * n], refs[2 * n:3 * n], refs[3 * n:]
    loads = [pltpu.make_async_copy(a, b, sem.at[0]) for a, b, sem in zip(ins, bufs, sems)]
    stores = [pltpu.make_async_copy(b, o, sem.at[1]) for b, o, sem in zip(bufs, outs, sems)]
    for cp in loads:
        cp.start()
    for load, store in zip(loads, stores):
        load.wait()
        store.start()
    for cp in stores:
        cp.wait()


def solution(mesh):
    spec = P(('part', 'grp', 'loc'))

    def device_step(x_rows, dy_rows, expert_ids, gate_vals, w_gate, w_up, w_down):
        any_ = pl.BlockSpec(memory_space=pl.ANY)
        vmem = pl.BlockSpec(memory_space=pltpu.VMEM)
        dma = pltpu.SemaphoreType.DMA
        sd = jax.ShapeDtypeStruct
        cube = (ROUNDS, SIDE, SIDE, SIDE, RS)
        lines = (ROUNDS, SIDE, SIDE, 1, LANES)
        out = pl.pallas_call(
            kernel,
            name='moe_backward',
            in_specs=[any_] * 7,
            out_specs=[any_, vmem] + [any_] * 9,
            out_shape=[sd((TOK, D), BF16), sd((TOP_K, TOK), F32), *[sd((D, F), BF16)] * 2, sd((F, D), BF16),
                       *[sd((*cube, w), BF16) for _, w in FWD + BWD]],
            scratch_shapes=[
                pltpu.VMEM((SIDE, TOK, 2 * D), BF16),
                pltpu.VMEM((*cube, 2 * D), BF16),
                pltpu.VMEM((2, *cube, 2 * D), BF16),
                pltpu.VMEM((D, 2 * F), BF16),
                pltpu.VMEM((F, D), BF16),
                pltpu.VMEM((3 * F, D), F32),
                pltpu.VMEM((CH, 3 * F), BF16),
                pltpu.VMEM((PLANE * GS, TOK), BF16),
                pltpu.VMEM((GROUPS, TOK), F32),
                pltpu.VMEM((3, SIDE, TOP_K, TOK), jnp.int32),
                pltpu.VMEM((SIDE, TOP_K, TOK), F32),
                pltpu.VMEM(lines, F32),
                pltpu.VMEM(lines, F32),
                pltpu.VMEM((2, *lines), F32),
                pltpu.VMEM((2, *lines), F32),
                pltpu.VMEM(lines, F32),
                pltpu.VMEM(lines, F32),
                pltpu.VMEM(lines, F32),
                pltpu.VMEM((ROUNDS, PLANE, LANES), F32),
                pltpu.VMEM((ROUNDS, SIDE, PLANE, LANES), F32),
                pltpu.VMEM((2, GROUPS, TOK), F32),
                dma((3, 4)), dma((13,)), *[dma((3, 2))] * 2, *[dma((3, 2, 2))] * 2, *[dma((3, 2))] * 2,
                *[dma((ROUNDS, 3))] * 4, dma((2, ROUNDS, 3)), *[dma((2, ROUNDS))] * 2,
                *[dma((ROUNDS,))] * 4, *[dma((2, ROUNDS))] * 2, *[dma((ROUNDS, 3))] * 6, dma((2, ROUNDS, 3)),
                *[dma((3, ROUNDS))] * 2, *[pltpu.SemaphoreType.REGULAR((ROUNDS,))] * 2,
            ],
            compiler_params=pltpu.CompilerParams(collective_id=0, has_side_effects=True, vmem_limit_bytes=67043328),
        )(x_rows, dy_rows, expert_ids.T, gate_vals.T, w_gate[0], w_up[0], w_down[0])
        dx, d_gates, dwg, dwu, dwd = pl.pallas_call(
            hand_over,
            name='hand_over',
            in_specs=[any_] * 5,
            out_specs=[any_] * 5,
            out_shape=[sd(o.shape, o.dtype) for o in out[:5]],
            scratch_shapes=[pltpu.VMEM(o.shape, o.dtype) for o in out[:5]] + [dma((2,))] * 5,
        )(*out[:5])
        return dx, d_gates.T, dwg[None], dwu[None], dwd[None]

    return jax.shard_map(device_step, mesh=mesh, in_specs=(spec,) * 7, out_specs=(spec,) * 5, check_vma=False)
```

```python
import jax
import jax.numpy as jnp
from jax import lax
from jax.experimental import pallas as pl
from jax.experimental.pallas import tpu as pltpu
from jax.sharding import PartitionSpec as P

MESH = pl.DeviceIdType.MESH
F32 = jnp.float32
BF16 = jnp.bfloat16
LANES = 128
WIDE = 256
SIDE = 4
PLANE = SIDE * SIDE
GROUPS = SIDE ** 3
TOK = 768
HALF = TOK // 2
TOP_K = 8
D = 1024
F = 384
SLOTS = 48
ROUNDS = 6
PAIRS = ROUNDS // 2
RS = SLOTS // ROUNDS
GS = 2 * RS
LINE = SIDE * RS
CH = GROUPS * RS
NBLK = TOK // LANES
FWD = ((0, 640), (640, 640), (1280, 768))
BWD = ((0, 384), (384, 384), (768, 256))
AXES = ((1, 2), (2, 0), (0, 1))
NEAR = (1, 3, 2)
BOTH = (1, 3)
scope = jax.named_scope


def dot(a, b, ca=1, cb=0):
    return lax.dot_general(a, b, (((ca,), (cb,)), ((), ())), preferred_element_type=F32)


def first(n):
    return pl.ds(0, n)


def over_lanes(v):
    return jnp.sum(v, axis=1, keepdims=True)


def over_rows(v):
    return jnp.sum(v, axis=0, keepdims=True)


def iota(shape, dim):
    return lax.broadcasted_iota(jnp.int32, shape, dim)


def onehot(mask):
    return mask.astype(F32).astype(BF16)


def kernel(x_hbm, dy_hbm, idst_hbm, gatt_hbm, wg_hbm, wu_hbm, wd_hbm,
           dx_hbm, dgate_ref, dwg_hbm, dwu_hbm, dwd_hbm, ja, jb, jc, ia, ib, ic,
           gat, snd, rx, wgu, wdn, acc, hd, pbuf, slott, idst, gatt, mg, jm, mr, dgb, dgr, km, dgi, dgj, dgh, dgacc,
           loc_sem, out_sem, meta_s, meta_r, g1_s, g1_r, g2_s, g2_r, fa_s, fa_r, fb_s, fb_r, fl, fm_s, fm_r,
           d2, c_sem, dm_s, dm_r, b_s, b_r, bl, bm_s, bm_r, credit, free):
    g = lax.axis_index('grp')
    l = lax.axis_index('loc')
    z, y, x = g // PLANE, (g // SIDE) % SIDE, g % SIDE
    coord = (x, y, z)
    other = 1 - l

    def rmod(v):
        return lax.rem(v, SIDE)

    def gid(zz, yy, xx):
        return zz * PLANE + yy * SIDE + xx

    def along(axis, k):
        return gid(*(k if a == axis else coord[a] for a in (2, 1, 0)))

    def in_plane(c, a, b):
        at = {c: coord[c], AXES[c][0]: a, AXES[c][1]: b}
        return gid(at[2], at[1], at[0])

    def remote(src, dst, ss, rs, grp=g, loc=l):
        return pltpu.make_async_remote_copy(src, dst, ss, rs, device_id={'grp': grp, 'loc': loc}, device_id_type=MESH)

    def local(src, dst, sem):
        return pltpu.make_async_copy(src, dst, sem)

    def wait(ref, sem):
        local(ref, ref, sem).wait()

    three_lines, three_planes, three_gates = mg.at[0, first(3)], dgh.at[0, first(3)], gatt.at[first(3)]
    half_slab = gat.at[0, first(HALF)]

    def blocks(n, w=2 * D):
        return snd.at[0, first(n), :, :, :, first(w)]

    neighbours = [along(axis, rmod(coord[axis] + k)) for axis in range(3) for k in NEAR]

    barrier = pltpu.get_barrier_semaphore()
    for p in neighbours:
        pl.semaphore_signal(barrier, inc=1, device_id={'grp': p, 'loc': l}, device_id_type=MESH)
    pl.semaphore_signal(barrier, inc=1, device_id={'grp': g, 'loc': other}, device_id_type=MESH)

    def slab_copies(c, rows, make):
        c0, w = FWD[c]
        out = []
        if c0 < D:
            n = min(w, D - c0)
            out.append(make(x_hbm.at[rows, pl.ds(c0, n)], pl.ds(c0, n)))
        if c0 + w > D:
            s = max(c0, D)
            out.append(make(dy_hbm.at[rows, pl.ds(s - D, c0 + w - s)], pl.ds(s, c0 + w - s)))
        return out

    def cols(c):
        return pl.ds(*FWD[c])

    def own_slab(c):
        return slab_copies(c, first(TOK), lambda src, cs: local(src, gat.at[coord[c], :, cs], loc_sem.at[1]))

    routing = [local(idst_hbm, idst.at[c, coord[c]], loc_sem.at[0]) for c in range(3)]
    routing.append(local(gatt_hbm, gatt.at[x], loc_sem.at[2]))
    weights = [local(wg_hbm, wgu.at[:, first(F)], loc_sem.at[3]), local(wu_hbm, wgu.at[:, pl.ds(F, F)], loc_sem.at[3]),
               local(wd_hbm, wdn, loc_sem.at[4])]
    for cp in routing + own_slab(0) + own_slab(1) + own_slab(2) + weights:
        cp.start()
    with scope('entry'):
        pl.semaphore_wait(barrier, len(neighbours) + 1)

    def slab_send(i):
        for d, k in enumerate(BOTH):
            h = (d + i) % 2
            rows = pl.ds(h * HALF, HALF)
            for c in range(3):
                t = along(c, rmod(coord[c] + k))
                for cp in slab_copies(c, rows, lambda src, cs: remote(src, gat.at[coord[c], rows, cs], g1_s.at[0],
                                                                      g1_r.at[d, h], t)):
                    cp.start()

    slab_send(0)
    for c in range(3):
        for k in NEAR:
            t = along(c, rmod(coord[c] + k))
            remote(idst_hbm, idst.at[c, coord[c]], meta_s.at[0], meta_r.at[0], t).start()
            if c == 0:
                remote(gatt_hbm, gatt.at[x], meta_s.at[1], meta_r.at[1], t).start()
    slab_send(1)
    wait(idst.at[:, 0], loc_sem.at[0])
    wait(gatt.at[0], loc_sem.at[2])

    tri = onehot(iota((LANES, LANES), 0) < iota((LANES, LANES), 1))
    tables = 3 * SIDE * PLANE

    def table(c, k, p):
        return acc.at[pl.ds((c * SIDE + k) * PLANE + p, 1), first(TOK)]

    def gates(k, e, p):
        return acc.at[pl.ds(tables + (k * 2 + e) * PLANE + p, 1), first(TOK)]

    def make_table(c, k):
        p = iota((PLANE, 1), 0)
        gids = in_plane(c, p // SIDE, rmod(p))
        carry = jnp.zeros((PLANE, 1), F32)
        for blk in range(NBLK):
            ls = pl.ds(blk * LANES, LANES)
            ids = idst[c, k, :, ls]
            member = jnp.zeros((PLANE, LANES), F32)
            w0 = jnp.zeros((PLANE, LANES), F32)
            w1 = jnp.zeros((PLANE, LANES), F32)
            for j in range(TOP_K):
                idj = ids[j:j + 1, :]
                e0 = idj == 2 * gids
                e1 = idj == 2 * gids + 1
                member = jnp.where(e0 | e1, 1.0, member)
                if c == 0:
                    gj = gatt[k, pl.ds(j, 1), ls]
                    w0 = jnp.where(e0, gj, w0)
                    w1 = jnp.where(e1, gj, w1)
            rank = dot(member.astype(BF16), tri) + carry
            carry = carry + over_lanes(member)
            acc[pl.ds((c * SIDE + k) * PLANE, PLANE), ls] = jnp.where(member > 0, rank, -1.0)
            if c == 0:
                acc[pl.ds(tables + k * 2 * PLANE, PLANE), ls] = w0
                acc[pl.ds(tables + (k * 2 + 1) * PLANE, PLANE), ls] = w1

    with scope('own_tables'):
        for c in range(3):
            make_table(c, coord[c])

    def home_gid():
        v = iota((GROUPS, 1), 0)
        return lax.rem(v, PLANE) * SIDE + v // PLANE

    with scope('home_table'):
        carry = jnp.zeros((GROUPS, 1), F32)
        for blk in range(NBLK):
            ls = pl.ds(blk * LANES, LANES)
            member = jnp.zeros((GROUPS, LANES), F32)
            for j in range(TOP_K):
                member = jnp.where(idst[0, x, pl.ds(j, 1), ls] // 2 == home_gid(), 1.0, member)
            rank = dot(member.astype(BF16), tri) + carry
            carry = carry + over_lanes(member)
            slott[:, ls] = jnp.where(member > 0, rank, -1.0)

    for r in range(ROUNDS):
        mg[r] = jnp.zeros((SIDE, SIDE, 1, LANES), F32)

    def gather(c, k, pair):
        base = (iota((GS, 1), 0) + pair * GS).astype(F32)
        row = iota((GS, LANES), 0)
        at = iota((GS, LANES), 1) - k * RS - lax.rem(row, RS)
        for p in range(PLANE):
            mask = table(c, k, p)[...] == base
            pbuf[pl.ds(p * GS, GS), :] = onehot(mask)
            if c == 0:
                both = jnp.zeros((GS, LANES), F32)
                for e in range(2):
                    col = over_lanes(jnp.where(mask, gates(k, e, p)[...], 0.0))
                    both = jnp.where(at == e * LINE, col, both)
                for i in range(2):
                    line = over_rows(jnp.where(row // RS == i, both, 0.0))
                    mg[2 * pair + i, p // SIDE, p % SIDE] = mg[2 * pair + i, p // SIDE, p % SIDE] + line
        w = FWD[c][1]
        rows = dot(pbuf[...], gat[k, :, cols(c)]).astype(BF16).reshape(SIDE, SIDE, 2, RS, w)
        for i in range(2):
            if c == 2:
                snd[2 * pair + i, :, k, :, :, cols(c)] = rows[:, :, i]
            else:
                snd[2 * pair + i, :, :, k, :, cols(c)] = rows[:, :, i]

    wait(gat.at[0], loc_sem.at[1])

    hop_bufs = (ja, jb, jc)

    def hop_part(r, c, k):
        axis = AXES[c][0]
        for off in NEAR:
            to = rmod(coord[axis] + off)
            if c == 2:
                src, dst = snd.at[r, to, k, :, :, cols(c)], jc.at[r, k, coord[axis]]
            else:
                src, dst = snd.at[r, to, :, k, :, cols(c)], hop_bufs[c].at[r, coord[axis], :, k]
            remote(src, dst, fa_s.at[lax.rem(r, 2)], fa_r.at[r], along(axis, to)).start()

    def hop_dst(r, c):
        axis = AXES[c][0]
        return jc.at[r, :, coord[axis], :, :, :] if c == 2 else hop_bufs[c].at[r, coord[axis]]

    def hop_rest(r):
        for c in range(3):
            local(snd.at[r, coord[AXES[c][0]], :, :, :, cols(c)], hop_dst(r, c), fl.at[0, lax.rem(r, 2)]).start()
        for off in NEAR:
            to = rmod(y + off)
            remote(mg.at[r, to], jm.at[r, y], fm_s.at[lax.rem(r, 2)], fm_r.at[0, r], along(AXES[0][0], to)).start()
        jm[r, y] = mg[r, y]

    def plane_hop(r):
        for c in range(3):
            axis = AXES[c][0]
            for off in NEAR:
                to = rmod(coord[axis] + off)
                remote(snd.at[r, to, :, :, :, cols(c)], hop_dst(r, c), fa_s.at[lax.rem(r, 2)], fa_r.at[r], along(axis, to)).start()
        hop_rest(r)

    def part(c, k, h):
        return gat.at[k, pl.ds(h * HALF, HALF), cols(c)]

    def pass_on(r):
        odd = lax.rem(r, 2)
        with scope('wait_fa'):
            wait(blocks(3), fa_r.at[r])
        wait(blocks(1), fl.at[0, odd])
        wait(three_lines, fm_r.at[0, r])
        for c, buf in enumerate(hop_bufs):
            axis = AXES[c][1]
            dst = (rx.at[l, r, z, :, :, :, cols(c)], rx.at[l, r, :, :, x, :, cols(c)], rx.at[l, r, :, y, :, :, cols(c)])[c]
            for k in (*NEAR, 0):
                to = rmod(coord[axis] + k)
                src = buf.at[r, :, :, to] if c == 2 else buf.at[r, :, to]
                if k:
                    remote(src, dst, fb_s.at[0], fb_r.at[r], along(axis, to)).start()
                    if c == 0:
                        remote(jm.at[r, :, to], mr.at[l, r, z], fm_s.at[2], fm_r.at[1, r], along(axis, to)).start()
                else:
                    local(src, dst, fl.at[1, odd]).start()
        mr[l, r, z] = jm[r, :, z]
        wait(blocks(3), fa_s.at[odd])
        wait(three_lines, fm_s.at[odd])
        for p in neighbours:
            pl.semaphore_signal(free.at[r], inc=1, device_id={'grp': p, 'loc': l}, device_id_type=MESH)

    def before_near():
        for r in range(2):
            for c in (0, 2):
                hop_part(r, c, coord[c])

        for sem in (meta_r, meta_s):
            wait(idst.at[:, first(3)], sem.at[0])
            wait(three_gates, sem.at[1])
        with scope('far_table'):
            def far_table(k, carry_):
                for c in range(3):
                    make_table(c, rmod(coord[c] + k))
                return carry_

            lax.fori_loop(1, SIDE, far_table, 0)

        for d, k in enumerate(BOTH):
            with scope('wait_g1'):
                wait(half_slab, g1_r.at[d, d])
            for c in range(3):
                src = part(c, rmod(coord[c] + SIDE - k), d)
                remote(src, src, g2_s.at[0], g2_r.at[d], along(c, rmod(coord[c] + k))).start()
        for d in range(2):
            with scope('wait_g1b'):
                wait(half_slab, g1_r.at[d, 1 - d])

    def before_second_near():
        hop_part(0, 1, y)
        for c in range(3):
            for k in BOTH:
                hop_part(0, c, rmod(coord[c] + k))

    def before_far():
        for d in range(2):
            with scope('wait_g2'):
                wait(half_slab, g2_r.at[d])

    def after_far():
        for c in range(3):
            hop_part(0, c, rmod(coord[c] + 2))
        hop_rest(0)
        hop_part(1, 1, y)
        for k in NEAR:
            for c in range(3):
                hop_part(1, c, rmod(coord[c] + k))
        hop_rest(1)

    events = ((3, before_near), (5, before_second_near), (7, before_far), (8, after_far))

    def gather_step(i, carry_):
        for at, event in events:
            @pl.when(i == at)
            def _():
                event()
        far = (i == 7) | (i == 8) | (i == 11)
        off = jnp.where(i < 3, 0, jnp.where(far, 2, jnp.where(lax.rem(i, 2) == 1, 3, 1)))
        pair = jnp.where(i < 3, i, jnp.where(i > 8, 2, jnp.where((i == 5) | (i == 6) | (i == 8), 1, 0)))
        with scope('gather'):
            for c in range(3):
                gather(c, rmod(coord[c] + off), pair)
        return carry_

    lax.fori_loop(0, SIDE * PAIRS, gather_step, 0)
    for r in range(2):
        with scope('pass_on'):
            pass_on(r)
        plane_hop(r + 2)
    wait(gat.at[0], g2_s.at[0])
    wait(gat.at[first(2)], g1_s.at[0])
    acc[...] = jnp.zeros_like(acc)
    wait(wgu, loc_sem.at[3])
    wait(wdn, loc_sem.at[4])

    mine = (iota((LINE, LANES), 1) == l * LINE + iota((LINE, LANES), 0))
    ubuf = gat.at[0, first(CH), pl.ds(D, D)]

    def result(kk, n=first(D)):
        return gat.at[kk, first(CH), n]

    def chunk(r, kk):
        lp = jnp.where(kk == 0, l, other)

        def col(c0, w):
            return rx[lp, r, :, :, :, :, pl.ds(c0, w)].reshape(CH, w)

        for m in range(PLANE):
            zz, yy = m // SIDE, m % SIDE
            gcol = over_lanes(jnp.where(mine, mr[lp, r, zz, yy], 0.0))
            rows = rx[lp, r, zz, yy, :, :, pl.ds(D, D)].reshape(LINE, D)
            ubuf[pl.ds(m * LINE, LINE), :] = (gcol * rows.astype(F32)).astype(BF16)
        for h in range(2):
            hs = pl.ds(h * WIDE, WIDE)
            ab = dot(rx[lp, r, pl.ds(2 * h, 2), :, :, :, first(D)].reshape(WIDE, D), wgu[...])
            dh = dot(ubuf[hs, :], wdn[...], 1, 1)
            a = ab[:, :F]
            b = ab[:, F:]
            sig = jax.nn.sigmoid(a)
            silu = a * sig
            hd[hs, first(F)] = (silu * b).astype(BF16)
            hd[hs, pl.ds(F, F)] = (dh * b * sig * (1.0 + a * (1.0 - sig))).astype(BF16)
            hd[hs, pl.ds(2 * F, F)] = (dh * silu).astype(BF16)
        dg = jnp.zeros((CH, 1), F32)
        for n in range(4):
            o = dot(hd[:, first(F)], wdn[:, pl.ds(n * WIDE, WIDE)])
            dg = dg + over_lanes(col(D + n * WIDE, WIDE).astype(F32) * o)
        for m in range(PLANE):
            line = over_rows(jnp.where(mine, dg[m * LINE:(m + 1) * LINE, :], 0.0))
            dgb[kk, r, m // SIDE, m % SIDE] = line
        acc[first(F), :] += dot(hd[:, first(F)], ubuf[...], 0, 0)
        for i in (1, 2):
            acc[pl.ds(i * F, F), :] += dot(hd[:, pl.ds(i * F, F)], col(0, D), 0, 0)
        for n in range(4):
            cval = dot(hd[:, pl.ds(F, 2 * F)], wgu[pl.ds(n * WIDE, WIDE), :], 1, 1)
            result(kk, pl.ds(n * WIDE, WIDE))[...] = cval.astype(BF16)

    def home_first(r):
        pl.semaphore_wait(free.at[r], len(neighbours))
        for c in range(3):
            axis = AXES[c][1]
            cs = pl.ds(*BWD[c])
            dst = snd.at[r, coord[axis], :, :, :, pl.ds(D + BWD[c][0], BWD[c][1])]
            for k in (*NEAR, 0):
                to = rmod(coord[axis] + k)
                src = (rx.at[l, r, to, :, :, :, cs], rx.at[l, r, :, :, to, :, cs], rx.at[l, r, :, to, :, :, cs])[c]
                if k:
                    remote(src, dst, b_s.at[0], b_r.at[0, r], along(axis, to)).start()
                    if c == 0:
                        remote(dgb.at[0, r, to], km.at[r, z], bm_s.at[0], bm_r.at[0, r], along(axis, to)).start()
                else:
                    dst[...] = src[...]
        km[r, z] = dgb[0, r, z]

    def home_second(r):
        with scope('wait_ba'):
            wait(blocks(3, D), b_r.at[0, r])
        wait(three_lines, bm_r.at[0, r])
        for c, buf in enumerate((ia, ib, ic)):
            axis = AXES[c][0]
            dst = buf.at[r, coord[axis]] if c == 1 else buf.at[r, :, coord[axis]]
            cs = pl.ds(D + BWD[c][0], BWD[c][1])
            for k in (*NEAR, 0):
                to = rmod(coord[axis] + k)
                src = snd.at[r, :, :, to, :, cs] if c == 2 else snd.at[r, :, to, :, :, cs]
                if k:
                    remote(src, dst, b_s.at[1], b_r.at[1, r], along(axis, to)).start()
                    if c == 0:
                        remote(km.at[r, :, to], dgi.at[r, :, y], bm_s.at[1], bm_r.at[1, r], along(axis, to)).start()
                else:
                    local(src, dst, bl.at[0, r]).start()
        dgi[r, :, y] = km[r, :, y]

    def home_third(r):
        with scope('wait_bb'):
            wait(blocks(3, D), b_r.at[1, r])
        wait(blocks(1, D), bl.at[0, r])
        wait(three_lines, bm_r.at[1, r])
        for p in range(PLANE):
            dgj[r, pl.ds(p, 1), :] = dgi[r, p // SIDE, p % SIDE]
        for c, buf in enumerate((ia, ib, ic)):
            cs = pl.ds(*BWD[c])
            dst = (snd.at[r, :, :, x, :, cs], snd.at[r, :, y, :, :, cs], snd.at[r, z, :, :, :, cs])[c]
            for k in (*NEAR, 0):
                to = rmod(coord[c] + k)
                src = buf.at[r, :, :, to]
                if k:
                    if c == 0:
                        remote(dgj.at[r], dgh.at[r, x], bm_s.at[2], bm_r.at[2, r], along(c, to)).start()
                    remote(src, dst, b_s.at[2], b_r.at[2, r], along(c, to)).start()
                else:
                    local(src, dst, bl.at[1, r]).start()
        dgh[r, x] = dgj[r]

    start, mid, end = range(3)
    moves = ((2, end, home_second, 0), (3, end, home_second, 1), (4, mid, home_second, 2), (4, end, home_third, 0),
             (5, start, home_second, 3), (5, mid, home_third, 1), (5, end, home_second, 4), (5, end, home_third, 2))

    def move(r, place):
        for rr, at, hop, which in moves:
            if at == place:
                @pl.when(r == rr)
                def _():
                    with scope(f'{hop.__name__}{which}'):
                        hop(which)

    def round_body(r, carry_):
        with scope('wait_fb'):
            wait(blocks(3), fb_r.at[r])
        wait(blocks(1), fl.at[1, lax.rem(r, 2)])
        wait(three_lines, fm_r.at[1, r])
        remote(rx.at[l, r], rx.at[l, r], d2.at[0], d2.at[1], loc=other).start()
        remote(mr.at[l, r], mr.at[l, r], dm_s.at[0], dm_r.at[0], loc=other).start()
        move(r, start)

        def step(kk, carry2):
            @pl.when(kk == 1)
            def _():
                wait(rx.at[l, r], d2.at[0])
                pl.semaphore_signal(credit.at[0], inc=1, device_id={'grp': g, 'loc': other}, device_id_type=MESH)
                with scope('wait_d2'):
                    wait(rx.at[other, r], d2.at[1])
                wait(mr.at[other, r], dm_r.at[0])
                move(r, mid)

            with scope('chunk'):
                chunk(r, kk)
            return carry2

        lax.fori_loop(0, 2, step, 0)
        with scope('credit'):
            pl.semaphore_wait(credit.at[0], 1)
        rx[other, r, :, :, :, :, first(D)] = result(1)[...].reshape(SIDE, SIDE, SIDE, RS, D)
        remote(rx.at[other, r, :, :, :, :, first(D)], rx.at[other, r, :, :, :, :, pl.ds(D, D)], c_sem.at[0], c_sem.at[1], loc=other).start()
        remote(dgb.at[1, r], dgr.at[r], dm_s.at[1], dm_r.at[1], loc=other).start()

        @pl.when(r < ROUNDS - 2)
        def _():
            with scope('pass_on'):
                pass_on(r + 2)

        @pl.when(r < ROUNDS - 4)
        def _():
            plane_hop(r + 4)

        with scope('wait_c'):
            wait(rx.at[l, r, :, :, :, :, pl.ds(D, D)], c_sem.at[1])

        def add(zy, carry2):
            zz, yy = zy // SIDE, rmod(zy)
            p0 = gat[0, pl.ds(zy * LINE, LINE), first(D)].astype(F32).reshape(SIDE, RS, D)
            p1 = rx[l, r, zz, yy, :, :, pl.ds(D, D)].astype(F32)
            rx[l, r, zz, yy, :, :, first(D)] = (p0 + p1).astype(BF16)
            return carry2

        with scope('add'):
            lax.fori_loop(0, PLANE, add, 0)
        wait(dgr.at[r], dm_r.at[1])
        dgb[0, r] = dgb[0, r] + dgr[r]
        with scope('home_first'):
            home_first(r)
        move(r, end)
        return carry_

    lax.fori_loop(0, ROUNDS, round_body, 0)

    with scope('flush'):
        gat[3, first(F), pl.ds(D, D)] = acc[first(F), :].astype(BF16)
        local(gat.at[3, first(F), pl.ds(D, D)], dwd_hbm, out_sem.at[0]).start()
        eye = onehot(iota((F, F), 0) == iota((F, F), 1))
        for i, out in enumerate((dwg_hbm, dwu_hbm)):
            for n in range(4):
                block = acc[pl.ds((i + 1) * F, F), pl.ds(n * WIDE, WIDE)].astype(BF16)
                stage = gat.at[1 + n // 3, pl.ds(n % 3 * WIDE, WIDE), pl.ds(i * F, F)]
                stage[...] = dot(block, eye, 0, 0).astype(BF16)
                local(stage, out.at[pl.ds(n * WIDE, WIDE), :], out_sem.at[1]).start()
        dgacc[...] = jnp.zeros_like(dgacc)
        acc[first(TOK), :] = jnp.zeros((TOK, D), F32)
        slotn = slott[...].astype(BF16)
        glane = iota((GROUPS, GROUPS * RS), 1) // RS
        spread = onehot(home_gid() == glane)
    def pick(r):
        want = (lax.rem(iota((1, GROUPS * RS), 1), RS) + r * RS).astype(F32)
        for n in range(2):
            ns = pl.ds(n * WIDE, WIDE)
            got = dot(slotn, spread[:, n * WIDE:(n + 1) * WIDE], 0, 0)
            gat[0, :, ns] = onehot(got == want[:, n * WIDE:(n + 1) * WIDE])

    def gate_gradients(r):
        wait(three_planes, bm_r.at[2, r])
        for e in range(2):
            cur = dgacc[e]
            lines = jnp.zeros((GROUPS, RS), F32)
            for k in range(SIDE):
                mine_k = dgh[r, :, :, pl.ds(e * LINE + k * RS, RS)].reshape(GROUPS, RS)
                lines = jnp.where(x == k, mine_k, lines)
            for i in range(RS):
                cur = jnp.where(slott[...] == jnp.float32(r * RS + i), lines[:, i:i + 1], cur)
            dgacc[e] = cur

    def arrived(r):
        with scope('wait_bc'):
            wait(blocks(3, D), b_r.at[2, r])
        wait(blocks(1, D), bl.at[1, r])

    def summed(r, ns):
        return acc[first(TOK), ns] + dot(gat[0, :, first(GROUPS * RS)], snd[r, :, :, :, :, ns].reshape(GROUPS * RS, WIDE))

    tail = ((1, home_second, 5), (1, home_third, 3), (2, home_third, 4), (3, home_third, 5))

    def last(r, carry_):
        for at, hop, which in tail:
            @pl.when(r == at)
            def _():
                with scope(f'{hop.__name__}{which}'):
                    hop(which)
        with scope('pick'):
            pick(r)
        with scope('dg'):
            gate_gradients(r)
        arrived(r)
        with scope('combine'):
            for n in range(4):
                ns = pl.ds(n * WIDE, WIDE)
                acc[first(TOK), ns] = summed(r, ns)
        return carry_

    lax.fori_loop(0, ROUNDS - 1, last, 0)
    with scope('pick'):
        pick(ROUNDS - 1)
    with scope('drain'):
        wait(snd.at[:, first(3)], fb_s.at[0])
        wait(mg.at[:, first(3)], fm_s.at[2])
        for i in range(2):
            wait(snd.at[:, first(3), :, :, :, first(D)], b_s.at[i])
            wait(mg.at[:, first(3)], bm_s.at[i])
        wait(rx.at[0, :, :, :, :, :, first(D)], c_sem.at[0])
        wait(mr.at[0], dm_s.at[0])
        wait(dgr, dm_s.at[1])
        wait(wdn, out_sem.at[0])
        wait(wgu, out_sem.at[1])
    with scope('dg'):
        gate_gradients(ROUNDS - 1)
        for j in range(TOP_K):
            idj = idst[0, x, pl.ds(j, 1), :]
            val = jnp.where(lax.rem(idj, 2) == 0, dgacc[0], dgacc[1])
            dgate_ref[pl.ds(j, 1), :] = over_rows(jnp.where(idj // 2 == home_gid(), val, 0.0))
    arrived(ROUNDS - 1)
    with scope('finish'):
        for n in range(4):
            ns = pl.ds(n * WIDE, WIDE)
            gat[3, :, ns] = summed(ROUNDS - 1, ns).astype(BF16)
            local(gat.at[3, :, ns], dx_hbm.at[:, ns], out_sem.at[2]).start()
        wait(dgh.at[:, first(3)], bm_s.at[2])
        wait(snd.at[:, first(3), :, :, :, first(D)], b_s.at[2])
        wait(gat.at[3, :, first(D)], out_sem.at[2])


def hand_over(*refs):
    n = len(refs) // 4
    ins, outs, bufs, sems = refs[:n], refs[n:2 * n], refs[2 * n:3 * n], refs[3 * n:]
    loads = [pltpu.make_async_copy(a, b, sem.at[0]) for a, b, sem in zip(ins, bufs, sems)]
    stores = [pltpu.make_async_copy(b, o, sem.at[1]) for b, o, sem in zip(bufs, outs, sems)]
    for cp in loads:
        cp.start()
    for load, store in zip(loads, stores):
        load.wait()
        store.start()
    for cp in stores:
        cp.wait()


def solution(mesh):
    spec = P(('part', 'grp', 'loc'))

    def device_step(x_rows, dy_rows, expert_ids, gate_vals, w_gate, w_up, w_down):
        any_ = pl.BlockSpec(memory_space=pl.ANY)
        vmem = pl.BlockSpec(memory_space=pltpu.VMEM)
        dma = pltpu.SemaphoreType.DMA
        one, two, three, per_round = (dma((n,)) for n in (1, 2, 3, ROUNDS))
        sd = jax.ShapeDtypeStruct
        cube = (ROUNDS, SIDE, SIDE, SIDE, RS)
        lines = (ROUNDS, SIDE, SIDE, 1, LANES)
        out = pl.pallas_call(
            kernel,
            name='moe_backward',
            in_specs=[any_] * 7,
            out_specs=[any_, vmem] + [any_] * 9,
            out_shape=[sd((TOK, D), BF16), sd((TOP_K, TOK), F32), *[sd((D, F), BF16)] * 2, sd((F, D), BF16),
                       *[sd((*cube, w), BF16) for _, w in FWD + BWD]],
            scratch_shapes=[
                pltpu.VMEM((SIDE, TOK, 2 * D), BF16),
                pltpu.VMEM((*cube, 2 * D), BF16),
                pltpu.VMEM((2, *cube, 2 * D), BF16),
                pltpu.VMEM((D, 2 * F), BF16),
                pltpu.VMEM((F, D), BF16),
                pltpu.VMEM((3 * F, D), F32),
                pltpu.VMEM((CH, 3 * F), BF16),
                pltpu.VMEM((PLANE * GS, TOK), BF16),
                pltpu.VMEM((GROUPS, TOK), F32),
                pltpu.VMEM((3, SIDE, TOP_K, TOK), jnp.int32),
                pltpu.VMEM((SIDE, TOP_K, TOK), F32),
                pltpu.VMEM(lines, F32),
                pltpu.VMEM(lines, F32),
                pltpu.VMEM((2, *lines), F32),
                pltpu.VMEM((2, *lines), F32),
                pltpu.VMEM(lines, F32),
                pltpu.VMEM(lines, F32),
                pltpu.VMEM(lines, F32),
                pltpu.VMEM((ROUNDS, PLANE, LANES), F32),
                pltpu.VMEM((ROUNDS, SIDE, PLANE, LANES), F32),
                pltpu.VMEM((2, GROUPS, TOK), F32),
                dma((5,)), three, two, two, one, dma((2, 2)), one, two, two, per_round, one, per_round, dma((2, 2)), three,
                dma((2, ROUNDS)), *[two] * 4, three, dma((3, ROUNDS)), dma((2, ROUNDS)), three, dma((3, ROUNDS)),
                pltpu.SemaphoreType.REGULAR((1,)), pltpu.SemaphoreType.REGULAR((ROUNDS,)),
            ],
            compiler_params=pltpu.CompilerParams(collective_id=0, has_side_effects=True, vmem_limit_bytes=67043328),
        )(x_rows, dy_rows, expert_ids.T, gate_vals.T, w_gate[0], w_up[0], w_down[0])
        dx, d_gates, dwg, dwu, dwd = pl.pallas_call(
            hand_over,
            name='hand_over',
            in_specs=[any_] * 5,
            out_specs=[any_] * 5,
            out_shape=[sd(o.shape, o.dtype) for o in out[:5]],
            scratch_shapes=[pltpu.VMEM(o.shape, o.dtype) for o in out[:5]] + [dma((2,))] * 5,
        )(*out[:5])
        return dx, d_gates.T, dwg[None], dwu[None], dwd[None]

    return jax.shard_map(device_step, mesh=mesh, in_specs=(spec,) * 7, out_specs=(spec,) * 5, check_vma=False)
```

```python
import jax
import jax.numpy as jnp
from jax import lax
from jax.experimental import pallas as pl
from jax.experimental.pallas import tpu as pltpu
from jax.sharding import PartitionSpec as P

MESH = pl.DeviceIdType.MESH
F32 = jnp.float32
BF16 = jnp.bfloat16
LANES = 128
WIDE = 256
SIDE = 4
PLANE = SIDE * SIDE
GROUPS = SIDE ** 3
TOK = 768
HALF = TOK // 2
TOP_K = 8
D = 1024
F = 384
SLOTS = 48
ROUNDS = 6
PAIRS = ROUNDS // 2
RS = SLOTS // ROUNDS
GS = 2 * RS
LINE = SIDE * RS
CH = GROUPS * RS
NBLK = TOK // LANES
FWD = ((0, 640), (640, 640), (1280, 768))
BWD = ((0, 384), (384, 384), (768, 256))
AXES = ((1, 2), (2, 0), (0, 1))
NEAR = (1, 3, 2)
BOTH = (1, 3)
scope = jax.named_scope


def dot(a, b, ca=1, cb=0):
    return lax.dot_general(a, b, (((ca,), (cb,)), ((), ())), preferred_element_type=F32)


def first(n):
    return pl.ds(0, n)


def over_lanes(v):
    return jnp.sum(v, axis=1, keepdims=True)


def over_rows(v):
    return jnp.sum(v, axis=0, keepdims=True)


def iota(shape, dim):
    return lax.broadcasted_iota(jnp.int32, shape, dim)


def onehot(mask):
    return mask.astype(F32).astype(BF16)


def kernel(x_hbm, dy_hbm, idst_hbm, gatt_hbm, wg_hbm, wu_hbm, wd_hbm,
           dx_ref, dgate_ref, dwg_ref, dwu_ref, dwd_ref, ja, jb, jc, ia, ib, ic,
           gat, snd, rx, wgu, wdn, acc, hd, pbuf, slott, idst, gatt, mg, jm, mr, dgb, dgr, km, dgi, dgj, dgh, dgacc,
           loc_sem, meta_s, meta_r, g1_s, g1_r, g2_s, g2_r, fa_s, fa_r, fb_s, fb_r, fl, fm_s, fm_r,
           d2, c_sem, dm_s, dm_r, b_s, b_r, bl, bm_s, bm_r, credit, free):
    g = lax.axis_index('grp')
    l = lax.axis_index('loc')
    z, y, x = g // PLANE, (g // SIDE) % SIDE, g % SIDE
    coord = (x, y, z)
    other = 1 - l

    def rmod(v):
        return lax.rem(v, SIDE)

    def gid(zz, yy, xx):
        return zz * PLANE + yy * SIDE + xx

    def along(axis, k):
        return gid(*(k if a == axis else coord[a] for a in (2, 1, 0)))

    def in_plane(c, a, b):
        at = {c: coord[c], AXES[c][0]: a, AXES[c][1]: b}
        return gid(at[2], at[1], at[0])

    def remote(src, dst, ss, rs, grp=g, loc=l):
        return pltpu.make_async_remote_copy(src, dst, ss, rs, device_id={'grp': grp, 'loc': loc}, device_id_type=MESH)

    def local(src, dst, sem):
        return pltpu.make_async_copy(src, dst, sem)

    def wait(ref, sem):
        local(ref, ref, sem).wait()

    three_lines, three_planes, three_gates = mg.at[0, first(3)], dgh.at[0, first(3)], gatt.at[first(3)]
    half_slab = gat.at[0, first(HALF)]

    def blocks(n, w=2 * D):
        return snd.at[0, first(n), :, :, :, first(w)]

    neighbours = [along(axis, rmod(coord[axis] + k)) for axis in range(3) for k in NEAR]

    barrier = pltpu.get_barrier_semaphore()
    for p in neighbours:
        pl.semaphore_signal(barrier, inc=1, device_id={'grp': p, 'loc': l}, device_id_type=MESH)
    pl.semaphore_signal(barrier, inc=1, device_id={'grp': g, 'loc': other}, device_id_type=MESH)

    def slab_copies(c, rows, make):
        c0, w = FWD[c]
        out = []
        if c0 < D:
            n = min(w, D - c0)
            out.append(make(x_hbm.at[rows, pl.ds(c0, n)], pl.ds(c0, n)))
        if c0 + w > D:
            s = max(c0, D)
            out.append(make(dy_hbm.at[rows, pl.ds(s - D, c0 + w - s)], pl.ds(s, c0 + w - s)))
        return out

    def cols(c):
        return pl.ds(*FWD[c])

    def own_slab(c):
        return slab_copies(c, first(TOK), lambda src, cs: local(src, gat.at[coord[c], :, cs], loc_sem.at[1]))

    routing = [local(idst_hbm, idst.at[c, coord[c]], loc_sem.at[0]) for c in range(3)]
    routing.append(local(gatt_hbm, gatt.at[x], loc_sem.at[2]))
    weights = [local(wg_hbm, wgu.at[:, first(F)], loc_sem.at[3]), local(wu_hbm, wgu.at[:, pl.ds(F, F)], loc_sem.at[3]),
               local(wd_hbm, wdn, loc_sem.at[4])]
    for cp in routing + own_slab(0) + own_slab(1) + own_slab(2) + weights:
        cp.start()
    with scope('entry'):
        pl.semaphore_wait(barrier, len(neighbours) + 1)

    def slab_send(i):
        for d, k in enumerate(BOTH):
            h = (d + i) % 2
            rows = pl.ds(h * HALF, HALF)
            for c in range(3):
                t = along(c, rmod(coord[c] + k))
                for cp in slab_copies(c, rows, lambda src, cs: remote(src, gat.at[coord[c], rows, cs], g1_s.at[0],
                                                                      g1_r.at[d, h], t)):
                    cp.start()

    slab_send(0)
    for c in range(3):
        for k in NEAR:
            t = along(c, rmod(coord[c] + k))
            remote(idst_hbm, idst.at[c, coord[c]], meta_s.at[0], meta_r.at[0], t).start()
            if c == 0:
                remote(gatt_hbm, gatt.at[x], meta_s.at[1], meta_r.at[1], t).start()
    slab_send(1)
    wait(idst.at[:, 0], loc_sem.at[0])
    wait(gatt.at[0], loc_sem.at[2])

    tri = onehot(iota((LANES, LANES), 0) < iota((LANES, LANES), 1))
    tables = 3 * SIDE * PLANE

    def table(c, k, p):
        return acc.at[pl.ds((c * SIDE + k) * PLANE + p, 1), first(TOK)]

    def gates(k, e, p):
        return acc.at[pl.ds(tables + (k * 2 + e) * PLANE + p, 1), first(TOK)]

    def make_table(c, k):
        p = iota((PLANE, 1), 0)
        gids = in_plane(c, p // SIDE, rmod(p))
        carry = jnp.zeros((PLANE, 1), F32)
        for blk in range(NBLK):
            ls = pl.ds(blk * LANES, LANES)
            ids = idst[c, k, :, ls]
            member = jnp.zeros((PLANE, LANES), F32)
            w0 = jnp.zeros((PLANE, LANES), F32)
            w1 = jnp.zeros((PLANE, LANES), F32)
            for j in range(TOP_K):
                idj = ids[j:j + 1, :]
                e0 = idj == 2 * gids
                e1 = idj == 2 * gids + 1
                member = jnp.where(e0 | e1, 1.0, member)
                if c == 0:
                    gj = gatt[k, pl.ds(j, 1), ls]
                    w0 = jnp.where(e0, gj, w0)
                    w1 = jnp.where(e1, gj, w1)
            rank = dot(member.astype(BF16), tri) + carry
            carry = carry + over_lanes(member)
            acc[pl.ds((c * SIDE + k) * PLANE, PLANE), ls] = jnp.where(member > 0, rank, -1.0)
            if c == 0:
                acc[pl.ds(tables + k * 2 * PLANE, PLANE), ls] = w0
                acc[pl.ds(tables + (k * 2 + 1) * PLANE, PLANE), ls] = w1

    with scope('own_tables'):
        for c in range(3):
            make_table(c, coord[c])

    def home_gid():
        v = iota((GROUPS, 1), 0)
        return lax.rem(v, PLANE) * SIDE + v // PLANE

    with scope('home_table'):
        carry = jnp.zeros((GROUPS, 1), F32)
        for blk in range(NBLK):
            ls = pl.ds(blk * LANES, LANES)
            member = jnp.zeros((GROUPS, LANES), F32)
            for j in range(TOP_K):
                member = jnp.where(idst[0, x, pl.ds(j, 1), ls] // 2 == home_gid(), 1.0, member)
            rank = dot(member.astype(BF16), tri) + carry
            carry = carry + over_lanes(member)
            slott[:, ls] = jnp.where(member > 0, rank, -1.0)

    for r in range(ROUNDS):
        mg[r] = jnp.zeros((SIDE, SIDE, 1, LANES), F32)

    def gather(c, k, pair):
        base = (iota((GS, 1), 0) + pair * GS).astype(F32)
        row = iota((GS, LANES), 0)
        at = iota((GS, LANES), 1) - k * RS - lax.rem(row, RS)
        for p in range(PLANE):
            mask = table(c, k, p)[...] == base
            pbuf[pl.ds(p * GS, GS), :] = onehot(mask)
            if c == 0:
                both = jnp.zeros((GS, LANES), F32)
                for e in range(2):
                    col = over_lanes(jnp.where(mask, gates(k, e, p)[...], 0.0))
                    both = jnp.where(at == e * LINE, col, both)
                for i in range(2):
                    line = over_rows(jnp.where(row // RS == i, both, 0.0))
                    mg[2 * pair + i, p // SIDE, p % SIDE] = mg[2 * pair + i, p // SIDE, p % SIDE] + line
        w = FWD[c][1]
        rows = dot(pbuf[...], gat[k, :, cols(c)]).astype(BF16).reshape(SIDE, SIDE, 2, RS, w)
        for i in range(2):
            if c == 2:
                snd[2 * pair + i, :, k, :, :, cols(c)] = rows[:, :, i]
            else:
                snd[2 * pair + i, :, :, k, :, cols(c)] = rows[:, :, i]

    wait(gat.at[0], loc_sem.at[1])

    hop_bufs = (ja, jb, jc)

    def hop_part(r, c, k):
        axis = AXES[c][0]
        for off in NEAR:
            to = rmod(coord[axis] + off)
            if c == 2:
                src, dst = snd.at[r, to, k, :, :, cols(c)], jc.at[r, k, coord[axis]]
            else:
                src, dst = snd.at[r, to, :, k, :, cols(c)], hop_bufs[c].at[r, coord[axis], :, k]
            remote(src, dst, fa_s.at[lax.rem(r, 2)], fa_r.at[r], along(axis, to)).start()

    def hop_dst(r, c):
        axis = AXES[c][0]
        return jc.at[r, :, coord[axis], :, :, :] if c == 2 else hop_bufs[c].at[r, coord[axis]]

    def hop_rest(r):
        for c in range(3):
            local(snd.at[r, coord[AXES[c][0]], :, :, :, cols(c)], hop_dst(r, c), fl.at[0, lax.rem(r, 2)]).start()
        for off in NEAR:
            to = rmod(y + off)
            remote(mg.at[r, to], jm.at[r, y], fm_s.at[lax.rem(r, 2)], fm_r.at[0, r], along(AXES[0][0], to)).start()
        jm[r, y] = mg[r, y]

    def plane_hop(r):
        for c in range(3):
            axis = AXES[c][0]
            for off in NEAR:
                to = rmod(coord[axis] + off)
                remote(snd.at[r, to, :, :, :, cols(c)], hop_dst(r, c), fa_s.at[lax.rem(r, 2)], fa_r.at[r], along(axis, to)).start()
        hop_rest(r)

    def part(c, k, h):
        return gat.at[k, pl.ds(h * HALF, HALF), cols(c)]

    def pass_on(r):
        odd = lax.rem(r, 2)
        with scope('wait_fa'):
            wait(blocks(3), fa_r.at[r])
        wait(blocks(1), fl.at[0, odd])
        wait(three_lines, fm_r.at[0, r])
        for c, buf in enumerate(hop_bufs):
            axis = AXES[c][1]
            dst = (rx.at[r, z, :, :, :, cols(c)], rx.at[r, :, :, x, :, cols(c)], rx.at[r, :, y, :, :, cols(c)])[c]
            for k in (*NEAR, 0):
                to = rmod(coord[axis] + k)
                src = buf.at[r, :, :, to] if c == 2 else buf.at[r, :, to]
                if k:
                    remote(src, dst, fb_s.at[0], fb_r.at[r], along(axis, to)).start()
                    if c == 0:
                        remote(jm.at[r, :, to], mr.at[l, r, z], fm_s.at[2], fm_r.at[1, r], along(axis, to)).start()
                else:
                    local(src, dst, fl.at[1, odd]).start()
        mr[l, r, z] = jm[r, :, z]
        wait(blocks(3), fa_s.at[odd])
        wait(three_lines, fm_s.at[odd])
        for p in neighbours:
            pl.semaphore_signal(free.at[r], inc=1, device_id={'grp': p, 'loc': l}, device_id_type=MESH)

    def before_near():
        for r in range(2):
            for c in (0, 2):
                hop_part(r, c, coord[c])

        for sem in (meta_r, meta_s):
            wait(idst.at[:, first(3)], sem.at[0])
            wait(three_gates, sem.at[1])
        with scope('far_table'):
            def far_table(k, carry_):
                for c in range(3):
                    make_table(c, rmod(coord[c] + k))
                return carry_

            lax.fori_loop(1, SIDE, far_table, 0)

        for d, k in enumerate(BOTH):
            with scope('wait_g1'):
                wait(half_slab, g1_r.at[d, d])
            for c in range(3):
                src = part(c, rmod(coord[c] + SIDE - k), d)
                remote(src, src, g2_s.at[0], g2_r.at[d], along(c, rmod(coord[c] + k))).start()
        for d in range(2):
            with scope('wait_g1b'):
                wait(half_slab, g1_r.at[d, 1 - d])

    def before_second_near():
        hop_part(0, 1, y)
        for c in range(3):
            for k in BOTH:
                hop_part(0, c, rmod(coord[c] + k))

    def before_far():
        for d in range(2):
            with scope('wait_g2'):
                wait(half_slab, g2_r.at[d])

    def after_far():
        for c in range(3):
            hop_part(0, c, rmod(coord[c] + 2))
        hop_rest(0)
        hop_part(1, 1, y)
        for k in NEAR:
            for c in range(3):
                hop_part(1, c, rmod(coord[c] + k))
        hop_rest(1)

    events = ((3, before_near), (5, before_second_near), (7, before_far), (8, after_far))

    def gather_step(i, carry_):
        for at, event in events:
            @pl.when(i == at)
            def _():
                event()
        far = (i == 7) | (i == 8) | (i == 11)
        off = jnp.where(i < 3, 0, jnp.where(far, 2, jnp.where(lax.rem(i, 2) == 1, 3, 1)))
        pair = jnp.where(i < 3, i, jnp.where(i > 8, 2, jnp.where((i == 5) | (i == 6) | (i == 8), 1, 0)))
        with scope('gather'):
            for c in range(3):
                gather(c, rmod(coord[c] + off), pair)
        return carry_

    lax.fori_loop(0, SIDE * PAIRS, gather_step, 0)
    for r in range(2):
        with scope('pass_on'):
            pass_on(r)
        plane_hop(r + 2)
    wait(gat.at[0], g2_s.at[0])
    wait(gat.at[first(2)], g1_s.at[0])
    acc[...] = jnp.zeros_like(acc)
    wait(wgu, loc_sem.at[3])
    wait(wdn, loc_sem.at[4])

    mine = (iota((LINE, LANES), 1) == l * LINE + iota((LINE, LANES), 0))
    ubuf = gat.at[0, first(CH), pl.ds(D, D)]

    def result(kk, n=first(D)):
        return gat.at[kk, first(CH), n]

    def guest(r):
        return ROUNDS + lax.rem(r, 2)

    def chunk(r, kk):
        lp = jnp.where(kk == 0, l, other)
        slot = jnp.where(kk == 0, r, guest(r))

        def col(c0, w):
            return rx[slot, :, :, :, :, pl.ds(c0, w)].reshape(CH, w)

        for m in range(PLANE):
            zz, yy = m // SIDE, m % SIDE
            gcol = over_lanes(jnp.where(mine, mr[lp, r, zz, yy], 0.0))
            rows = rx[slot, zz, yy, :, :, pl.ds(D, D)].reshape(LINE, D)
            ubuf[pl.ds(m * LINE, LINE), :] = (gcol * rows.astype(F32)).astype(BF16)
        for h in range(2):
            hs = pl.ds(h * WIDE, WIDE)
            ab = dot(rx[slot, pl.ds(2 * h, 2), :, :, :, first(D)].reshape(WIDE, D), wgu[...])
            dh = dot(ubuf[hs, :], wdn[...], 1, 1)
            a = ab[:, :F]
            b = ab[:, F:]
            sig = jax.nn.sigmoid(a)
            silu = a * sig
            hd[hs, first(F)] = (silu * b).astype(BF16)
            hd[hs, pl.ds(F, F)] = (dh * b * sig * (1.0 + a * (1.0 - sig))).astype(BF16)
            hd[hs, pl.ds(2 * F, F)] = (dh * silu).astype(BF16)
        dg = jnp.zeros((CH, 1), F32)
        for n in range(4):
            o = dot(hd[:, first(F)], wdn[:, pl.ds(n * WIDE, WIDE)])
            dg = dg + over_lanes(col(D + n * WIDE, WIDE).astype(F32) * o)
        for m in range(PLANE):
            line = over_rows(jnp.where(mine, dg[m * LINE:(m + 1) * LINE, :], 0.0))
            dgb[kk, r, m // SIDE, m % SIDE] = line
        acc[first(F), :] += dot(hd[:, first(F)], ubuf[...], 0, 0)
        for i in (1, 2):
            acc[pl.ds(i * F, F), :] += dot(hd[:, pl.ds(i * F, F)], col(0, D), 0, 0)
        for n in range(4):
            cval = dot(hd[:, pl.ds(F, 2 * F)], wgu[pl.ds(n * WIDE, WIDE), :], 1, 1)
            result(kk, pl.ds(n * WIDE, WIDE))[...] = cval.astype(BF16)

    def home_first(r):
        pl.semaphore_wait(free.at[r], len(neighbours))
        for c in range(3):
            axis = AXES[c][1]
            cs = pl.ds(*BWD[c])
            dst = snd.at[r, coord[axis], :, :, :, pl.ds(D + BWD[c][0], BWD[c][1])]
            for k in (*NEAR, 0):
                to = rmod(coord[axis] + k)
                src = (rx.at[r, to, :, :, :, cs], rx.at[r, :, :, to, :, cs], rx.at[r, :, to, :, :, cs])[c]
                if k:
                    remote(src, dst, b_s.at[0], b_r.at[0, r], along(axis, to)).start()
                    if c == 0:
                        remote(dgb.at[0, r, to], km.at[r, z], bm_s.at[0], bm_r.at[0, r], along(axis, to)).start()
                else:
                    dst[...] = src[...]
        km[r, z] = dgb[0, r, z]

    def home_second(r):
        with scope('wait_ba'):
            wait(blocks(3, D), b_r.at[0, r])
        wait(three_lines, bm_r.at[0, r])
        for c, buf in enumerate((ia, ib, ic)):
            axis = AXES[c][0]
            dst = buf.at[r, coord[axis]] if c == 1 else buf.at[r, :, coord[axis]]
            cs = pl.ds(D + BWD[c][0], BWD[c][1])
            for k in (*NEAR, 0):
                to = rmod(coord[axis] + k)
                src = snd.at[r, :, :, to, :, cs] if c == 2 else snd.at[r, :, to, :, :, cs]
                if k:
                    remote(src, dst, b_s.at[1], b_r.at[1, r], along(axis, to)).start()
                    if c == 0:
                        remote(km.at[r, :, to], dgi.at[r, :, y], bm_s.at[1], bm_r.at[1, r], along(axis, to)).start()
                else:
                    local(src, dst, bl.at[0, r]).start()
        dgi[r, :, y] = km[r, :, y]

    def home_third(r):
        with scope('wait_bb'):
            wait(blocks(3, D), b_r.at[1, r])
        wait(blocks(1, D), bl.at[0, r])
        wait(three_lines, bm_r.at[1, r])
        for p in range(PLANE):
            dgj[r, pl.ds(p, 1), :] = dgi[r, p // SIDE, p % SIDE]
        for c, buf in enumerate((ia, ib, ic)):
            cs = pl.ds(*BWD[c])
            dst = (snd.at[r, :, :, x, :, cs], snd.at[r, :, y, :, :, cs], snd.at[r, z, :, :, :, cs])[c]
            for k in (*NEAR, 0):
                to = rmod(coord[c] + k)
                src = buf.at[r, :, :, to]
                if k:
                    if c == 0:
                        remote(dgj.at[r], dgh.at[r, x], bm_s.at[2], bm_r.at[2, r], along(c, to)).start()
                    remote(src, dst, b_s.at[2], b_r.at[2, r], along(c, to)).start()
                else:
                    local(src, dst, bl.at[1, r]).start()
        dgh[r, x] = dgj[r]

    start, mid, end = range(3)
    moves = ((2, end, home_second, 0), (3, end, home_second, 1), (4, mid, home_second, 2), (4, end, home_third, 0),
             (5, start, home_second, 3), (5, mid, home_third, 1), (5, end, home_second, 4), (5, end, home_third, 2))

    def move(r, place):
        for rr, at, hop, which in moves:
            if at == place:
                @pl.when(r == rr)
                def _():
                    with scope(f'{hop.__name__}{which}'):
                        hop(which)

    def round_body(r, carry_):
        with scope('wait_fb'):
            wait(blocks(3), fb_r.at[r])
        wait(blocks(1), fl.at[1, lax.rem(r, 2)])
        wait(three_lines, fm_r.at[1, r])
        remote(rx.at[r], rx.at[guest(r)], d2.at[0], d2.at[1], loc=other).start()
        remote(mr.at[l, r], mr.at[l, r], dm_s.at[0], dm_r.at[0], loc=other).start()
        move(r, start)

        def step(kk, carry2):
            @pl.when(kk == 1)
            def _():
                wait(rx.at[r], d2.at[0])
                pl.semaphore_signal(credit.at[0], inc=1, device_id={'grp': g, 'loc': other}, device_id_type=MESH)
                with scope('wait_d2'):
                    wait(rx.at[r], d2.at[1])
                wait(mr.at[other, r], dm_r.at[0])
                move(r, mid)

            with scope('chunk'):
                chunk(r, kk)
            return carry2

        lax.fori_loop(0, 2, step, 0)
        with scope('credit'):
            pl.semaphore_wait(credit.at[0], 1)

        @pl.when(r > 0)
        def _():
            wait(rx.at[r, :, :, :, :, first(D)], c_sem.at[0])

        mine_there = rx.at[guest(r), :, :, :, :, first(D)]
        mine_there[...] = result(1)[...].reshape(SIDE, SIDE, SIDE, RS, D)
        remote(mine_there, rx.at[r, :, :, :, :, pl.ds(D, D)], c_sem.at[0], c_sem.at[1], loc=other).start()
        remote(dgb.at[1, r], dgr.at[r], dm_s.at[1], dm_r.at[1], loc=other).start()

        @pl.when(r < ROUNDS - 2)
        def _():
            with scope('pass_on'):
                pass_on(r + 2)

        @pl.when(r < ROUNDS - 4)
        def _():
            plane_hop(r + 4)

        with scope('wait_c'):
            wait(rx.at[r, :, :, :, :, pl.ds(D, D)], c_sem.at[1])

        def add(zy, carry2):
            zz, yy = zy // SIDE, rmod(zy)
            p0 = gat[0, pl.ds(zy * LINE, LINE), first(D)].astype(F32).reshape(SIDE, RS, D)
            p1 = rx[r, zz, yy, :, :, pl.ds(D, D)].astype(F32)
            rx[r, zz, yy, :, :, first(D)] = (p0 + p1).astype(BF16)
            return carry2

        with scope('add'):
            lax.fori_loop(0, PLANE, add, 0)
        wait(dgr.at[r], dm_r.at[1])
        dgb[0, r] = dgb[0, r] + dgr[r]
        with scope('home_first'):
            home_first(r)
        move(r, end)
        return carry_

    lax.fori_loop(0, ROUNDS, round_body, 0)

    with scope('flush'):
        dwd_ref[...] = acc[first(F), :].astype(BF16)
        eye = onehot(iota((F, F), 0) == iota((F, F), 1))
        for i, out in enumerate((dwg_ref, dwu_ref)):
            for n in range(4):
                ns = pl.ds(n * WIDE, WIDE)
                out[ns, :] = dot(acc[pl.ds((i + 1) * F, F), ns].astype(BF16), eye, 0, 0).astype(BF16)
        dgacc[...] = jnp.zeros_like(dgacc)
        acc[first(TOK), :] = jnp.zeros((TOK, D), F32)
        slotn = slott[...].astype(BF16)
        glane = iota((GROUPS, GROUPS * RS), 1) // RS
        spread = onehot(home_gid() == glane)
    def pick(r):
        want = (lax.rem(iota((1, GROUPS * RS), 1), RS) + r * RS).astype(F32)
        for n in range(2):
            ns = pl.ds(n * WIDE, WIDE)
            got = dot(slotn, spread[:, n * WIDE:(n + 1) * WIDE], 0, 0)
            gat[0, :, ns] = onehot(got == want[:, n * WIDE:(n + 1) * WIDE])

    def gate_gradients(r):
        wait(three_planes, bm_r.at[2, r])
        for e in range(2):
            cur = dgacc[e]
            lines = jnp.zeros((GROUPS, RS), F32)
            for k in range(SIDE):
                mine_k = dgh[r, :, :, pl.ds(e * LINE + k * RS, RS)].reshape(GROUPS, RS)
                lines = jnp.where(x == k, mine_k, lines)
            for i in range(RS):
                cur = jnp.where(slott[...] == jnp.float32(r * RS + i), lines[:, i:i + 1], cur)
            dgacc[e] = cur

    def arrived(r):
        with scope('wait_bc'):
            wait(blocks(3, D), b_r.at[2, r])
        wait(blocks(1, D), bl.at[1, r])

    def summed(r, ns):
        return acc[first(TOK), ns] + dot(gat[0, :, first(GROUPS * RS)], snd[r, :, :, :, :, ns].reshape(GROUPS * RS, WIDE))

    tail = ((1, home_second, 5), (1, home_third, 3), (2, home_third, 4), (3, home_third, 5))

    def last(r, carry_):
        for at, hop, which in tail:
            @pl.when(r == at)
            def _():
                with scope(f'{hop.__name__}{which}'):
                    hop(which)
        with scope('pick'):
            pick(r)
        with scope('dg'):
            gate_gradients(r)
        arrived(r)
        with scope('combine'):
            for n in range(4):
                ns = pl.ds(n * WIDE, WIDE)
                acc[first(TOK), ns] = summed(r, ns)
        return carry_

    lax.fori_loop(0, ROUNDS - 1, last, 0)
    with scope('pick'):
        pick(ROUNDS - 1)
    with scope('drain'):
        wait(snd.at[:, first(3)], fb_s.at[0])
        wait(mg.at[:, first(3)], fm_s.at[2])
        for i in range(2):
            wait(snd.at[:, first(3), :, :, :, first(D)], b_s.at[i])
            wait(mg.at[:, first(3)], bm_s.at[i])
        wait(rx.at[0, :, :, :, :, first(D)], c_sem.at[0])
        wait(mr.at[0], dm_s.at[0])
        wait(dgr, dm_s.at[1])
    with scope('dg'):
        gate_gradients(ROUNDS - 1)
        for j in range(TOP_K):
            idj = idst[0, x, pl.ds(j, 1), :]
            val = jnp.where(lax.rem(idj, 2) == 0, dgacc[0], dgacc[1])
            dgate_ref[pl.ds(j, 1), :] = over_rows(jnp.where(idj // 2 == home_gid(), val, 0.0))
    arrived(ROUNDS - 1)
    with scope('finish'):
        for n in range(4):
            ns = pl.ds(n * WIDE, WIDE)
            dx_ref[:, ns] = summed(ROUNDS - 1, ns).astype(BF16)
        wait(dgh.at[:, first(3)], bm_s.at[2])
        wait(snd.at[:, first(3), :, :, :, first(D)], b_s.at[2])


def hand_over(*refs):
    n = len(refs) // 3
    copies = [pltpu.make_async_copy(a, b, sem) for a, b, sem in zip(refs[:n], refs[n:2 * n], refs[2 * n:])]
    for cp in copies:
        cp.start()
    for cp in copies:
        cp.wait()


def solution(mesh):
    spec = P(('part', 'grp', 'loc'))

    def device_step(x_rows, dy_rows, expert_ids, gate_vals, w_gate, w_up, w_down):
        any_ = pl.BlockSpec(memory_space=pl.ANY)
        vmem = pl.BlockSpec(memory_space=pltpu.VMEM)
        dma = pltpu.SemaphoreType.DMA
        one, two, three, per_round = (dma((n,)) for n in (1, 2, 3, ROUNDS))
        sd = jax.ShapeDtypeStruct
        results = [sd((TOK, D), BF16), sd((TOP_K, TOK), F32), *[sd((D, F), BF16)] * 2, sd((F, D), BF16)]
        cube = (ROUNDS, SIDE, SIDE, SIDE, RS)
        lines = (ROUNDS, SIDE, SIDE, 1, LANES)
        out = pl.pallas_call(
            kernel,
            name='moe_backward',
            in_specs=[any_] * 7,
            out_specs=[vmem] * 5 + [any_] * 6,
            out_shape=[*[pltpu.VMEM(o.shape, o.dtype) for o in results], *[sd((*cube, w), BF16) for _, w in FWD + BWD]],
            scratch_shapes=[
                pltpu.VMEM((SIDE, TOK, 2 * D), BF16),
                pltpu.VMEM((*cube, 2 * D), BF16),
                pltpu.VMEM((ROUNDS + 2, SIDE, SIDE, SIDE, RS, 2 * D), BF16),
                pltpu.VMEM((D, 2 * F), BF16),
                pltpu.VMEM((F, D), BF16),
                pltpu.VMEM((3 * F, D), F32),
                pltpu.VMEM((CH, 3 * F), BF16),
                pltpu.VMEM((PLANE * GS, TOK), BF16),
                pltpu.VMEM((GROUPS, TOK), F32),
                pltpu.VMEM((3, SIDE, TOP_K, TOK), jnp.int32),
                pltpu.VMEM((SIDE, TOP_K, TOK), F32),
                pltpu.VMEM(lines, F32),
                pltpu.VMEM(lines, F32),
                pltpu.VMEM((2, *lines), F32),
                pltpu.VMEM((2, *lines), F32),
                pltpu.VMEM(lines, F32),
                pltpu.VMEM(lines, F32),
                pltpu.VMEM(lines, F32),
                pltpu.VMEM((ROUNDS, PLANE, LANES), F32),
                pltpu.VMEM((ROUNDS, SIDE, PLANE, LANES), F32),
                pltpu.VMEM((2, GROUPS, TOK), F32),
                dma((5,)), two, two, one, dma((2, 2)), one, two, two, per_round, one, per_round, dma((2, 2)), three,
                dma((2, ROUNDS)), *[two] * 4, three, dma((3, ROUNDS)), dma((2, ROUNDS)), three, dma((3, ROUNDS)),
                pltpu.SemaphoreType.REGULAR((1,)), pltpu.SemaphoreType.REGULAR((ROUNDS,)),
            ],
            compiler_params=pltpu.CompilerParams(collective_id=0, has_side_effects=True, vmem_limit_bytes=60 << 20),
        )(x_rows, dy_rows, expert_ids.T, gate_vals.T, w_gate[0], w_up[0], w_down[0])
        dx, d_gates, dwg, dwu, dwd = pl.pallas_call(
            hand_over,
            name='hand_over',
            in_specs=[vmem] * 5,
            out_specs=[any_] * 5,
            out_shape=results,
            scratch_shapes=[pltpu.SemaphoreType.DMA] * 5,
            compiler_params=pltpu.CompilerParams(vmem_limit_bytes=1 << 20),
        )(*[pltpu.with_memory_space_constraint(o, pltpu.VMEM) for o in out[:5]])
        return dx, d_gates.T, dwg[None], dwu[None], dwd[None]

    return jax.shard_map(device_step, mesh=mesh, in_specs=(spec,) * 7, out_specs=(spec,) * 5, check_vma=False)
```

```python
import jax
import jax.numpy as jnp
from jax import lax
from jax.experimental import pallas as pl
from jax.experimental.pallas import tpu as pltpu
from jax.sharding import PartitionSpec as P

MESH = pl.DeviceIdType.MESH
F32 = jnp.float32
BF16 = jnp.bfloat16
LANES = 128
WIDE = 256
SIDE = 4
PLANE = SIDE * SIDE
GROUPS = SIDE ** 3
TOK = 768
HALF = TOK // 2
TOP_K = 8
D = 1024
F = 384
SLOTS = 48
ROUNDS = 6
PAIRS = ROUNDS // 2
RS = SLOTS // ROUNDS
GS = 2 * RS
LINE = SIDE * RS
CH = GROUPS * RS
NBLK = TOK // LANES
FWD = ((0, 640), (640, 640), (1280, 768))
BWD = ((0, 384), (384, 384), (768, 256))
AXES = ((1, 2), (2, 0), (0, 1))
NEAR = (1, 3, 2)
BOTH = (1, 3)
scope = jax.named_scope


def dot(a, b, ca=1, cb=0):
    return lax.dot_general(a, b, (((ca,), (cb,)), ((), ())), preferred_element_type=F32)


def first(n):
    return pl.ds(0, n)


def over_lanes(v):
    return jnp.sum(v, axis=1, keepdims=True)


def over_rows(v):
    return jnp.sum(v, axis=0, keepdims=True)


def iota(shape, dim):
    return lax.broadcasted_iota(jnp.int32, shape, dim)


def onehot(mask):
    return mask.astype(F32).astype(BF16)


def kernel(x_hbm, dy_hbm, idst_hbm, gatt_hbm, wg_hbm, wu_hbm, wd_hbm,
           dx_ref, dgate_ref, dwg_ref, dwu_ref, dwd_ref, ja, jb, jc, ia, ib, ic,
           gat, snd, rx, wgu, wdn, acc, hd, pbuf, slott, idst, gatt, mg, jm, mr, dgb, dgr, km, dgi, dgj, dgh, dgacc,
           loc_sem, meta_s, meta_r, g1_s, g1_r, g2_s, g2_r, fa_s, fa_r, fb_s, fb_r, fl, fm_s, fm_r,
           d2, c_sem, dm_s, dm_r, b_s, b_r, bl, bm_s, bm_r, credit, free):
    g = lax.axis_index('grp')
    l = lax.axis_index('loc')
    cz, cy, cx = g // PLANE, (g // SIDE) % SIDE, g % SIDE
    x, y, z = cx + l * (cz - cx), cy + l * (cx - cy), cz + l * (cy - cz)
    step_x, step_y, step_z = 1 + l * (PLANE - 1), SIDE + l * (1 - SIDE), PLANE + l * (SIDE - PLANE)
    coord = (x, y, z)
    other = 1 - l

    def rmod(v):
        return lax.rem(v, SIDE)

    def gid(zz, yy, xx):
        return zz * step_z + yy * step_y + xx * step_x

    def along(axis, k):
        return gid(*(k if a == axis else coord[a] for a in (2, 1, 0)))

    def in_plane(c, a, b):
        at = {c: coord[c], AXES[c][0]: a, AXES[c][1]: b}
        return gid(at[2], at[1], at[0])

    def remote(src, dst, ss, rs, grp=g, loc=l):
        return pltpu.make_async_remote_copy(src, dst, ss, rs, device_id={'grp': grp, 'loc': loc}, device_id_type=MESH)

    def local(src, dst, sem):
        return pltpu.make_async_copy(src, dst, sem)

    def wait(ref, sem):
        local(ref, ref, sem).wait()

    three_lines, three_planes, three_gates = mg.at[0, first(3)], dgh.at[0, first(3)], gatt.at[first(3)]
    half_slab = gat.at[0, first(HALF)]

    def blocks(n, w=2 * D):
        return snd.at[0, first(n), :, :, :, first(w)]

    neighbours = [along(axis, rmod(coord[axis] + k)) for axis in range(3) for k in NEAR]

    barrier = pltpu.get_barrier_semaphore()
    for p in neighbours:
        pl.semaphore_signal(barrier, inc=1, device_id={'grp': p, 'loc': l}, device_id_type=MESH)
    pl.semaphore_signal(barrier, inc=1, device_id={'grp': g, 'loc': other}, device_id_type=MESH)

    def slab_copies(c, rows, make):
        c0, w = FWD[c]
        out = []
        if c0 < D:
            n = min(w, D - c0)
            out.append(make(x_hbm.at[rows, pl.ds(c0, n)], pl.ds(c0, n)))
        if c0 + w > D:
            s = max(c0, D)
            out.append(make(dy_hbm.at[rows, pl.ds(s - D, c0 + w - s)], pl.ds(s, c0 + w - s)))
        return out

    def cols(c):
        return pl.ds(*FWD[c])

    def own_slab(c):
        return slab_copies(c, first(TOK), lambda src, cs: local(src, gat.at[coord[c], :, cs], loc_sem.at[1]))

    routing = [local(idst_hbm, idst.at[c, coord[c]], loc_sem.at[0]) for c in range(3)]
    routing.append(local(gatt_hbm, gatt.at[x], loc_sem.at[2]))
    weights = [local(wg_hbm, wgu.at[:, first(F)], loc_sem.at[3]), local(wu_hbm, wgu.at[:, pl.ds(F, F)], loc_sem.at[3]),
               local(wd_hbm, wdn, loc_sem.at[4])]
    for cp in routing + own_slab(0) + own_slab(1) + own_slab(2) + weights:
        cp.start()
    with scope('entry'):
        pl.semaphore_wait(barrier, len(neighbours) + 1)

    def slab_send(i):
        for d, k in enumerate(BOTH):
            h = (d + i) % 2
            rows = pl.ds(h * HALF, HALF)
            for c in range(3):
                t = along(c, rmod(coord[c] + k))
                for cp in slab_copies(c, rows, lambda src, cs: remote(src, gat.at[coord[c], rows, cs], g1_s.at[0],
                                                                      g1_r.at[d, h], t)):
                    cp.start()

    slab_send(0)
    for c in range(3):
        for k in NEAR:
            t = along(c, rmod(coord[c] + k))
            remote(idst_hbm, idst.at[c, coord[c]], meta_s.at[0], meta_r.at[0], t).start()
            if c == 0:
                remote(gatt_hbm, gatt.at[x], meta_s.at[1], meta_r.at[1], t).start()
    slab_send(1)
    wait(idst.at[:, 0], loc_sem.at[0])
    wait(gatt.at[0], loc_sem.at[2])

    tri = onehot(iota((LANES, LANES), 0) < iota((LANES, LANES), 1))
    tables = 3 * SIDE * PLANE

    def table(c, k, p):
        return acc.at[pl.ds((c * SIDE + k) * PLANE + p, 1), first(TOK)]

    def gates(k, e, p):
        return acc.at[pl.ds(tables + (k * 2 + e) * PLANE + p, 1), first(TOK)]

    def make_table(c, k):
        p = iota((PLANE, 1), 0)
        gids = in_plane(c, p // SIDE, rmod(p))
        carry = jnp.zeros((PLANE, 1), F32)
        for blk in range(NBLK):
            ls = pl.ds(blk * LANES, LANES)
            ids = idst[c, k, :, ls]
            member = jnp.zeros((PLANE, LANES), F32)
            w0 = jnp.zeros((PLANE, LANES), F32)
            w1 = jnp.zeros((PLANE, LANES), F32)
            for j in range(TOP_K):
                idj = ids[j:j + 1, :]
                e0 = idj == 2 * gids
                e1 = idj == 2 * gids + 1
                member = jnp.where(e0 | e1, 1.0, member)
                if c == 0:
                    gj = gatt[k, pl.ds(j, 1), ls]
                    w0 = jnp.where(e0, gj, w0)
                    w1 = jnp.where(e1, gj, w1)
            rank = dot(member.astype(BF16), tri) + carry
            carry = carry + over_lanes(member)
            acc[pl.ds((c * SIDE + k) * PLANE, PLANE), ls] = jnp.where(member > 0, rank, -1.0)
            if c == 0:
                acc[pl.ds(tables + k * 2 * PLANE, PLANE), ls] = w0
                acc[pl.ds(tables + (k * 2 + 1) * PLANE, PLANE), ls] = w1

    with scope('own_tables'):
        for c in range(3):
            make_table(c, coord[c])

    def home_gid():
        v = iota((GROUPS, 1), 0)
        return gid(lax.rem(v, PLANE) // SIDE, rmod(v), v // PLANE)

    with scope('home_table'):
        carry = jnp.zeros((GROUPS, 1), F32)
        for blk in range(NBLK):
            ls = pl.ds(blk * LANES, LANES)
            member = jnp.zeros((GROUPS, LANES), F32)
            for j in range(TOP_K):
                member = jnp.where(idst[0, x, pl.ds(j, 1), ls] // 2 == home_gid(), 1.0, member)
            rank = dot(member.astype(BF16), tri) + carry
            carry = carry + over_lanes(member)
            slott[:, ls] = jnp.where(member > 0, rank, -1.0)

    for r in range(ROUNDS):
        mg[r] = jnp.zeros((SIDE, SIDE, 1, LANES), F32)

    def gather(c, k, pair):
        base = (iota((GS, 1), 0) + pair * GS).astype(F32)
        row = iota((GS, LANES), 0)
        at = iota((GS, LANES), 1) - k * RS - lax.rem(row, RS)
        for p in range(PLANE):
            mask = table(c, k, p)[...] == base
            pbuf[pl.ds(p * GS, GS), :] = onehot(mask)
            if c == 0:
                both = jnp.zeros((GS, LANES), F32)
                for e in range(2):
                    col = over_lanes(jnp.where(mask, gates(k, e, p)[...], 0.0))
                    both = jnp.where(at == e * LINE, col, both)
                for i in range(2):
                    line = over_rows(jnp.where(row // RS == i, both, 0.0))
                    mg[2 * pair + i, p // SIDE, p % SIDE] = mg[2 * pair + i, p // SIDE, p % SIDE] + line
        w = FWD[c][1]
        rows = dot(pbuf[...], gat[k, :, cols(c)]).astype(BF16).reshape(SIDE, SIDE, 2, RS, w)
        for i in range(2):
            if c == 2:
                snd[2 * pair + i, :, k, :, :, cols(c)] = rows[:, :, i]
            else:
                snd[2 * pair + i, :, :, k, :, cols(c)] = rows[:, :, i]

    wait(gat.at[0], loc_sem.at[1])

    hop_bufs = (ja, jb, jc)

    def hop_part(r, c, k):
        axis = AXES[c][0]
        for off in NEAR:
            to = rmod(coord[axis] + off)
            if c == 2:
                src, dst = snd.at[r, to, k, :, :, cols(c)], jc.at[r, k, coord[axis]]
            else:
                src, dst = snd.at[r, to, :, k, :, cols(c)], hop_bufs[c].at[r, coord[axis], :, k]
            remote(src, dst, fa_s.at[lax.rem(r, 2)], fa_r.at[r], along(axis, to)).start()

    def hop_dst(r, c):
        axis = AXES[c][0]
        return jc.at[r, :, coord[axis], :, :, :] if c == 2 else hop_bufs[c].at[r, coord[axis]]

    def hop_rest(r):
        for c in range(3):
            local(snd.at[r, coord[AXES[c][0]], :, :, :, cols(c)], hop_dst(r, c), fl.at[0, lax.rem(r, 2)]).start()
        for off in NEAR:
            to = rmod(y + off)
            remote(mg.at[r, to], jm.at[r, y], fm_s.at[lax.rem(r, 2)], fm_r.at[0, r], along(AXES[0][0], to)).start()
        jm[r, y] = mg[r, y]

    def plane_hop(r):
        for c in range(3):
            axis = AXES[c][0]
            for off in NEAR:
                to = rmod(coord[axis] + off)
                remote(snd.at[r, to, :, :, :, cols(c)], hop_dst(r, c), fa_s.at[lax.rem(r, 2)], fa_r.at[r], along(axis, to)).start()
        hop_rest(r)

    def part(c, k, h):
        return gat.at[k, pl.ds(h * HALF, HALF), cols(c)]

    def pass_on(r):
        odd = lax.rem(r, 2)
        with scope('wait_fa'):
            wait(blocks(3), fa_r.at[r])
        wait(blocks(1), fl.at[0, odd])
        wait(three_lines, fm_r.at[0, r])
        for c, buf in enumerate(hop_bufs):
            axis = AXES[c][1]
            dst = (rx.at[r, z, :, :, :, cols(c)], rx.at[r, :, :, x, :, cols(c)], rx.at[r, :, y, :, :, cols(c)])[c]
            for k in (*NEAR, 0):
                to = rmod(coord[axis] + k)
                src = buf.at[r, :, :, to] if c == 2 else buf.at[r, :, to]
                if k:
                    remote(src, dst, fb_s.at[0], fb_r.at[r], along(axis, to)).start()
                    if c == 0:
                        remote(jm.at[r, :, to], mr.at[l, r, z], fm_s.at[2], fm_r.at[1, r], along(axis, to)).start()
                else:
                    local(src, dst, fl.at[1, odd]).start()
        mr[l, r, z] = jm[r, :, z]
        wait(blocks(3), fa_s.at[odd])
        wait(three_lines, fm_s.at[odd])
        for p in neighbours:
            pl.semaphore_signal(free.at[r], inc=1, device_id={'grp': p, 'loc': l}, device_id_type=MESH)

    def own_part(r, early):
        for c, core in ((2, 0), (0, 1)):
            @pl.when(l == (core if early else 1 - core))
            def _():
                hop_part(r, c, coord[c])
        if not early:
            hop_part(r, 1, y)

    def before_near():
        for r in range(2):
            own_part(r, early=True)

        for sem in (meta_r, meta_s):
            wait(idst.at[:, first(3)], sem.at[0])
            wait(three_gates, sem.at[1])
        with scope('far_table'):
            def far_table(k, carry_):
                for c in range(3):
                    make_table(c, rmod(coord[c] + k))
                return carry_

            lax.fori_loop(1, SIDE, far_table, 0)

        for d, k in enumerate(BOTH):
            with scope('wait_g1'):
                wait(half_slab, g1_r.at[d, d])
            for c in range(3):
                src = part(c, rmod(coord[c] + SIDE - k), d)
                remote(src, src, g2_s.at[0], g2_r.at[d], along(c, rmod(coord[c] + k))).start()
        for d in range(2):
            with scope('wait_g1b'):
                wait(half_slab, g1_r.at[d, 1 - d])

    def before_second_near():
        own_part(0, early=False)
        for c in range(3):
            for k in BOTH:
                hop_part(0, c, rmod(coord[c] + k))

    def before_far():
        for d in range(2):
            with scope('wait_g2'):
                wait(half_slab, g2_r.at[d])

    def after_far():
        for c in range(3):
            hop_part(0, c, rmod(coord[c] + 2))
        hop_rest(0)
        own_part(1, early=False)
        for k in NEAR:
            for c in range(3):
                hop_part(1, c, rmod(coord[c] + k))
        hop_rest(1)

    events = ((3, before_near), (5, before_second_near), (7, before_far), (8, after_far))

    def gather_step(i, carry_):
        for at, event in events:
            @pl.when(i == at)
            def _():
                event()
        far = (i == 7) | (i == 8) | (i == 11)
        off = jnp.where(i < 3, 0, jnp.where(far, 2, jnp.where(lax.rem(i, 2) == 1, 3, 1)))
        pair = jnp.where(i < 3, i, jnp.where(i > 8, 2, jnp.where((i == 5) | (i == 6) | (i == 8), 1, 0)))
        with scope('gather'):
            for c in range(3):
                gather(c, rmod(coord[c] + off), pair)
        return carry_

    lax.fori_loop(0, SIDE * PAIRS, gather_step, 0)
    for r in range(2):
        with scope('pass_on'):
            pass_on(r)
        plane_hop(r + 2)
    wait(gat.at[0], g2_s.at[0])
    wait(gat.at[first(2)], g1_s.at[0])
    acc[...] = jnp.zeros_like(acc)
    wait(wgu, loc_sem.at[3])
    wait(wdn, loc_sem.at[4])

    mine = (iota((LINE, LANES), 1) == l * LINE + iota((LINE, LANES), 0))
    ubuf = gat.at[0, first(CH), pl.ds(D, D)]

    def result(kk, n=first(D)):
        return gat.at[kk, first(CH), n]

    def guest(r):
        return ROUNDS + lax.rem(r, 2)

    def chunk(r, kk):
        lp = jnp.where(kk == 0, l, other)
        slot = jnp.where(kk == 0, r, guest(r))

        def col(c0, w):
            return rx[slot, :, :, :, :, pl.ds(c0, w)].reshape(CH, w)

        for m in range(PLANE):
            zz, yy = m // SIDE, m % SIDE
            gcol = over_lanes(jnp.where(mine, mr[lp, r, zz, yy], 0.0))
            rows = rx[slot, zz, yy, :, :, pl.ds(D, D)].reshape(LINE, D)
            ubuf[pl.ds(m * LINE, LINE), :] = (gcol * rows.astype(F32)).astype(BF16)
        for h in range(2):
            hs = pl.ds(h * WIDE, WIDE)
            ab = dot(rx[slot, pl.ds(2 * h, 2), :, :, :, first(D)].reshape(WIDE, D), wgu[...])
            dh = dot(ubuf[hs, :], wdn[...], 1, 1)
            a = ab[:, :F]
            b = ab[:, F:]
            sig = jax.nn.sigmoid(a)
            silu = a * sig
            hd[hs, first(F)] = (silu * b).astype(BF16)
            hd[hs, pl.ds(F, F)] = (dh * b * sig * (1.0 + a * (1.0 - sig))).astype(BF16)
            hd[hs, pl.ds(2 * F, F)] = (dh * silu).astype(BF16)
        dg = jnp.zeros((CH, 1), F32)
        for n in range(4):
            o = dot(hd[:, first(F)], wdn[:, pl.ds(n * WIDE, WIDE)])
            dg = dg + over_lanes(col(D + n * WIDE, WIDE).astype(F32) * o)
        for m in range(PLANE):
            line = over_rows(jnp.where(mine, dg[m * LINE:(m + 1) * LINE, :], 0.0))
            dgb[kk, r, m // SIDE, m % SIDE] = line
        acc[first(F), :] += dot(hd[:, first(F)], ubuf[...], 0, 0)
        for i in (1, 2):
            acc[pl.ds(i * F, F), :] += dot(hd[:, pl.ds(i * F, F)], col(0, D), 0, 0)
        for n in range(4):
            cval = dot(hd[:, pl.ds(F, 2 * F)], wgu[pl.ds(n * WIDE, WIDE), :], 1, 1)
            result(kk, pl.ds(n * WIDE, WIDE))[...] = cval.astype(BF16)

    def home_first(r):
        pl.semaphore_wait(free.at[r], len(neighbours))
        for c in range(3):
            axis = AXES[c][1]
            cs = pl.ds(*BWD[c])
            dst = snd.at[r, coord[axis], :, :, :, pl.ds(D + BWD[c][0], BWD[c][1])]
            for k in (*NEAR, 0):
                to = rmod(coord[axis] + k)
                src = (rx.at[r, to, :, :, :, cs], rx.at[r, :, :, to, :, cs], rx.at[r, :, to, :, :, cs])[c]
                if k:
                    remote(src, dst, b_s.at[0], b_r.at[0, r], along(axis, to)).start()
                    if c == 0:
                        remote(dgb.at[0, r, to], km.at[r, z], bm_s.at[0], bm_r.at[0, r], along(axis, to)).start()
                else:
                    dst[...] = src[...]
        km[r, z] = dgb[0, r, z]

    def home_second(r):
        with scope('wait_ba'):
            wait(blocks(3, D), b_r.at[0, r])
        wait(three_lines, bm_r.at[0, r])
        for c, buf in enumerate((ia, ib, ic)):
            axis = AXES[c][0]
            dst = buf.at[r, coord[axis]] if c == 1 else buf.at[r, :, coord[axis]]
            cs = pl.ds(D + BWD[c][0], BWD[c][1])
            for k in (*NEAR, 0):
                to = rmod(coord[axis] + k)
                src = snd.at[r, :, :, to, :, cs] if c == 2 else snd.at[r, :, to, :, :, cs]
                if k:
                    remote(src, dst, b_s.at[1], b_r.at[1, r], along(axis, to)).start()
                    if c == 0:
                        remote(km.at[r, :, to], dgi.at[r, :, y], bm_s.at[1], bm_r.at[1, r], along(axis, to)).start()
                else:
                    local(src, dst, bl.at[0, r]).start()
        dgi[r, :, y] = km[r, :, y]

    def home_third(r):
        with scope('wait_bb'):
            wait(blocks(3, D), b_r.at[1, r])
        wait(blocks(1, D), bl.at[0, r])
        wait(three_lines, bm_r.at[1, r])
        for p in range(PLANE):
            dgj[r, pl.ds(p, 1), :] = dgi[r, p // SIDE, p % SIDE]
        for c, buf in enumerate((ia, ib, ic)):
            cs = pl.ds(*BWD[c])
            dst = (snd.at[r, :, :, x, :, cs], snd.at[r, :, y, :, :, cs], snd.at[r, z, :, :, :, cs])[c]
            for k in (*NEAR, 0):
                to = rmod(coord[c] + k)
                src = buf.at[r, :, :, to]
                if k:
                    if c == 0:
                        remote(dgj.at[r], dgh.at[r, x], bm_s.at[2], bm_r.at[2, r], along(c, to)).start()
                    remote(src, dst, b_s.at[2], b_r.at[2, r], along(c, to)).start()
                else:
                    local(src, dst, bl.at[1, r]).start()
        dgh[r, x] = dgj[r]

    start, mid, end = range(3)
    moves = ((2, end, home_second, 0), (3, end, home_second, 1), (4, mid, home_second, 2), (4, end, home_third, 0),
             (5, start, home_second, 3), (5, mid, home_third, 1), (5, end, home_second, 4), (5, end, home_third, 2))

    def move(r, place):
        for rr, at, hop, which in moves:
            if at == place:
                @pl.when(r == rr)
                def _():
                    with scope(f'{hop.__name__}{which}'):
                        hop(which)

    def round_body(r, carry_):
        with scope('wait_fb'):
            wait(blocks(3), fb_r.at[r])
        wait(blocks(1), fl.at[1, lax.rem(r, 2)])
        wait(three_lines, fm_r.at[1, r])
        remote(rx.at[r], rx.at[guest(r)], d2.at[0], d2.at[1], loc=other).start()
        remote(mr.at[l, r], mr.at[l, r], dm_s.at[0], dm_r.at[0], loc=other).start()
        move(r, start)

        def step(kk, carry2):
            @pl.when(kk == 1)
            def _():
                wait(rx.at[r], d2.at[0])
                pl.semaphore_signal(credit.at[0], inc=1, device_id={'grp': g, 'loc': other}, device_id_type=MESH)
                with scope('wait_d2'):
                    wait(rx.at[r], d2.at[1])
                wait(mr.at[other, r], dm_r.at[0])
                move(r, mid)

            with scope('chunk'):
                chunk(r, kk)
            return carry2

        lax.fori_loop(0, 2, step, 0)
        with scope('credit'):
            pl.semaphore_wait(credit.at[0], 1)

        @pl.when(r > 0)
        def _():
            wait(rx.at[r, :, :, :, :, first(D)], c_sem.at[0])

        mine_there = rx.at[guest(r), :, :, :, :, first(D)]
        mine_there[...] = result(1)[...].reshape(SIDE, SIDE, SIDE, RS, D)
        remote(mine_there, rx.at[r, :, :, :, :, pl.ds(D, D)], c_sem.at[0], c_sem.at[1], loc=other).start()
        remote(dgb.at[1, r], dgr.at[r], dm_s.at[1], dm_r.at[1], loc=other).start()

        @pl.when(r < ROUNDS - 2)
        def _():
            with scope('pass_on'):
                pass_on(r + 2)

        @pl.when(r < ROUNDS - 4)
        def _():
            plane_hop(r + 4)

        with scope('wait_c'):
            wait(rx.at[r, :, :, :, :, pl.ds(D, D)], c_sem.at[1])

        def add(zy, carry2):
            zz, yy = zy // SIDE, rmod(zy)
            p0 = gat[0, pl.ds(zy * LINE, LINE), first(D)].astype(F32).reshape(SIDE, RS, D)
            p1 = rx[r, zz, yy, :, :, pl.ds(D, D)].astype(F32)
            rx[r, zz, yy, :, :, first(D)] = (p0 + p1).astype(BF16)
            return carry2

        with scope('add'):
            lax.fori_loop(0, PLANE, add, 0)
        wait(dgr.at[r], dm_r.at[1])
        dgb[0, r] = dgb[0, r] + dgr[r]
        with scope('home_first'):
            home_first(r)
        move(r, end)
        return carry_

    lax.fori_loop(0, ROUNDS, round_body, 0)

    with scope('flush'):
        dwd_ref[...] = acc[first(F), :].astype(BF16)
        eye = onehot(iota((F, F), 0) == iota((F, F), 1))
        for i, out in enumerate((dwg_ref, dwu_ref)):
            for n in range(4):
                ns = pl.ds(n * WIDE, WIDE)
                out[ns, :] = dot(acc[pl.ds((i + 1) * F, F), ns].astype(BF16), eye, 0, 0).astype(BF16)
        dgacc[...] = jnp.zeros_like(dgacc)
        acc[first(TOK), :] = jnp.zeros((TOK, D), F32)
        slotn = slott[...].astype(BF16)
        at = iota((1, GROUPS * RS), 1) // RS
        spread = onehot(home_gid() == gid(at // PLANE, rmod(at // SIDE), rmod(at)))
    def pick(r):
        want = (lax.rem(iota((1, GROUPS * RS), 1), RS) + r * RS).astype(F32)
        for n in range(2):
            ns = pl.ds(n * WIDE, WIDE)
            got = dot(slotn, spread[:, n * WIDE:(n + 1) * WIDE], 0, 0)
            gat[0, :, ns] = onehot(got == want[:, n * WIDE:(n + 1) * WIDE])

    def gate_gradients(r):
        wait(three_planes, bm_r.at[2, r])
        for e in range(2):
            cur = dgacc[e]
            lines = jnp.zeros((GROUPS, RS), F32)
            for k in range(SIDE):
                mine_k = dgh[r, :, :, pl.ds(e * LINE + k * RS, RS)].reshape(GROUPS, RS)
                lines = jnp.where(x == k, mine_k, lines)
            for i in range(RS):
                cur = jnp.where(slott[...] == jnp.float32(r * RS + i), lines[:, i:i + 1], cur)
            dgacc[e] = cur

    def arrived(r):
        with scope('wait_bc'):
            wait(blocks(3, D), b_r.at[2, r])
        wait(blocks(1, D), bl.at[1, r])

    def summed(r, ns):
        return acc[first(TOK), ns] + dot(gat[0, :, first(GROUPS * RS)], snd[r, :, :, :, :, ns].reshape(GROUPS * RS, WIDE))

    tail = ((1, home_second, 5), (1, home_third, 3), (2, home_third, 4), (3, home_third, 5))

    def last(r, carry_):
        for at, hop, which in tail:
            @pl.when(r == at)
            def _():
                with scope(f'{hop.__name__}{which}'):
                    hop(which)
        with scope('pick'):
            pick(r)
        with scope('dg'):
            gate_gradients(r)
        arrived(r)
        with scope('combine'):
            for n in range(4):
                ns = pl.ds(n * WIDE, WIDE)
                acc[first(TOK), ns] = summed(r, ns)
        return carry_

    lax.fori_loop(0, ROUNDS - 1, last, 0)
    with scope('pick'):
        pick(ROUNDS - 1)
    with scope('drain'):
        wait(snd.at[:, first(3)], fb_s.at[0])
        wait(mg.at[:, first(3)], fm_s.at[2])
        for i in range(2):
            wait(snd.at[:, first(3), :, :, :, first(D)], b_s.at[i])
            wait(mg.at[:, first(3)], bm_s.at[i])
        wait(rx.at[0, :, :, :, :, first(D)], c_sem.at[0])
        wait(mr.at[0], dm_s.at[0])
        wait(dgr, dm_s.at[1])
    with scope('dg'):
        gate_gradients(ROUNDS - 1)
        for j in range(TOP_K):
            idj = idst[0, x, pl.ds(j, 1), :]
            val = jnp.where(lax.rem(idj, 2) == 0, dgacc[0], dgacc[1])
            dgate_ref[pl.ds(j, 1), :] = over_rows(jnp.where(idj // 2 == home_gid(), val, 0.0))
    arrived(ROUNDS - 1)
    with scope('finish'):
        for n in range(4):
            ns = pl.ds(n * WIDE, WIDE)
            dx_ref[:, ns] = summed(ROUNDS - 1, ns).astype(BF16)
        wait(dgh.at[:, first(3)], bm_s.at[2])
        wait(snd.at[:, first(3), :, :, :, first(D)], b_s.at[2])


def hand_over(*refs):
    n = len(refs) // 3
    copies = [pltpu.make_async_copy(a, b, sem) for a, b, sem in zip(refs[:n], refs[n:2 * n], refs[2 * n:])]
    for cp in copies:
        cp.start()
    for cp in copies:
        cp.wait()


def solution(mesh):
    spec = P(('part', 'grp', 'loc'))

    def device_step(x_rows, dy_rows, expert_ids, gate_vals, w_gate, w_up, w_down):
        any_ = pl.BlockSpec(memory_space=pl.ANY)
        vmem = pl.BlockSpec(memory_space=pltpu.VMEM)
        dma = pltpu.SemaphoreType.DMA
        one, two, three, per_round = (dma((n,)) for n in (1, 2, 3, ROUNDS))
        sd = jax.ShapeDtypeStruct
        results = [sd((TOK, D), BF16), sd((TOP_K, TOK), F32), *[sd((D, F), BF16)] * 2, sd((F, D), BF16)]
        cube = (ROUNDS, SIDE, SIDE, SIDE, RS)
        lines = (ROUNDS, SIDE, SIDE, 1, LANES)
        out = pl.pallas_call(
            kernel,
            name='moe_backward',
            in_specs=[any_] * 7,
            out_specs=[vmem] * 5 + [any_] * 6,
            out_shape=[*[pltpu.VMEM(o.shape, o.dtype) for o in results], *[sd((*cube, w), BF16) for _, w in FWD + BWD]],
            scratch_shapes=[
                pltpu.VMEM((SIDE, TOK, 2 * D), BF16),
                pltpu.VMEM((*cube, 2 * D), BF16),
                pltpu.VMEM((ROUNDS + 2, SIDE, SIDE, SIDE, RS, 2 * D), BF16),
                pltpu.VMEM((D, 2 * F), BF16),
                pltpu.VMEM((F, D), BF16),
                pltpu.VMEM((3 * F, D), F32),
                pltpu.VMEM((CH, 3 * F), BF16),
                pltpu.VMEM((PLANE * GS, TOK), BF16),
                pltpu.VMEM((GROUPS, TOK), F32),
                pltpu.VMEM((3, SIDE, TOP_K, TOK), jnp.int32),
                pltpu.VMEM((SIDE, TOP_K, TOK), F32),
                pltpu.VMEM(lines, F32),
                pltpu.VMEM(lines, F32),
                pltpu.VMEM((2, *lines), F32),
                pltpu.VMEM((2, *lines), F32),
                pltpu.VMEM(lines, F32),
                pltpu.VMEM(lines, F32),
                pltpu.VMEM(lines, F32),
                pltpu.VMEM((ROUNDS, PLANE, LANES), F32),
                pltpu.VMEM((ROUNDS, SIDE, PLANE, LANES), F32),
                pltpu.VMEM((2, GROUPS, TOK), F32),
                dma((5,)), two, two, one, dma((2, 2)), one, two, two, per_round, one, per_round, dma((2, 2)), three,
                dma((2, ROUNDS)), *[two] * 4, three, dma((3, ROUNDS)), dma((2, ROUNDS)), three, dma((3, ROUNDS)),
                pltpu.SemaphoreType.REGULAR((1,)), pltpu.SemaphoreType.REGULAR((ROUNDS,)),
            ],
            compiler_params=pltpu.CompilerParams(collective_id=0, has_side_effects=True, vmem_limit_bytes=60 << 20),
        )(x_rows, dy_rows, expert_ids.T, gate_vals.T, w_gate[0], w_up[0], w_down[0])
        dx, d_gates, dwg, dwu, dwd = pl.pallas_call(
            hand_over,
            name='hand_over',
            in_specs=[vmem] * 5,
            out_specs=[any_] * 5,
            out_shape=results,
            scratch_shapes=[pltpu.SemaphoreType.DMA] * 5,
            compiler_params=pltpu.CompilerParams(vmem_limit_bytes=1 << 20),
        )(*[pltpu.with_memory_space_constraint(o, pltpu.VMEM) for o in out[:5]])
        return dx, d_gates.T, dwg[None], dwu[None], dwd[None]

    return jax.shard_map(device_step, mesh=mesh, in_specs=(spec,) * 7, out_specs=(spec,) * 5, check_vma=False)
```

```python
import jax
import jax.numpy as jnp
from jax import lax
from jax.experimental import pallas as pl
from jax.experimental.pallas import tpu as pltpu
from jax.sharding import PartitionSpec as P

MESH = pl.DeviceIdType.MESH
F32 = jnp.float32
BF16 = jnp.bfloat16
LANES = 128
WIDE = 256
SIDE = 4
PLANE = SIDE * SIDE
GROUPS = SIDE ** 3
TOK = 768
HALF = TOK // 2
TOP_K = 8
D = 1024
F = 384
SLOTS = 48
ROUNDS = 6
PAIRS = ROUNDS // 2
RS = SLOTS // ROUNDS
GS = 2 * RS
LINE = SIDE * RS
CH = GROUPS * RS
NBLK = TOK // LANES
FWD = ((0, 640), (640, 640), (1280, 768))
BWD = ((0, 384), (384, 384), (768, 256))
AXES = ((1, 2), (2, 0), (0, 1))
NEAR = (1, 3, 2)
BOTH = (1, 3)
scope = jax.named_scope


def dot(a, b, ca=1, cb=0):
    return lax.dot_general(a, b, (((ca,), (cb,)), ((), ())), preferred_element_type=F32)


def first(n):
    return pl.ds(0, n)


def over_lanes(v):
    return jnp.sum(v, axis=1, keepdims=True)


def over_rows(v):
    return jnp.sum(v, axis=0, keepdims=True)


def iota(shape, dim):
    return lax.broadcasted_iota(jnp.int32, shape, dim)


def onehot(mask):
    return mask.astype(F32).astype(BF16)


def kernel(x_hbm, dy_hbm, idst_hbm, gatt_hbm, wg_hbm, wu_hbm, wd_hbm,
           dx_ref, dgate_ref, dwg_ref, dwu_ref, dwd_ref, ja, jb, jc, ia, ib, ic,
           gat, snd, rx, wgu, wdn, acc, hd, pbuf, slott, idst, gatt, mg, jm, mr, dgb, dgr, km, dgi, dgj, dgh, dgacc,
           loc_sem, meta_s, meta_r, g1_s, g1_r, g2_s, g2_r, fa_s, fa_r, fb_s, fb_r, fl, fm_s, fm_r,
           d2, c_sem, dm_s, dm_r, b_s, b_r, bl, bm_s, bm_r, credit, free):
    g = lax.axis_index('grp')
    l = lax.axis_index('loc')
    cz, cy, cx = g // PLANE, (g // SIDE) % SIDE, g % SIDE
    x, y, z = cx + l * (cz - cx), cy + l * (cx - cy), cz + l * (cy - cz)
    step_x, step_y, step_z = 1 + l * (PLANE - 1), SIDE + l * (1 - SIDE), PLANE + l * (SIDE - PLANE)
    coord = (x, y, z)
    other = 1 - l

    def rmod(v):
        return lax.rem(v, SIDE)

    def gid(zz, yy, xx):
        return zz * step_z + yy * step_y + xx * step_x

    def along(axis, k):
        return gid(*(k if a == axis else coord[a] for a in (2, 1, 0)))

    def in_plane(c, a, b):
        at = {c: coord[c], AXES[c][0]: a, AXES[c][1]: b}
        return gid(at[2], at[1], at[0])

    def remote(src, dst, ss, rs, grp=g, loc=l):
        return pltpu.make_async_remote_copy(src, dst, ss, rs, device_id={'grp': grp, 'loc': loc}, device_id_type=MESH)

    def local(src, dst, sem):
        return pltpu.make_async_copy(src, dst, sem)

    def wait(ref, sem):
        local(ref, ref, sem).wait()

    three_lines, three_planes, three_gates = mg.at[0, first(3)], dgh.at[0, first(3)], gatt.at[first(3)]
    half_slab = gat.at[0, first(HALF)]

    def blocks(n, w=2 * D):
        return snd.at[0, first(n), :, :, :, first(w)]

    neighbours = [along(axis, rmod(coord[axis] + k)) for axis in range(3) for k in NEAR]

    barrier = pltpu.get_barrier_semaphore()
    for p in neighbours:
        pl.semaphore_signal(barrier, inc=1, device_id={'grp': p, 'loc': l}, device_id_type=MESH)
    pl.semaphore_signal(barrier, inc=1, device_id={'grp': g, 'loc': other}, device_id_type=MESH)

    def slab_copies(c, rows, make):
        c0, w = FWD[c]
        out = []
        if c0 < D:
            n = min(w, D - c0)
            out.append(make(x_hbm.at[rows, pl.ds(c0, n)], pl.ds(c0, n)))
        if c0 + w > D:
            s = max(c0, D)
            out.append(make(dy_hbm.at[rows, pl.ds(s - D, c0 + w - s)], pl.ds(s, c0 + w - s)))
        return out

    def cols(c):
        return pl.ds(*FWD[c])

    def own_slab(c):
        return slab_copies(c, first(TOK), lambda src, cs: local(src, gat.at[coord[c], :, cs], loc_sem.at[1]))

    routing = [local(idst_hbm, idst.at[c, coord[c]], loc_sem.at[0]) for c in range(3)]
    routing.append(local(gatt_hbm, gatt.at[x], loc_sem.at[2]))
    weights = [local(wg_hbm, wgu.at[:, first(F)], loc_sem.at[3]), local(wu_hbm, wgu.at[:, pl.ds(F, F)], loc_sem.at[3]),
               local(wd_hbm, wdn, loc_sem.at[4])]
    for cp in routing + own_slab(0) + own_slab(1) + own_slab(2) + weights:
        cp.start()
    with scope('entry'):
        pl.semaphore_wait(barrier, len(neighbours) + 1)

    def slab_send(i):
        for d, k in enumerate(BOTH):
            h = (d + i) % 2
            rows = pl.ds(h * HALF, HALF)
            for c in range(3):
                t = along(c, rmod(coord[c] + k))
                for cp in slab_copies(c, rows, lambda src, cs: remote(src, gat.at[coord[c], rows, cs], g1_s.at[0],
                                                                      g1_r.at[d, h], t)):
                    cp.start()

    slab_send(0)
    for c in range(3):
        for k in NEAR:
            t = along(c, rmod(coord[c] + k))
            remote(idst_hbm, idst.at[c, coord[c]], meta_s.at[0], meta_r.at[0], t).start()
            if c == 0:
                remote(gatt_hbm, gatt.at[x], meta_s.at[1], meta_r.at[1], t).start()
    slab_send(1)
    wait(idst.at[:, 0], loc_sem.at[0])
    wait(gatt.at[0], loc_sem.at[2])

    tri = onehot(iota((LANES, LANES), 0) < iota((LANES, LANES), 1))
    tables = 3 * SIDE * PLANE

    def table(c, k, p):
        return acc.at[pl.ds((c * SIDE + k) * PLANE + p, 1), first(TOK)]

    def gates(k, e, p):
        return acc.at[pl.ds(tables + (k * 2 + e) * PLANE + p, 1), first(TOK)]

    def make_table(c, k):
        p = iota((PLANE, 1), 0)
        gids = in_plane(c, p // SIDE, rmod(p))
        carry = jnp.zeros((PLANE, 1), F32)
        for blk in range(NBLK):
            ls = pl.ds(blk * LANES, LANES)
            ids = idst[c, k, :, ls]
            member = jnp.zeros((PLANE, LANES), F32)
            w0 = jnp.zeros((PLANE, LANES), F32)
            w1 = jnp.zeros((PLANE, LANES), F32)
            for j in range(TOP_K):
                idj = ids[j:j + 1, :]
                e0 = idj == 2 * gids
                e1 = idj == 2 * gids + 1
                member = jnp.where(e0 | e1, 1.0, member)
                if c == 0:
                    gj = gatt[k, pl.ds(j, 1), ls]
                    w0 = jnp.where(e0, gj, w0)
                    w1 = jnp.where(e1, gj, w1)
            rank = dot(member.astype(BF16), tri) + carry
            carry = carry + over_lanes(member)
            acc[pl.ds((c * SIDE + k) * PLANE, PLANE), ls] = jnp.where(member > 0, rank, -1.0)
            if c == 0:
                acc[pl.ds(tables + k * 2 * PLANE, PLANE), ls] = w0
                acc[pl.ds(tables + (k * 2 + 1) * PLANE, PLANE), ls] = w1

    with scope('own_tables'):
        for c in range(3):
            make_table(c, coord[c])

    def home_gid():
        v = iota((GROUPS, 1), 0)
        return gid(lax.rem(v, PLANE) // SIDE, rmod(v), v // PLANE)

    with scope('home_table'):
        carry = jnp.zeros((GROUPS, 1), F32)
        for blk in range(NBLK):
            ls = pl.ds(blk * LANES, LANES)
            member = jnp.zeros((GROUPS, LANES), F32)
            for j in range(TOP_K):
                member = jnp.where(idst[0, x, pl.ds(j, 1), ls] // 2 == home_gid(), 1.0, member)
            rank = dot(member.astype(BF16), tri) + carry
            carry = carry + over_lanes(member)
            slott[:, ls] = jnp.where(member > 0, rank, -1.0)

    for r in range(ROUNDS):
        mg[r] = jnp.zeros((SIDE, SIDE, 1, LANES), F32)

    def gather(c, k, pair):
        base = (iota((GS, 1), 0) + pair * GS).astype(F32)
        row = iota((GS, LANES), 0)
        at = iota((GS, LANES), 1) - k * RS - lax.rem(row, RS)
        for p in range(PLANE):
            mask = table(c, k, p)[...] == base
            pbuf[pl.ds(p * GS, GS), :] = onehot(mask)
            if c == 0:
                both = jnp.zeros((GS, LANES), F32)
                for e in range(2):
                    col = over_lanes(jnp.where(mask, gates(k, e, p)[...], 0.0))
                    both = jnp.where(at == e * LINE, col, both)
                for i in range(2):
                    line = over_rows(jnp.where(row // RS == i, both, 0.0))
                    mg[2 * pair + i, p // SIDE, p % SIDE] = mg[2 * pair + i, p // SIDE, p % SIDE] + line
        w = FWD[c][1]
        rows = dot(pbuf[...], gat[k, :, cols(c)]).astype(BF16).reshape(SIDE, SIDE, 2, RS, w)
        for i in range(2):
            if c == 2:
                snd[2 * pair + i, :, k, :, :, cols(c)] = rows[:, :, i]
            else:
                snd[2 * pair + i, :, :, k, :, cols(c)] = rows[:, :, i]

    wait(gat.at[0], loc_sem.at[1])

    hop_bufs = (ja, jb, jc)

    def hop_part(r, c, k):
        axis = AXES[c][0]
        for off in NEAR:
            to = rmod(coord[axis] + off)
            if c == 2:
                src, dst = snd.at[r, to, k, :, :, cols(c)], jc.at[r, k, coord[axis]]
            else:
                src, dst = snd.at[r, to, :, k, :, cols(c)], hop_bufs[c].at[r, coord[axis], :, k]
            remote(src, dst, fa_s.at[lax.rem(r, 2)], fa_r.at[r], along(axis, to)).start()

    def hop_dst(r, c):
        axis = AXES[c][0]
        return jc.at[r, :, coord[axis], :, :, :] if c == 2 else hop_bufs[c].at[r, coord[axis]]

    def hop_rest(r):
        for c in range(3):
            local(snd.at[r, coord[AXES[c][0]], :, :, :, cols(c)], hop_dst(r, c), fl.at[0, lax.rem(r, 2)]).start()
        for off in NEAR:
            to = rmod(y + off)
            remote(mg.at[r, to], jm.at[r, y], fm_s.at[lax.rem(r, 2)], fm_r.at[0, r], along(AXES[0][0], to)).start()
        jm[r, y] = mg[r, y]

    def plane_hop(r):
        for c in range(3):
            axis = AXES[c][0]
            for off in NEAR:
                to = rmod(coord[axis] + off)
                remote(snd.at[r, to, :, :, :, cols(c)], hop_dst(r, c), fa_s.at[lax.rem(r, 2)], fa_r.at[r], along(axis, to)).start()
        hop_rest(r)

    def part(c, k, h):
        return gat.at[k, pl.ds(h * HALF, HALF), cols(c)]

    def pass_on(r):
        odd = lax.rem(r, 2)
        with scope('wait_fa'):
            wait(blocks(3), fa_r.at[r])
        wait(blocks(1), fl.at[0, odd])
        wait(three_lines, fm_r.at[0, r])
        for c, buf in enumerate(hop_bufs):
            axis = AXES[c][1]
            dst = (rx.at[r, z, :, :, :, cols(c)], rx.at[r, :, :, x, :, cols(c)], rx.at[r, :, y, :, :, cols(c)])[c]
            for k in (*NEAR, 0):
                to = rmod(coord[axis] + k)
                src = buf.at[r, :, :, to] if c == 2 else buf.at[r, :, to]
                if k:
                    remote(src, dst, fb_s.at[0], fb_r.at[r], along(axis, to)).start()
                    if c == 0:
                        remote(jm.at[r, :, to], mr.at[l, r, z], fm_s.at[2], fm_r.at[1, r], along(axis, to)).start()
                else:
                    local(src, dst, fl.at[1, odd]).start()
        mr[l, r, z] = jm[r, :, z]
        wait(blocks(3), fa_s.at[odd])
        wait(three_lines, fm_s.at[odd])
        for p in neighbours:
            pl.semaphore_signal(free.at[r], inc=1, device_id={'grp': p, 'loc': l}, device_id_type=MESH)

    def own_part(r, early):
        for c, core in ((2, 0), (0, 1)):
            @pl.when(l == (core if early else 1 - core))
            def _():
                hop_part(r, c, coord[c])
        if not early:
            hop_part(r, 1, y)

    def before_near():
        for r in range(2):
            own_part(r, early=True)

        for sem in (meta_r, meta_s):
            wait(idst.at[:, first(3)], sem.at[0])
            wait(three_gates, sem.at[1])
        with scope('far_table'):
            def far_table(k, carry_):
                for c in range(3):
                    make_table(c, rmod(coord[c] + k))
                return carry_

            lax.fori_loop(1, SIDE, far_table, 0)

        for d, k in enumerate(BOTH):
            with scope('wait_g1'):
                wait(half_slab, g1_r.at[d, d])
            for c in range(3):
                src = part(c, rmod(coord[c] + SIDE - k), d)
                remote(src, src, g2_s.at[0], g2_r.at[d], along(c, rmod(coord[c] + k))).start()
        for d in range(2):
            with scope('wait_g1b'):
                wait(half_slab, g1_r.at[d, 1 - d])

    def before_second_near():
        own_part(0, early=False)
        for c in range(3):
            for k in BOTH:
                hop_part(0, c, rmod(coord[c] + k))

    def before_far():
        for d in range(2):
            with scope('wait_g2'):
                wait(half_slab, g2_r.at[d])

    def after_far():
        for c in range(3):
            hop_part(0, c, rmod(coord[c] + 2))
        hop_rest(0)
        own_part(1, early=False)
        for k in NEAR:
            for c in range(3):
                hop_part(1, c, rmod(coord[c] + k))
        hop_rest(1)

    events = ((3, before_near), (5, before_second_near), (7, before_far), (8, after_far))

    def gather_step(i, carry_):
        for at, event in events:
            @pl.when(i == at)
            def _():
                event()
        far = (i == 7) | (i == 8) | (i == 11)
        off = jnp.where(i < 3, 0, jnp.where(far, 2, jnp.where(lax.rem(i, 2) == 1, 3, 1)))
        pair = jnp.where(i < 3, i, jnp.where(i > 8, 2, jnp.where((i == 5) | (i == 6) | (i == 8), 1, 0)))
        with scope('gather'):
            for c in range(3):
                gather(c, rmod(coord[c] + off), pair)
        return carry_

    lax.fori_loop(0, SIDE * PAIRS, gather_step, 0)
    for r in range(2):
        with scope('pass_on'):
            pass_on(r)
        plane_hop(r + 2)
    wait(gat.at[0], g2_s.at[0])
    wait(gat.at[first(2)], g1_s.at[0])
    acc[...] = jnp.zeros_like(acc)
    wait(wgu, loc_sem.at[3])
    wait(wdn, loc_sem.at[4])

    mine = (iota((LINE, LANES), 1) == l * LINE + iota((LINE, LANES), 0))
    ubuf = gat.at[0, first(CH), pl.ds(D, D)]

    def result(kk, n=first(D)):
        return gat.at[kk, first(CH), n]

    def guest(r):
        return ROUNDS + lax.rem(r, 2)

    def chunk(r, kk):
        lp = jnp.where(kk == 0, l, other)
        slot = jnp.where(kk == 0, r, guest(r))

        def col(c0, w):
            return rx[slot, :, :, :, :, pl.ds(c0, w)].reshape(CH, w)

        for m in range(PLANE):
            zz, yy = m // SIDE, m % SIDE
            gcol = over_lanes(jnp.where(mine, mr[lp, r, zz, yy], 0.0))
            rows = rx[slot, zz, yy, :, :, pl.ds(D, D)].reshape(LINE, D)
            ubuf[pl.ds(m * LINE, LINE), :] = (gcol * rows.astype(F32)).astype(BF16)
        for h in range(2):
            hs = pl.ds(h * WIDE, WIDE)
            ab = dot(rx[slot, pl.ds(2 * h, 2), :, :, :, first(D)].reshape(WIDE, D), wgu[...])
            dh = dot(ubuf[hs, :], wdn[...], 1, 1)
            a = ab[:, :F]
            b = ab[:, F:]
            sig = jax.nn.sigmoid(a)
            silu = a * sig
            hd[hs, first(F)] = (silu * b).astype(BF16)
            hd[hs, pl.ds(F, F)] = (dh * b * sig * (1.0 + a * (1.0 - sig))).astype(BF16)
            hd[hs, pl.ds(2 * F, F)] = (dh * silu).astype(BF16)
        dg = jnp.zeros((CH, 1), F32)
        for n in range(4):
            o = dot(hd[:, first(F)], wdn[:, pl.ds(n * WIDE, WIDE)])
            dg = dg + over_lanes(col(D + n * WIDE, WIDE).astype(F32) * o)
        for m in range(PLANE):
            line = over_rows(jnp.where(mine, dg[m * LINE:(m + 1) * LINE, :], 0.0))
            dgb[kk, r, m // SIDE, m % SIDE] = line
        acc[first(F), :] += dot(hd[:, first(F)], ubuf[...], 0, 0)
        for i in (1, 2):
            acc[pl.ds(i * F, F), :] += dot(hd[:, pl.ds(i * F, F)], col(0, D), 0, 0)
        for n in range(4):
            cval = dot(hd[:, pl.ds(F, 2 * F)], wgu[pl.ds(n * WIDE, WIDE), :], 1, 1)
            result(kk, pl.ds(n * WIDE, WIDE))[...] = cval.astype(BF16)

    def home_first(r):
        pl.semaphore_wait(free.at[r], len(neighbours))
        for c in range(3):
            axis = AXES[c][1]
            cs = pl.ds(*BWD[c])
            dst = snd.at[r, coord[axis], :, :, :, pl.ds(D + BWD[c][0], BWD[c][1])]
            for k in (*NEAR, 0):
                to = rmod(coord[axis] + k)
                src = (rx.at[r, to, :, :, :, cs], rx.at[r, :, :, to, :, cs], rx.at[r, :, to, :, :, cs])[c]
                if k:
                    remote(src, dst, b_s.at[0], b_r.at[0, r], along(axis, to)).start()
                    if c == 0:
                        remote(dgb.at[0, r, to], km.at[r, z], bm_s.at[0], bm_r.at[0, r], along(axis, to)).start()
                else:
                    dst[...] = src[...]
        km[r, z] = dgb[0, r, z]

    def home_second(r):
        with scope('wait_ba'):
            wait(blocks(3, D), b_r.at[0, r])
        wait(three_lines, bm_r.at[0, r])
        for c, buf in enumerate((ia, ib, ic)):
            axis = AXES[c][0]
            dst = buf.at[r, coord[axis]] if c == 1 else buf.at[r, :, coord[axis]]
            cs = pl.ds(D + BWD[c][0], BWD[c][1])
            for k in (*NEAR, 0):
                to = rmod(coord[axis] + k)
                src = snd.at[r, :, :, to, :, cs] if c == 2 else snd.at[r, :, to, :, :, cs]
                if k:
                    remote(src, dst, b_s.at[1], b_r.at[1, r], along(axis, to)).start()
                    if c == 0:
                        remote(km.at[r, :, to], dgi.at[r, :, y], bm_s.at[1], bm_r.at[1, r], along(axis, to)).start()
                else:
                    local(src, dst, bl.at[0, lax.rem(r, 3)]).start()
        dgi[r, :, y] = km[r, :, y]

    def home_third(r):
        with scope('wait_bb'):
            wait(blocks(3, D), b_r.at[1, r])
        wait(blocks(1, D), bl.at[0, lax.rem(r, 3)])
        wait(three_lines, bm_r.at[1, r])
        for p in range(PLANE):
            dgj[r, pl.ds(p, 1), :] = dgi[r, p // SIDE, p % SIDE]
        for c, buf in enumerate((ia, ib, ic)):
            cs = pl.ds(*BWD[c])
            dst = (snd.at[r, :, :, x, :, cs], snd.at[r, :, y, :, :, cs], snd.at[r, z, :, :, :, cs])[c]
            for k in (*NEAR, 0):
                to = rmod(coord[c] + k)
                src = buf.at[r, :, :, to]
                if k:
                    if c == 0:
                        remote(dgj.at[r], dgh.at[r, x], bm_s.at[2], bm_r.at[2, r], along(c, to)).start()
                    remote(src, dst, b_s.at[2], b_r.at[2, r], along(c, to)).start()
                else:
                    local(src, dst, bl.at[1, lax.rem(r, 3)]).start()
        dgh[r, x] = dgj[r]

    start, mid, end = range(3)
    moves = ((2, end, home_second, 0), (3, end, home_second, 1), (4, mid, home_second, 2), (4, end, home_third, 0),
             (5, start, home_second, 3), (5, mid, home_third, 1), (5, end, home_second, 4), (5, end, home_third, 2))

    def move(r, place):
        for rr, at, hop, which in moves:
            if at == place:
                @pl.when(r == rr)
                def _():
                    with scope(f'{hop.__name__}{which}'):
                        hop(which)

    def round_body(r, carry_):
        with scope('wait_fb'):
            wait(blocks(3), fb_r.at[r])
        wait(blocks(1), fl.at[1, lax.rem(r, 2)])
        wait(three_lines, fm_r.at[1, r])
        remote(rx.at[r], rx.at[guest(r)], d2.at[0], d2.at[1], loc=other).start()
        remote(mr.at[l, r], mr.at[l, r], dm_s.at[0], dm_r.at[0], loc=other).start()
        move(r, start)

        def step(kk, carry2):
            @pl.when(kk == 1)
            def _():
                wait(rx.at[r], d2.at[0])
                pl.semaphore_signal(credit.at[0], inc=1, device_id={'grp': g, 'loc': other}, device_id_type=MESH)
                with scope('wait_d2'):
                    wait(rx.at[r], d2.at[1])
                wait(mr.at[other, r], dm_r.at[0])
                move(r, mid)

            with scope('chunk'):
                chunk(r, kk)
            return carry2

        lax.fori_loop(0, 2, step, 0)
        with scope('credit'):
            pl.semaphore_wait(credit.at[0], 1)

        @pl.when(r > 0)
        def _():
            wait(rx.at[r, :, :, :, :, first(D)], c_sem.at[0])

        mine_there = rx.at[guest(r), :, :, :, :, first(D)]
        mine_there[...] = result(1)[...].reshape(SIDE, SIDE, SIDE, RS, D)
        remote(mine_there, rx.at[r, :, :, :, :, pl.ds(D, D)], c_sem.at[0], c_sem.at[1], loc=other).start()
        remote(dgb.at[1, r], dgr.at[r], dm_s.at[1], dm_r.at[1], loc=other).start()

        @pl.when(r < ROUNDS - 2)
        def _():
            with scope('pass_on'):
                pass_on(r + 2)

        @pl.when(r < ROUNDS - 4)
        def _():
            plane_hop(r + 4)

        with scope('wait_c'):
            wait(rx.at[r, :, :, :, :, pl.ds(D, D)], c_sem.at[1])

        def add(zy, carry2):
            zz, yy = zy // SIDE, rmod(zy)
            p0 = gat[0, pl.ds(zy * LINE, LINE), first(D)].astype(F32).reshape(SIDE, RS, D)
            p1 = rx[r, zz, yy, :, :, pl.ds(D, D)].astype(F32)
            rx[r, zz, yy, :, :, first(D)] = (p0 + p1).astype(BF16)
            return carry2

        with scope('add'):
            lax.fori_loop(0, PLANE, add, 0)
        wait(dgr.at[r], dm_r.at[1])
        dgb[0, r] = dgb[0, r] + dgr[r]
        with scope('home_first'):
            home_first(r)
        move(r, end)
        return carry_

    lax.fori_loop(0, ROUNDS, round_body, 0)

    with scope('flush'):
        dwd_ref[...] = acc[first(F), :].astype(BF16)
        eye = onehot(iota((F, F), 0) == iota((F, F), 1))
        for i, out in enumerate((dwg_ref, dwu_ref)):
            for n in range(4):
                ns = pl.ds(n * WIDE, WIDE)
                out[ns, :] = dot(acc[pl.ds((i + 1) * F, F), ns].astype(BF16), eye, 0, 0).astype(BF16)
        dgacc[...] = jnp.zeros_like(dgacc)
        acc[first(TOK), :] = jnp.zeros((TOK, D), F32)
        slotn = slott[...].astype(BF16)
        at = iota((1, GROUPS * RS), 1) // RS
        spread = onehot(home_gid() == gid(at // PLANE, rmod(at // SIDE), rmod(at)))
    def pick(r):
        want = (lax.rem(iota((1, GROUPS * RS), 1), RS) + r * RS).astype(F32)
        for n in range(2):
            ns = pl.ds(n * WIDE, WIDE)
            got = dot(slotn, spread[:, n * WIDE:(n + 1) * WIDE], 0, 0)
            gat[0, :, ns] = onehot(got == want[:, n * WIDE:(n + 1) * WIDE])

    def gate_gradients(r):
        wait(three_planes, bm_r.at[2, r])
        for e in range(2):
            cur = dgacc[e]
            lines = jnp.zeros((GROUPS, RS), F32)
            for k in range(SIDE):
                mine_k = dgh[r, :, :, pl.ds(e * LINE + k * RS, RS)].reshape(GROUPS, RS)
                lines = jnp.where(x == k, mine_k, lines)
            for i in range(RS):
                cur = jnp.where(slott[...] == jnp.float32(r * RS + i), lines[:, i:i + 1], cur)
            dgacc[e] = cur

    def arrived(r):
        with scope('wait_bc'):
            wait(blocks(3, D), b_r.at[2, r])
        wait(blocks(1, D), bl.at[1, lax.rem(r, 3)])

    def summed(r, ns):
        return acc[first(TOK), ns] + dot(gat[0, :, first(GROUPS * RS)], snd[r, :, :, :, :, ns].reshape(GROUPS * RS, WIDE))

    tail = ((1, home_second, 5), (1, home_third, 3), (2, home_third, 4), (3, home_third, 5))

    def last(r, carry_):
        for at, hop, which in tail:
            @pl.when(r == at)
            def _():
                with scope(f'{hop.__name__}{which}'):
                    hop(which)
        with scope('pick'):
            pick(r)
        with scope('dg'):
            gate_gradients(r)
        arrived(r)
        with scope('combine'):
            for n in range(4):
                ns = pl.ds(n * WIDE, WIDE)
                acc[first(TOK), ns] = summed(r, ns)
        return carry_

    lax.fori_loop(0, ROUNDS - 1, last, 0)
    with scope('pick'):
        pick(ROUNDS - 1)
    with scope('drain'):
        wait(snd.at[:, first(3)], fb_s.at[0])
        wait(mg.at[:, first(3)], fm_s.at[2])
        for i in range(2):
            wait(snd.at[:, first(3), :, :, :, first(D)], b_s.at[i])
            wait(mg.at[:, first(3)], bm_s.at[i])
        wait(rx.at[0, :, :, :, :, first(D)], c_sem.at[0])
        wait(mr.at[0], dm_s.at[0])
        wait(dgr, dm_s.at[1])
    with scope('dg'):
        gate_gradients(ROUNDS - 1)
        for j in range(TOP_K):
            idj = idst[0, x, pl.ds(j, 1), :]
            val = jnp.where(lax.rem(idj, 2) == 0, dgacc[0], dgacc[1])
            dgate_ref[pl.ds(j, 1), :] = over_rows(jnp.where(idj // 2 == home_gid(), val, 0.0))
    arrived(ROUNDS - 1)
    with scope('finish'):
        for n in range(4):
            ns = pl.ds(n * WIDE, WIDE)
            dx_ref[:, ns] = summed(ROUNDS - 1, ns).astype(BF16)
        wait(dgh.at[:, first(3)], bm_s.at[2])
        wait(snd.at[:, first(3), :, :, :, first(D)], b_s.at[2])


def hand_over(*refs):
    n = len(refs) // 3
    copies = [pltpu.make_async_copy(a, b, sem) for a, b, sem in zip(refs[:n], refs[n:2 * n], refs[2 * n:])]
    for cp in copies:
        cp.start()
    for cp in copies:
        cp.wait()


def solution(mesh):
    spec = P(('part', 'grp', 'loc'))

    def device_step(x_rows, dy_rows, expert_ids, gate_vals, w_gate, w_up, w_down):
        any_ = pl.BlockSpec(memory_space=pl.ANY)
        vmem = pl.BlockSpec(memory_space=pltpu.VMEM)
        dma = pltpu.SemaphoreType.DMA
        one, two, three, per_round = (dma((n,)) for n in (1, 2, 3, ROUNDS))
        sd = jax.ShapeDtypeStruct
        results = [sd((TOK, D), BF16), sd((TOP_K, TOK), F32), *[sd((D, F), BF16)] * 2, sd((F, D), BF16)]
        cube = (ROUNDS, SIDE, SIDE, SIDE, RS)
        lines = (ROUNDS, SIDE, SIDE, 1, LANES)
        out = pl.pallas_call(
            kernel,
            name='moe_backward',
            in_specs=[any_] * 7,
            out_specs=[vmem] * 5 + [any_] * 6,
            out_shape=[*[pltpu.VMEM(o.shape, o.dtype) for o in results], *[sd((*cube, w), BF16) for _, w in FWD + BWD]],
            scratch_shapes=[
                pltpu.VMEM((SIDE, TOK, 2 * D), BF16),
                pltpu.VMEM((*cube, 2 * D), BF16),
                pltpu.VMEM((ROUNDS + 2, SIDE, SIDE, SIDE, RS, 2 * D), BF16),
                pltpu.VMEM((D, 2 * F), BF16),
                pltpu.VMEM((F, D), BF16),
                pltpu.VMEM((3 * F, D), F32),
                pltpu.VMEM((CH, 3 * F), BF16),
                pltpu.VMEM((PLANE * GS, TOK), BF16),
                pltpu.VMEM((GROUPS, TOK), F32),
                pltpu.VMEM((3, SIDE, TOP_K, TOK), jnp.int32),
                pltpu.VMEM((SIDE, TOP_K, TOK), F32),
                pltpu.VMEM(lines, F32),
                pltpu.VMEM(lines, F32),
                pltpu.VMEM((2, *lines), F32),
                pltpu.VMEM((2, *lines), F32),
                pltpu.VMEM(lines, F32),
                pltpu.VMEM(lines, F32),
                pltpu.VMEM(lines, F32),
                pltpu.VMEM((ROUNDS, PLANE, LANES), F32),
                pltpu.VMEM((ROUNDS, SIDE, PLANE, LANES), F32),
                pltpu.VMEM((2, GROUPS, TOK), F32),
                dma((5,)), two, two, one, dma((2, 2)), one, two, two, per_round, one, per_round, dma((2, 2)), three,
                dma((2, ROUNDS)), *[two] * 4, three, dma((3, ROUNDS)), dma((2, 3)), three, dma((3, ROUNDS)),
                pltpu.SemaphoreType.REGULAR((1,)), pltpu.SemaphoreType.REGULAR((ROUNDS,)),
            ],
            compiler_params=pltpu.CompilerParams(collective_id=0, has_side_effects=True, vmem_limit_bytes=60 << 20),
        )(x_rows, dy_rows, expert_ids.T, gate_vals.T, w_gate[0], w_up[0], w_down[0])
        dx, d_gates, dwg, dwu, dwd = pl.pallas_call(
            hand_over,
            name='hand_over',
            in_specs=[vmem] * 5,
            out_specs=[any_] * 5,
            out_shape=results,
            scratch_shapes=[pltpu.SemaphoreType.DMA] * 5,
            compiler_params=pltpu.CompilerParams(vmem_limit_bytes=1 << 20),
        )(*[pltpu.with_memory_space_constraint(o, pltpu.VMEM) for o in out[:5]])
        return dx, d_gates.T, dwg[None], dwu[None], dwd[None]

    return jax.shard_map(device_step, mesh=mesh, in_specs=(spec,) * 7, out_specs=(spec,) * 5, check_vma=False)
```
